32 devices in a mesh: dp: 1 (over z), sp: 32 (over y, x, core).
Axes of the slice: x: 4, y: 4, z: 1, core: 2. Of those that a mesh axis runs over, the one named last changes fastest.
The devices are a block of a 4x4x8 slice.
Arguments:
- images: bfloat16 [32, 64, 512, 32], P('dp', 'sp')
- w_a: bfloat16 [1, 3, 3, 32, 32], replicated
- bn_a: float32 [1, 2, 32], replicated
- w_down: bfloat16 [3, 3, 32, 128], replicated
- bn_down: float32 [2, 128], replicated
- w_in: bfloat16 [3, 128, 64], replicated
- bn_in: float32 [3, 2, 64], replicated
- w_mid: bfloat16 [3, 3, 3, 64, 64], replicated
- bn_mid: float32 [3, 2, 64], replicated
- w_out: bfloat16 [3, 64, 128], replicated
- bn_out: float32 [3, 2, 128], replicated
Outputs:
- output: bfloat16 [32, 32, 256, 128], P('dp', 'sp')
All inputs are finite; a program needn't handle non-finite values.
Results may differ from the reference program's by a relative error of at most 0.0190335.
Values are sent between devices in bfloat16 or wider.
A program may use at most 768 MiB of HBM per device.

```python
import jax
import jax.numpy as jnp
from jax import lax

IMAGES = 32
ROWS_DEV = 2
IMG_WIDTH = 512
LAYERS_A = 1
BLOCKS_B = 3
CHAN_A = 32
CHAN_MID = 64
CHAN_B = 128
GROUP_SIZE = 32
NORM_EPS = 1e-5
CONV_DIMS = ("NHWC", "HWIO", "NHWC")


def conv_weight(draw_key, full_shape, fan_in):
    return (jax.random.normal(draw_key, full_shape, jnp.float32) * fan_in ** -0.5).astype(jnp.bfloat16)


def norm_params(draw_key, lead_dims, chan_count):
    key_gain, key_shift = jax.random.split(draw_key)
    norm_gain = jax.random.uniform(key_gain, lead_dims + (chan_count,), jnp.float32, 0.6, 1.4)
    norm_shift = 0.4 * jax.random.normal(key_shift, lead_dims + (chan_count,), jnp.float32)
    return jnp.stack([norm_gain, norm_shift], axis=-2)


def setup_inputs(seed: int = 0, part: int = 0) -> dict:
    base_key = jax.random.key(seed)
    part_key = jax.random.fold_in(base_key, part)
    key_noise, key_amp, key_phase = jax.random.split(part_key, 3)
    weight_keys = jax.random.split(base_key, 10)
    height = GROUP_SIZE * ROWS_DEV
    row_pos = (jnp.arange(height, dtype=jnp.float32) + 0.5) / height
    band_amp = 1.5 * jax.random.normal(key_amp, (CHAN_A,), jnp.float32)
    band_phase = 6.2832 * jax.random.uniform(key_phase, (CHAN_A,), jnp.float32)
    row_band = band_amp * (1.0 - 2.0 * row_pos)[:, None] + jnp.sin(12.566 * row_pos[:, None] + band_phase)
    pixel_noise = jax.random.normal(key_noise, (IMAGES, height, IMG_WIDTH, CHAN_A), jnp.float32)
    return {
        "images": (pixel_noise + row_band[None, :, None, :]).astype(jnp.bfloat16),
        "w_a": conv_weight(weight_keys[0], (LAYERS_A, 3, 3, CHAN_A, CHAN_A), 9 * CHAN_A),
        "bn_a": norm_params(weight_keys[1], (LAYERS_A,), CHAN_A),
        "w_down": conv_weight(weight_keys[2], (3, 3, CHAN_A, CHAN_B), 9 * CHAN_A),
        "bn_down": norm_params(weight_keys[3], (), CHAN_B),
        "w_in": conv_weight(weight_keys[4], (BLOCKS_B, CHAN_B, CHAN_MID), CHAN_B),
        "bn_in": norm_params(weight_keys[5], (BLOCKS_B,), CHAN_MID),
        "w_mid": conv_weight(weight_keys[6], (BLOCKS_B, 3, 3, CHAN_MID, CHAN_MID), 9 * CHAN_MID),
        "bn_mid": norm_params(weight_keys[7], (BLOCKS_B,), CHAN_MID),
        "w_out": conv_weight(weight_keys[8], (BLOCKS_B, CHAN_MID, CHAN_B), CHAN_MID),
        "bn_out": norm_params(weight_keys[9], (BLOCKS_B,), CHAN_B),
    }


def conv_full(hidden, weight, stride):
    return lax.conv_general_dilated(hidden.astype(jnp.float32), weight.astype(jnp.float32), (stride, stride), "SAME", dimension_numbers=CONV_DIMS)


def conv_point(hidden, weight):
    return jnp.einsum("bhwc,cd->bhwd", hidden.astype(jnp.float32), weight.astype(jnp.float32))


def batch_norm(pre_act, params):
    chan_mean = jnp.mean(pre_act, axis=(0, 1, 2))
    chan_var = jnp.mean(pre_act * pre_act, axis=(0, 1, 2)) - chan_mean * chan_mean
    chan_scale = params[0] * lax.rsqrt(chan_var + NORM_EPS)
    return (pre_act - chan_mean) * chan_scale + params[1]


def norm_relu(pre_act, params):
    return jax.nn.relu(batch_norm(pre_act, params)).astype(jnp.bfloat16)


def reference(images, w_a, bn_a, w_down, bn_down, w_in, bn_in, w_mid, bn_mid, w_out, bn_out):
    def stage_a(hidden, layer_args):
        return norm_relu(conv_full(hidden, layer_args[0], 1), layer_args[1]), None

    def bottleneck(hidden, block_args):
        w_first, bn_first, w_three, bn_three, w_last, bn_last = block_args
        branch = norm_relu(conv_point(hidden, w_first), bn_first)
        branch = norm_relu(conv_full(branch, w_three, 1), bn_three)
        summed = batch_norm(conv_point(branch, w_last), bn_last) + hidden.astype(jnp.float32)
        return jax.nn.relu(summed).astype(jnp.bfloat16), None

    hidden, _ = lax.scan(stage_a, images, (w_a, bn_a))
    hidden = norm_relu(conv_full(hidden, w_down, 2), bn_down)
    hidden, _ = lax.scan(bottleneck, hidden, (w_in, bn_in, w_mid, bn_mid, w_out, bn_out))
    return hidden
```

```python
import functools

import jax
import jax.numpy as jnp
import numpy as np
from jax import lax
from jax.experimental import pallas as pl
from jax.experimental.pallas import tpu as pltpu
from jax.sharding import PartitionSpec as P

NORM_EPS = 1e-5
MESH = pl.DeviceIdType.MESH
LANES = 128
F32 = jnp.float32
BF16 = jnp.bfloat16


def place_taps(taps, index):
    count, ci, co = taps.shape
    rows, cols = index.shape
    pick = np.zeros((rows, cols, count), np.float32)
    for r in range(rows):
        for c in range(cols):
            if index[r, c] < count:
                pick[r, c, index[r, c]] = 1.0
    blocks = jnp.einsum("rct,tio->rico", jnp.asarray(pick, BF16), taps, preferred_element_type=F32)
    return blocks.astype(BF16).reshape(rows * ci, cols * co)


def stage_a_index(halo):
    index = np.full((8, 16), 9, np.int64)
    for pi in range(2):
        for a in range(2):
            for ri in range(2):
                for shift in range(2):
                    for ro in range(2):
                        for po in range(2):
                            if halo:
                                if ri != ro:
                                    continue
                                ky = 0 if ri == 0 else 2
                            else:
                                ky = ri - ro + 1
                            if shift == 0:
                                kx = pi - po + 1
                            elif pi != po:
                                kx = 0 if pi == 1 else 2
                            else:
                                continue
                            index[(pi * 2 + a) * 2 + ri, ((shift * 2 + a) * 2 + ro) * 2 + po] = ky * 3 + kx
    return index


def down_own_index():
    index = np.full((4, 2), 9, np.int64)
    for row in range(2):
        for par in range(2):
            index[row * 2 + par, 0] = row * 3 + par
        index[row * 2, 1] = row * 3 + 2
    return index


def down_halo_index():
    index = np.full((4, 4), 9, np.int64)
    for a in range(2):
        for par in range(2):
            index[a * 2 + par, a * 2] = 6 + par
        index[a * 2, a * 2 + 1] = 8
    return index


def mid_index():
    index = np.full((6, 6), 9, np.int64)
    for src, ky in enumerate((1, 0, 2)):
        for kx in range(3):
            for a in range(2):
                index[src * 2 + a, kx * 2 + a] = ky * 3 + kx
    return index


def kernel(
    n, img_hbm, wao_ref, wah_ref, wdo_ref, wdh_ref, win_ref, wmid_ref, wout_ref, bn_ref, out_hbm,
    ximg, xabove, xbelow, tscr, za, rsend, rrecv, zd, h, zi, u2, habove, hbelow, zm, zo, stats, recv,
    img_sem, isend_sem, irecv_sem, rsend_sem, rrecv_sem, hsend_sem, hrecv_sem, ssem, rsem, out_sem,
):
    me = lax.axis_index("sp")
    nxt, prv = me + 1, me - 1
    has_next, has_prev = me < n - 1, me > 0
    pairs, chunks = ximg.shape[1], isend_sem.shape[1]
    per = pairs // chunks
    half_w = tscr.shape[0] // 2
    full_w = tscr.shape[0]
    rows_all = lax.axis_size("sp")
    count_a = float(2 * pairs * 2 * full_w) * rows_all
    count_b = float(2 * pairs * half_w) * rows_all

    local_img = [
        pltpu.make_async_copy(img_hbm.at[:, pl.ds(c * per, per)], ximg.at[:, pl.ds(c * per, per)], img_sem.at[c])
        for c in range(chunks)
    ]
    for copy in local_img:
        copy.start()

    xabove[...] = jnp.zeros_like(xabove)
    xbelow[...] = jnp.zeros_like(xbelow)

    @pl.when(me == n - 1)
    def _():
        rrecv[...] = jnp.zeros_like(rrecv)
        hbelow[...] = jnp.zeros_like(hbelow)

    @pl.when(me == 0)
    def _():
        habove[...] = jnp.zeros_like(habove)

    barrier = pltpu.get_barrier_semaphore()

    def greet(d, carry):
        pl.semaphore_signal(barrier, inc=1, device_id={"sp": lax.rem(me + d, n)}, device_id_type=MESH)
        return carry

    lax.fori_loop(1, n, greet, 0)
    pl.semaphore_wait(barrier, n - 1)

    def to_dev(src, dst, send_sem, recv_sem, dev):
        return pltpu.make_async_remote_copy(
            src_ref=src, dst_ref=dst, send_sem=send_sem, recv_sem=recv_sem, device_id={"sp": dev}, device_id_type=MESH
        )

    def img_down(c):
        part = pl.ds(c * per, per)
        return to_dev(img_hbm.at[:, part, 1], xabove.at[:, part], isend_sem.at[0, c], irecv_sem.at[0, c], nxt)

    def img_up(c):
        part = pl.ds(c * per, per)
        return to_dev(img_hbm.at[:, part, 0], xbelow.at[:, part], isend_sem.at[1, c], irecv_sem.at[1, c], prv)

    for c in range(chunks):
        @pl.when(has_next)
        def _():
            img_down(c).start()

        @pl.when(has_prev)
        def _():
            img_up(c).start()

    def shift_down(y):
        row = lax.broadcasted_iota(jnp.int32, y.shape, 0)
        return jnp.where(row == 0, 0.0, pltpu.roll(y, 1, 0))

    def shift_up(y):
        row = lax.broadcasted_iota(jnp.int32, y.shape, 0)
        return jnp.where(row == y.shape[0] - 1, 0.0, pltpu.roll(y, y.shape[0] - 1, 0))

    def add_stats(acc, z):
        blocks = z.reshape(z.shape[0] // 8, 8, LANES)
        return acc[0] + jnp.sum(blocks, axis=0), acc[1] + jnp.sum(blocks * blocks, axis=0)

    zero_acc = (jnp.zeros((8, LANES), F32), jnp.zeros((8, LANES), F32))

    def group_stats(k, acc, group):
        def fold(v):
            width = group
            while width < LANES:
                v = v + pltpu.roll(v, width, 1)
                width *= 2
            return jnp.sum(v, axis=0, keepdims=True)

        mine = jnp.concatenate([fold(acc[0]), fold(acc[1])], axis=0)
        stats[k] = mine

        def send(d, carry):
            to_dev(stats.at[k], recv.at[k, d - 1], ssem.at[k], rsem.at[k], lax.rem(me + d, n)).start()
            return carry

        lax.fori_loop(1, n, send, 0)
        to_dev(recv.at[k], recv.at[k], ssem.at[k], rsem.at[k], me).wait_recv()
        return mine + jnp.sum(recv[k], axis=0)

    def norm_of(k, total, count):
        moments = total * (1.0 / count)
        mean = moments[0:1]
        var = moments[1:2] - mean * mean
        scale = bn_ref[k, 0:1] * lax.rsqrt(var + NORM_EPS)
        return mean, scale, bn_ref[k, 1:2]

    def bn(z, norm):
        mean, scale, shift = norm
        return (z - mean) * scale + shift

    lane2 = lax.broadcasted_iota(jnp.int32, (half_w, 2 * LANES), 1)
    even_lane = lax.rem(lane2 // 32, 2) == 0

    def stage_a_part(x, w_ref):
        tscr[...] = x.astype(F32).T
        lhs = jnp.concatenate(
            [tscr[pl.ds(0, half_w, stride=2), :], tscr[pl.ds(1, half_w, stride=2), :]], axis=1
        ).astype(BF16)
        y = jnp.dot(lhs, w_ref[...], preferred_element_type=F32)
        cross = y[:, 2 * LANES:]
        return y[:, : 2 * LANES] + jnp.where(even_lane, shift_down(cross), shift_up(cross))

    for c in range(chunks):
        local_img[c].wait()

        def own_a(q, carry):
            x = jnp.concatenate(
                [ximg[0, q].reshape(2 * 32, full_w), ximg[1, q].reshape(2 * 32, full_w)], axis=0
            )
            z = stage_a_part(x, wao_ref)
            za[0, q] = z[:, :LANES]
            za[1, q] = z[:, LANES:]
            return carry

        lax.fori_loop(c * per, (c + 1) * per, own_a, 0)

    acc = zero_acc
    for c in range(chunks):
        @pl.when(has_prev)
        def _():
            img_down(c).wait_recv()

        @pl.when(has_next)
        def _():
            img_up(c).wait_recv()

        def halo_a(q, acc):
            x = jnp.concatenate([xabove[0, q], xbelow[0, q], xabove[1, q], xbelow[1, q]], axis=0)
            z = stage_a_part(x, wah_ref)
            z0 = za[0, q] + z[:, :LANES]
            z1 = za[1, q] + z[:, LANES:]
            za[0, q] = z0
            za[1, q] = z1
            return add_stats(add_stats(acc, z0), z1)

        acc = lax.fori_loop(c * per, (c + 1) * per, halo_a, acc)
    norm = norm_of(0, group_stats(0, acc, 32), count_a)

    lane1 = lax.broadcasted_iota(jnp.int32, (half_w, LANES), 1)
    low_lane = lane1 < 64

    def row_up(c):
        part = pl.ds(c * per, per)
        return to_dev(rsend.at[part], rrecv.at[part], rsend_sem.at[c], rrecv_sem.at[c], prv)

    for c in range(chunks):
        def own_down(q, carry):
            t0 = jnp.maximum(bn(za[0, q], norm), 0.0)
            t1 = jnp.maximum(bn(za[1, q], norm), 0.0)
            rsend[q] = jnp.where(low_lane, t0, pltpu.roll(t1, 64, 1)).astype(BF16)
            for a, t in enumerate((t0, t1)):
                y = jnp.dot(t.astype(BF16), wdo_ref[...], preferred_element_type=F32)
                zd[a, q] = y[:, :LANES] + shift_up(y[:, LANES:])
            return carry

        lax.fori_loop(c * per, (c + 1) * per, own_down, 0)

        @pl.when(has_prev)
        def _():
            row_up(c).start()

    acc = zero_acc
    for c in range(chunks):
        @pl.when(has_next)
        def _():
            row_up(c).wait_recv()

        def halo_down(q, acc):
            y = jnp.dot(rrecv[q], wdh_ref[...], preferred_element_type=F32)
            for a in range(2):
                lo = 2 * a * LANES
                z = zd[a, q] + y[:, lo:lo + LANES] + shift_up(y[:, lo + LANES:lo + 2 * LANES])
                zd[a, q] = z
                acc = add_stats(acc, z)
            return acc

        acc = lax.fori_loop(c * per, (c + 1) * per, halo_down, acc)
    norm = norm_of(1, group_stats(1, acc, LANES), count_b)

    blocks = win_ref.shape[0]

    def mid_down(j, c):
        part = pl.ds(c * per, per)
        return to_dev(u2.at[j, part], habove.at[j, part], hsend_sem.at[j, 0, c], hrecv_sem.at[j, 0, c], nxt)

    def mid_up(j, c):
        part = pl.ds(c * per, per)
        return to_dev(u2.at[j, part], hbelow.at[j, part], hsend_sem.at[j, 1, c], hrecv_sem.at[j, 1, c], prv)

    for j in range(blocks):
        def layer_in(q, acc):
            parts = []
            for a in range(2):
                if j == 0:
                    t = bn(zd[a, q], norm)
                else:
                    t = bn(zo[a, q], norm) + h[a, q].astype(F32)
                t = jnp.maximum(t, 0.0).astype(BF16)
                h[a, q] = t
                parts.append(t)
            z = jnp.dot(jnp.concatenate(parts, axis=1), win_ref[j], preferred_element_type=F32)
            zi[q] = z
            return add_stats(acc, z)

        acc = lax.fori_loop(0, pairs, layer_in, zero_acc)
        norm = norm_of(2 + 3 * j, group_stats(2 + 3 * j, acc, 64), count_b)

        for c in range(chunks):
            def act_in(q, carry):
                u2[j, q] = jnp.maximum(bn(zi[q], norm), 0.0).astype(BF16)
                return carry

            lax.fori_loop(c * per, (c + 1) * per, act_in, 0)

            @pl.when(has_next)
            def _():
                mid_down(j, c).start()

            @pl.when(has_prev)
            def _():
                mid_up(j, c).start()

        acc = zero_acc
        for c in range(chunks):
            @pl.when(has_prev)
            def _():
                mid_down(j, c).wait_recv()

            @pl.when(has_next)
            def _():
                mid_up(j, c).wait_recv()

            def layer_mid(q, acc):
                lhs = jnp.concatenate([u2[j, q], habove[j, q], hbelow[j, q]], axis=1)
                y = jnp.dot(lhs, wmid_ref[j], preferred_element_type=F32)
                z = shift_down(y[:, :LANES]) + y[:, LANES:2 * LANES] + shift_up(y[:, 2 * LANES:])
                zm[q] = z
                return add_stats(acc, z)

            acc = lax.fori_loop(c * per, (c + 1) * per, layer_mid, acc)
        norm = norm_of(3 + 3 * j, group_stats(3 + 3 * j, acc, 64), count_b)

        def layer_out(q, acc):
            u = jnp.maximum(bn(zm[q], norm), 0.0).astype(BF16)
            y = jnp.dot(u, wout_ref[j], preferred_element_type=F32)
            for a in range(2):
                z = y[:, a * LANES:(a + 1) * LANES]
                zo[a, q] = z
                acc = add_stats(acc, z)
            return acc

        acc = lax.fori_loop(0, pairs, layer_out, zero_acc)
        norm = norm_of(4 + 3 * j, group_stats(4 + 3 * j, acc, LANES), count_b)

    def store(c):
        part = pl.ds(c * per, per)
        return pltpu.make_async_copy(h.at[:, part], out_hbm.at[:, part], out_sem.at[c])

    for c in range(chunks):
        def final(q, carry):
            for a in range(2):
                h[a, q] = jnp.maximum(bn(zo[a, q], norm) + h[a, q].astype(F32), 0.0).astype(BF16)
            return carry

        lax.fori_loop(c * per, (c + 1) * per, final, 0)
        store(c).start()

    for k in range(stats.shape[0]):
        to_dev(recv.at[k], recv.at[k], ssem.at[k], rsem.at[k], me).wait_send()

    @pl.when(has_next)
    def _():
        for c in range(chunks):
            img_down(c).wait_send()
            for j in range(blocks):
                mid_down(j, c).wait_send()

    @pl.when(has_prev)
    def _():
        for c in range(chunks):
            img_up(c).wait_send()
            row_up(c).wait_send()
            for j in range(blocks):
                mid_up(j, c).wait_send()

    for c in range(chunks):
        store(c).wait()


def solution(mesh):
    n = mesh.shape["sp"]

    def forward(images, w_a, bn_a, w_down, bn_down, w_in, bn_in, w_mid, bn_mid, w_out, bn_out):
        count, rows, width, chan_a = images.shape
        pairs, half_w = count // 2, width // 2
        blocks = w_in.shape[0]
        chunks = min(8, pairs)
        img = jnp.transpose(images, (0, 1, 3, 2)).reshape(2, pairs, rows, chan_a, width)
        taps_a = w_a[0].reshape(9, chan_a, chan_a)
        wao = place_taps(taps_a, stage_a_index(False))
        wah = place_taps(taps_a, stage_a_index(True))
        taps_d = w_down.reshape(9, chan_a, LANES)
        wdo = place_taps(taps_d, down_own_index())
        wdh = place_taps(taps_d, down_halo_index())
        eye = np.array([[0, 1], [1, 0]], np.int64)
        win = jnp.stack([place_taps(w_in[j][None], eye) for j in range(blocks)])
        wmid = jnp.stack([place_taps(w_mid[j].reshape(9, 64, 64), mid_index()) for j in range(blocks)])
        wout = jnp.stack([place_taps(w_out[j][None], eye) for j in range(blocks)])
        layers = [jnp.tile(bn_a[0], (1, 4)), bn_down]
        for j in range(blocks):
            layers += [jnp.tile(bn_in[j], (1, 2)), jnp.tile(bn_mid[j], (1, 2)), bn_out[j]]
        bn_all = jnp.stack(layers)
        steps = len(layers)

        vmem = pl.BlockSpec(memory_space=pltpu.VMEM)
        anyspace = pl.BlockSpec(memory_space=pl.ANY)
        dma = pltpu.SemaphoreType.DMA
        out = pl.pallas_call(
            functools.partial(kernel, n),
            out_shape=jax.ShapeDtypeStruct((2, pairs, half_w, LANES), BF16),
            in_specs=[anyspace] + [vmem] * 8,
            out_specs=anyspace,
            scratch_shapes=[
                pltpu.VMEM((2, pairs, rows, chan_a, width), BF16),
                pltpu.VMEM((2, pairs, chan_a, width), BF16),
                pltpu.VMEM((2, pairs, chan_a, width), BF16),
                pltpu.VMEM((width, LANES), F32),
                pltpu.VMEM((2, pairs, half_w, LANES), F32),
                pltpu.VMEM((pairs, half_w, LANES), BF16),
                pltpu.VMEM((pairs, half_w, LANES), BF16),
                pltpu.VMEM((2, pairs, half_w, LANES), F32),
                pltpu.VMEM((2, pairs, half_w, LANES), BF16),
                pltpu.VMEM((pairs, half_w, LANES), F32),
                pltpu.VMEM((blocks, pairs, half_w, LANES), BF16),
                pltpu.VMEM((blocks, pairs, half_w, LANES), BF16),
                pltpu.VMEM((blocks, pairs, half_w, LANES), BF16),
                pltpu.VMEM((pairs, half_w, LANES), F32),
                pltpu.VMEM((2, pairs, half_w, LANES), F32),
                pltpu.VMEM((steps, 2, LANES), F32),
                pltpu.VMEM((steps, n - 1, 2, LANES), F32),
                dma((chunks,)),
                dma((2, chunks)),
                dma((2, chunks)),
                dma((chunks,)),
                dma((chunks,)),
                dma((blocks, 2, chunks)),
                dma((blocks, 2, chunks)),
                dma((steps,)),
                dma((steps,)),
                dma((chunks,)),
            ],
            compiler_params=pltpu.CompilerParams(
                collective_id=0, has_side_effects=True, vmem_limit_bytes=60 * 1024 * 1024
            ),
        )(img, wao, wah, wdo, wdh, win, wmid, wout, bn_all)
        return out.reshape(count, rows // 2, half_w, LANES)

    act_spec = P("dp", "sp", None, None)
    return jax.shard_map(forward, mesh=mesh, in_specs=(act_spec,) + (P(),) * 10, out_specs=act_spec, check_vma=False)
```

```python
import functools

import jax
import jax.numpy as jnp
from jax import lax
from jax.experimental import pallas as pl
from jax.experimental.pallas import tpu as pltpu
from jax.sharding import PartitionSpec as P

NORM_EPS = 1e-5
MESH = pl.DeviceIdType.MESH
LANES = 128
F32 = jnp.float32
BF16 = jnp.bfloat16


def placement(size, copies):
    row = lax.broadcasted_iota(jnp.int32, (size, copies * LANES), 0)
    lane = lax.broadcasted_iota(jnp.int32, (size, copies * LANES), 1)
    hit = lane == row
    for i in range(1, copies):
        hit = jnp.logical_or(hit, lane == row + i * (LANES + size))
    return hit.astype(F32).astype(BF16)


def expand_stage_a(w, own_ref, halo_ref):
    spread = jnp.dot(w, placement(32, 4), preferred_element_type=F32)
    own_ref[...] = jnp.zeros_like(own_ref)
    halo_ref[...] = jnp.zeros_like(halo_ref)
    for ref, halo in ((own_ref, False), (halo_ref, True)):
        for pi in range(2):
            for ri in range(2):
                for shift in range(2):
                    total = jnp.zeros((32, LANES), F32)
                    for ro in range(2):
                        for po in range(2):
                            if halo and ri != ro:
                                continue
                            if shift and pi == po:
                                continue
                            ky = 2 * ri if halo else ri - ro + 1
                            kx = (0 if pi == 1 else 2) if shift else pi - po + 1
                            tap, i = ky * 3 + kx, ro * 2 + po
                            total += spread[tap * 32:(tap + 1) * 32, i * LANES:(i + 1) * LANES]
                    block = total.astype(BF16)
                    for a in range(2):
                        row, col = ((pi * 2 + a) * 2 + ri) * 32, (shift * 2 + a) * LANES
                        ref[row:row + 32, col:col + LANES] = block


def expand_down(w_ref, own_ref, halo_ref):
    own_ref[...] = jnp.zeros_like(own_ref)
    halo_ref[...] = jnp.zeros_like(halo_ref)
    for par in range(2):
        for shift in range(2 - par):
            kx = 2 if shift else par
            for row in range(2):
                at = (row * 2 + par) * 32
                own_ref[at:at + 32, shift * LANES:(shift + 1) * LANES] = w_ref[row * 3 + kx]
            for a in range(2):
                at, col = (a * 2 + par) * 32, (a * 2 + shift) * LANES
                halo_ref[at:at + 32, col:col + LANES] = w_ref[6 + kx]


def expand_blocks(w_in_ref, w_mid_ref, w_out_ref, win_ref, wmid_ref, wout_ref):
    spot = placement(64, 2)
    for j in range(win_ref.shape[0]):
        w_in = w_in_ref[j].astype(F32).T.astype(BF16)
        spread = jnp.dot(w_in, spot, preferred_element_type=F32).astype(BF16)
        for a in range(2):
            win_ref[j, a * LANES:(a + 1) * LANES, :] = spread[:, a * LANES:(a + 1) * LANES]
        for src, ky in enumerate((1, 0, 2)):
            for kx in range(3):
                spread = jnp.dot(w_mid_ref[j, ky * 3 + kx], spot, preferred_element_type=F32).astype(BF16)
                for a in range(2):
                    at = (src * 2 + a) * 64
                    wmid_ref[j, at:at + 64, kx * LANES:(kx + 1) * LANES] = spread[:, a * LANES:(a + 1) * LANES]
        zeros = jnp.zeros((64, LANES), BF16)
        for a in range(2):
            for b in range(2):
                wout_ref[j, a * 64:(a + 1) * 64, b * LANES:(b + 1) * LANES] = w_out_ref[j] if a == b else zeros


def kernel(
    n, img_hbm, wa_hbm, wd_hbm, wi_hbm, wm_hbm, wo_hbm, ba_hbm, bd_hbm, bi_hbm, bm_hbm, bo_hbm, out_hbm,
    wa_raw, wd_raw, wi_raw, wm_raw, wo_raw, ba_raw, bd_raw, bi_raw, bm_raw, bo_raw, w_sem,
    wao_ref, wah_ref, wdo_ref, wdh_ref, win_ref, wmid_ref, wout_ref, bn_ref,
    ximg, xabove, xbelow, tscr, za, rsend, rrecv, zd, h, zi, u2, habove, hbelow, zm, zo, stats, recv,
    img_sem, isend_sem, irecv_sem, rsend_sem, rrecv_sem, hsend_sem, hrecv_sem, ssem, rsem, out_sem,
):
    me = lax.axis_index("sp")
    nxt, prv = me + 1, me - 1
    has_next, has_prev = me < n - 1, me > 0
    pairs, chunks = ximg.shape[1], isend_sem.shape[1]
    per = pairs // chunks
    half_w = tscr.shape[0] // 2
    full_w = tscr.shape[0]
    rows_all = lax.axis_size("sp")
    count_a = float(2 * pairs * 2 * full_w) * rows_all
    count_b = float(2 * pairs * half_w) * rows_all

    local_img = [
        pltpu.make_async_copy(img_hbm.at[:, pl.ds(c * per, per)], ximg.at[:, pl.ds(c * per, per)], img_sem.at[c])
        for c in range(chunks)
    ]
    params = [
        pltpu.make_async_copy(src, dst, w_sem.at[i])
        for i, (src, dst) in enumerate((
            (wa_hbm, wa_raw), (wd_hbm, wd_raw), (wi_hbm, wi_raw), (wm_hbm, wm_raw), (wo_hbm, wo_raw),
            (ba_hbm, ba_raw), (bd_hbm, bd_raw), (bi_hbm, bi_raw), (bm_hbm, bm_raw), (bo_hbm, bo_raw),
        ))
    ]
    params[0].start()
    for copy in local_img:
        copy.start()
    for copy in params[1:]:
        copy.start()

    xabove[...] = jnp.zeros_like(xabove)
    xbelow[...] = jnp.zeros_like(xbelow)

    @pl.when(me == n - 1)
    def _():
        rrecv[...] = jnp.zeros_like(rrecv)
        hbelow[...] = jnp.zeros_like(hbelow)

    @pl.when(me == 0)
    def _():
        habove[...] = jnp.zeros_like(habove)

    barrier = pltpu.get_barrier_semaphore()

    def greet(d, carry):
        pl.semaphore_signal(barrier, inc=1, device_id={"sp": lax.rem(me + d, n)}, device_id_type=MESH)
        return carry

    lax.fori_loop(1, n, greet, 0)
    pl.semaphore_wait(barrier, n - 1)

    def to_dev(src, dst, send_sem, recv_sem, dev):
        return pltpu.make_async_remote_copy(
            src_ref=src, dst_ref=dst, send_sem=send_sem, recv_sem=recv_sem, device_id={"sp": dev}, device_id_type=MESH
        )

    def img_down(c):
        part = pl.ds(c * per, per)
        return to_dev(img_hbm.at[:, part, 1], xabove.at[:, part], isend_sem.at[0, c], irecv_sem.at[0, c], nxt)

    def img_up(c):
        part = pl.ds(c * per, per)
        return to_dev(img_hbm.at[:, part, 0], xbelow.at[:, part], isend_sem.at[1, c], irecv_sem.at[1, c], prv)

    for c in range(chunks):
        @pl.when(has_next)
        def _():
            img_down(c).start()

        @pl.when(has_prev)
        def _():
            img_up(c).start()

    params[0].wait()
    expand_stage_a(wa_raw[...], wao_ref, wah_ref)

    def shift_down(y):
        row = lax.broadcasted_iota(jnp.int32, y.shape, 0)
        return jnp.where(row == 0, 0.0, pltpu.roll(y, 1, 0))

    def shift_up(y):
        row = lax.broadcasted_iota(jnp.int32, y.shape, 0)
        return jnp.where(row == y.shape[0] - 1, 0.0, pltpu.roll(y, y.shape[0] - 1, 0))

    def add_stats(acc, z):
        blocks = z.reshape(z.shape[0] // 8, 8, LANES)
        return acc[0] + jnp.sum(blocks, axis=0), acc[1] + jnp.sum(blocks * blocks, axis=0)

    zero_acc = (jnp.zeros((8, LANES), F32), jnp.zeros((8, LANES), F32))

    def group_stats(k, acc, group):
        def fold(v):
            width = group
            while width < LANES:
                v = v + pltpu.roll(v, width, 1)
                width *= 2
            return jnp.sum(v, axis=0, keepdims=True)

        mine = jnp.concatenate([fold(acc[0]), fold(acc[1])], axis=0)
        stats[k] = mine

        def send(d, carry):
            to_dev(stats.at[k], recv.at[k, d - 1], ssem.at[k], rsem.at[k], lax.rem(me + d, n)).start()
            return carry

        for d in sorted(range(1, n), key=lambda d: abs(2 * d - n)):
            send(d, 0)
        to_dev(recv.at[k], recv.at[k], ssem.at[k], rsem.at[k], me).wait_recv()
        return mine + jnp.sum(recv[k], axis=0)

    def norm_of(k, total, count):
        moments = total * (1.0 / count)
        mean = moments[0:1]
        var = moments[1:2] - mean * mean
        scale = bn_ref[k, 0:1] * lax.rsqrt(var + NORM_EPS)
        return mean, scale, bn_ref[k, 1:2]

    def bn(z, norm):
        mean, scale, shift = norm
        return (z - mean) * scale + shift

    lane2 = lax.broadcasted_iota(jnp.int32, (half_w, 2 * LANES), 1)
    even_lane = lax.rem(lane2 // 32, 2) == 0

    def stage_a_part(x, w_ref):
        tscr[...] = x.astype(F32).T
        lhs = jnp.concatenate(
            [tscr[pl.ds(0, half_w, stride=2), :], tscr[pl.ds(1, half_w, stride=2), :]], axis=1
        ).astype(BF16)
        y = jnp.dot(lhs, w_ref[...], preferred_element_type=F32)
        cross = y[:, 2 * LANES:]
        return y[:, : 2 * LANES] + jnp.where(even_lane, shift_down(cross), shift_up(cross))

    for c in range(chunks):
        local_img[c].wait()

        def own_a(q, carry):
            x = jnp.concatenate(
                [ximg[0, q].reshape(2 * 32, full_w), ximg[1, q].reshape(2 * 32, full_w)], axis=0
            )
            z = stage_a_part(x, wao_ref)
            za[0, q] = z[:, :LANES]
            za[1, q] = z[:, LANES:]
            return carry

        lax.fori_loop(c * per, (c + 1) * per, own_a, 0)

    for copy in params[1:]:
        copy.wait()
    expand_down(wd_raw, wdo_ref, wdh_ref)
    expand_blocks(wi_raw, wm_raw, wo_raw, win_ref, wmid_ref, wout_ref)
    bn_ref[0] = jnp.concatenate([ba_raw[0]] * 4, axis=1)
    bn_ref[1] = bd_raw[...]
    for j in range(wi_raw.shape[0]):
        bn_ref[2 + 3 * j] = jnp.concatenate([bi_raw[j]] * 2, axis=1)
        bn_ref[3 + 3 * j] = jnp.concatenate([bm_raw[j]] * 2, axis=1)
        bn_ref[4 + 3 * j] = bo_raw[j]

    acc = zero_acc
    for c in range(chunks):
        @pl.when(has_prev)
        def _():
            img_down(c).wait_recv()

        @pl.when(has_next)
        def _():
            img_up(c).wait_recv()

        def halo_a(q, acc):
            x = jnp.concatenate([xabove[0, q], xbelow[0, q], xabove[1, q], xbelow[1, q]], axis=0)
            z = stage_a_part(x, wah_ref)
            z0 = za[0, q] + z[:, :LANES]
            z1 = za[1, q] + z[:, LANES:]
            za[0, q] = z0
            za[1, q] = z1
            return add_stats(add_stats(acc, z0), z1)

        acc = lax.fori_loop(c * per, (c + 1) * per, halo_a, acc)
    norm = norm_of(0, group_stats(0, acc, 32), count_a)

    lane1 = lax.broadcasted_iota(jnp.int32, (half_w, LANES), 1)
    low_lane = lane1 < 64

    def row_up(c):
        part = pl.ds(c * per, per)
        return to_dev(rsend.at[part], rrecv.at[part], rsend_sem.at[c], rrecv_sem.at[c], prv)

    for c in range(chunks):
        def own_down(q, carry):
            t0 = jnp.maximum(bn(za[0, q], norm), 0.0)
            t1 = jnp.maximum(bn(za[1, q], norm), 0.0)
            rsend[q] = jnp.where(low_lane, t0, pltpu.roll(t1, 64, 1)).astype(BF16)
            for a, t in enumerate((t0, t1)):
                y = jnp.dot(t.astype(BF16), wdo_ref[...], preferred_element_type=F32)
                zd[a, q] = y[:, :LANES] + shift_up(y[:, LANES:])
            return carry

        lax.fori_loop(c * per, (c + 1) * per, own_down, 0)

        @pl.when(has_prev)
        def _():
            row_up(c).start()

    acc = zero_acc
    for c in range(chunks):
        @pl.when(has_next)
        def _():
            row_up(c).wait_recv()

        def halo_down(q, acc):
            y = jnp.dot(rrecv[q], wdh_ref[...], preferred_element_type=F32)
            for a in range(2):
                lo = 2 * a * LANES
                z = zd[a, q] + y[:, lo:lo + LANES] + shift_up(y[:, lo + LANES:lo + 2 * LANES])
                zd[a, q] = z
                acc = add_stats(acc, z)
            return acc

        acc = lax.fori_loop(c * per, (c + 1) * per, halo_down, acc)
    norm = norm_of(1, group_stats(1, acc, LANES), count_b)

    blocks = win_ref.shape[0]

    def mid_down(j, c):
        part = pl.ds(c * per, per)
        return to_dev(u2.at[j, part], habove.at[j, part], hsend_sem.at[j, 0, c], hrecv_sem.at[j, 0, c], nxt)

    def mid_up(j, c):
        part = pl.ds(c * per, per)
        return to_dev(u2.at[j, part], hbelow.at[j, part], hsend_sem.at[j, 1, c], hrecv_sem.at[j, 1, c], prv)

    for j in range(blocks):
        def layer_in(q, acc):
            parts = []
            for a in range(2):
                if j == 0:
                    t = bn(zd[a, q], norm)
                else:
                    t = bn(zo[a, q], norm) + h[a, q].astype(F32)
                t = jnp.maximum(t, 0.0).astype(BF16)
                h[a, q] = t
                parts.append(t)
            z = jnp.dot(jnp.concatenate(parts, axis=1), win_ref[j], preferred_element_type=F32)
            zi[q] = z
            return add_stats(acc, z)

        acc = lax.fori_loop(0, pairs, layer_in, zero_acc)
        norm = norm_of(2 + 3 * j, group_stats(2 + 3 * j, acc, 64), count_b)

        for c in range(chunks):
            def act_in(q, carry):
                u2[j, q] = jnp.maximum(bn(zi[q], norm), 0.0).astype(BF16)
                return carry

            lax.fori_loop(c * per, (c + 1) * per, act_in, 0)

            @pl.when(has_next)
            def _():
                mid_down(j, c).start()

            @pl.when(has_prev)
            def _():
                mid_up(j, c).start()

        acc = zero_acc
        for c in range(chunks):
            @pl.when(has_prev)
            def _():
                mid_down(j, c).wait_recv()

            @pl.when(has_next)
            def _():
                mid_up(j, c).wait_recv()

            def layer_mid(q, acc):
                lhs = jnp.concatenate([u2[j, q], habove[j, q], hbelow[j, q]], axis=1)
                y = jnp.dot(lhs, wmid_ref[j], preferred_element_type=F32)
                z = shift_down(y[:, :LANES]) + y[:, LANES:2 * LANES] + shift_up(y[:, 2 * LANES:])
                zm[q] = z
                return add_stats(acc, z)

            acc = lax.fori_loop(c * per, (c + 1) * per, layer_mid, acc)
        norm = norm_of(3 + 3 * j, group_stats(3 + 3 * j, acc, 64), count_b)

        def layer_out(q, acc):
            u = jnp.maximum(bn(zm[q], norm), 0.0).astype(BF16)
            y = jnp.dot(u, wout_ref[j], preferred_element_type=F32)
            for a in range(2):
                z = y[:, a * LANES:(a + 1) * LANES]
                zo[a, q] = z
                acc = add_stats(acc, z)
            return acc

        acc = lax.fori_loop(0, pairs, layer_out, zero_acc)
        norm = norm_of(4 + 3 * j, group_stats(4 + 3 * j, acc, LANES), count_b)

    def store(c):
        part = pl.ds(c * per, per)
        return pltpu.make_async_copy(h.at[:, part], out_hbm.at[:, part], out_sem.at[c])

    for c in range(chunks):
        def final(q, carry):
            for a in range(2):
                h[a, q] = jnp.maximum(bn(zo[a, q], norm) + h[a, q].astype(F32), 0.0).astype(BF16)
            return carry

        lax.fori_loop(c * per, (c + 1) * per, final, 0)
        store(c).start()

    for k in range(stats.shape[0]):
        to_dev(recv.at[k], recv.at[k], ssem.at[k], rsem.at[k], me).wait_send()

    @pl.when(has_next)
    def _():
        for c in range(chunks):
            img_down(c).wait_send()
            for j in range(blocks):
                mid_down(j, c).wait_send()

    @pl.when(has_prev)
    def _():
        for c in range(chunks):
            img_up(c).wait_send()
            row_up(c).wait_send()
            for j in range(blocks):
                mid_up(j, c).wait_send()

    for c in range(chunks):
        store(c).wait()


def solution(mesh):
    n = mesh.shape["sp"]

    def forward(images, w_a, bn_a, w_down, bn_down, w_in, bn_in, w_mid, bn_mid, w_out, bn_out):
        count, rows, width, chan_a = images.shape
        pairs, half_w = count // 2, width // 2
        blocks = w_in.shape[0]
        chunks = min(8, pairs)
        img = jnp.transpose(images, (0, 1, 3, 2)).reshape(2, pairs, rows, chan_a, width)
        taps = w_a.shape[1] * w_a.shape[2]
        raw = [
            w_a.reshape(taps * chan_a, chan_a), w_down.reshape(taps, chan_a, LANES), jnp.transpose(w_in, (0, 2, 1)),
            w_mid.reshape(blocks, taps, 64, 64), w_out, bn_a, bn_down, bn_in, bn_mid, bn_out,
        ]
        steps = 2 + 3 * blocks

        anyspace = pl.BlockSpec(memory_space=pl.ANY)
        dma = pltpu.SemaphoreType.DMA
        out = pl.pallas_call(
            functools.partial(kernel, n),
            out_shape=jax.ShapeDtypeStruct((2, pairs, half_w, LANES), BF16),
            in_specs=[pl.BlockSpec(memory_space=pltpu.HBM)] * 11,
            out_specs=anyspace,
            scratch_shapes=[pltpu.VMEM(x.shape, x.dtype) for x in raw] + [
                dma((len(raw),)),
                pltpu.VMEM((2 * LANES, 4 * LANES), BF16),
                pltpu.VMEM((2 * LANES, 4 * LANES), BF16),
                pltpu.VMEM((LANES, 2 * LANES), BF16),
                pltpu.VMEM((LANES, 4 * LANES), BF16),
                pltpu.VMEM((blocks, 2 * LANES, LANES), BF16),
                pltpu.VMEM((blocks, 3 * LANES, 3 * LANES), BF16),
                pltpu.VMEM((blocks, LANES, 2 * LANES), BF16),
                pltpu.VMEM((steps, 2, LANES), F32),
                pltpu.VMEM((2, pairs, rows, chan_a, width), BF16),
                pltpu.VMEM((2, pairs, chan_a, width), BF16),
                pltpu.VMEM((2, pairs, chan_a, width), BF16),
                pltpu.VMEM((width, LANES), F32),
                pltpu.VMEM((2, pairs, half_w, LANES), F32),
                pltpu.VMEM((pairs, half_w, LANES), BF16),
                pltpu.VMEM((pairs, half_w, LANES), BF16),
                pltpu.VMEM((2, pairs, half_w, LANES), F32),
                pltpu.VMEM((2, pairs, half_w, LANES), BF16),
                pltpu.VMEM((pairs, half_w, LANES), F32),
                pltpu.VMEM((blocks, pairs, half_w, LANES), BF16),
                pltpu.VMEM((blocks, pairs, half_w, LANES), BF16),
                pltpu.VMEM((blocks, pairs, half_w, LANES), BF16),
                pltpu.VMEM((pairs, half_w, LANES), F32),
                pltpu.VMEM((2, pairs, half_w, LANES), F32),
                pltpu.VMEM((steps, 2, LANES), F32),
                pltpu.VMEM((steps, n - 1, 2, LANES), F32),
                dma((chunks,)),
                dma((2, chunks)),
                dma((2, chunks)),
                dma((chunks,)),
                dma((chunks,)),
                dma((blocks, 2, chunks)),
                dma((blocks, 2, chunks)),
                dma((steps,)),
                dma((steps,)),
                dma((chunks,)),
            ],
            compiler_params=pltpu.CompilerParams(
                collective_id=0, has_side_effects=True, vmem_limit_bytes=60 * 1024 * 1024
            ),
        )(img, *raw)
        return out.reshape(count, rows // 2, half_w, LANES)

    act_spec = P("dp", "sp", None, None)
    return jax.shard_map(forward, mesh=mesh, in_specs=(act_spec,) + (P(),) * 10, out_specs=act_spec, check_vma=False)
```

```python
import functools

import jax
import jax.numpy as jnp
from jax import lax
from jax.experimental import pallas as pl
from jax.experimental.pallas import tpu as pltpu
from jax.sharding import PartitionSpec as P

NORM_EPS = 1e-5
MESH = pl.DeviceIdType.MESH
LANES = 128
IMG_CUTS = (5, 5, 4, 2)
LATE_CUTS = (4, 4, 2, 1)
EARLY_CUTS = (1, 4)
OUT_CUTS = (6, 6, 3, 1)
ROW_EARLY, MID_EARLY, OF_PAIRS = 3, 5, 16
F32 = jnp.float32
BF16 = jnp.bfloat16


def cuts(first, last, weights):
    total, seen, edge, spans = sum(weights), 0, first, []
    for weight in weights:
        seen += weight
        end = first + (last - first) * seen // total
        if end > edge:
            spans.append((edge, end - edge))
        edge = end
    return spans


def over(span, body, carry=0, step=1):
    start, length = span
    trips = length // step

    def trip(i, carry):
        for k in range(step):
            carry = body(start + i * step + k, carry)
        return carry

    if trips == 1:
        carry = trip(0, carry)
    elif trips > 1:
        carry = lax.fori_loop(0, trips, trip, carry)
    for q in range(start + trips * step, start + length):
        carry = body(q, carry)
    return carry


def placement(size, copies):
    row = lax.broadcasted_iota(jnp.int32, (size, copies * LANES), 0)
    lane = lax.broadcasted_iota(jnp.int32, (size, copies * LANES), 1)
    hit = lane == row
    for i in range(1, copies):
        hit = jnp.logical_or(hit, lane == row + i * (LANES + size))
    return hit.astype(F32).astype(BF16)


def expand_stage_a(w, own_ref, halo_ref):
    spread = jnp.dot(w, placement(32, 4), preferred_element_type=F32)
    own_ref[...] = jnp.zeros_like(own_ref)
    halo_ref[...] = jnp.zeros_like(halo_ref)
    for ref, halo in ((own_ref, False), (halo_ref, True)):
        for pi in range(2):
            for ri in range(2):
                for shift in range(2):
                    total = jnp.zeros((32, LANES), F32)
                    for ro in range(2):
                        for po in range(2):
                            if halo and ri != ro:
                                continue
                            if shift and pi == po:
                                continue
                            ky = 2 * ri if halo else ri - ro + 1
                            kx = (0 if pi == 1 else 2) if shift else pi - po + 1
                            tap, i = ky * 3 + kx, ro * 2 + po
                            total += spread[tap * 32:(tap + 1) * 32, i * LANES:(i + 1) * LANES]
                    block = total.astype(BF16)
                    for a in range(2):
                        row, col = ((pi * 2 + a) * 2 + ri) * 32, (shift * 2 + a) * LANES
                        ref[row:row + 32, col:col + LANES] = block


def expand_down(w_ref, own_ref, halo_ref):
    own_ref[...] = jnp.zeros_like(own_ref)
    halo_ref[...] = jnp.zeros_like(halo_ref)
    for par in range(2):
        for shift in range(2 - par):
            kx = 2 if shift else par
            for row in range(2):
                at = (row * 2 + par) * 32
                own_ref[at:at + 32, shift * LANES:(shift + 1) * LANES] = w_ref[row * 3 + kx]
            for a in range(2):
                at, col = (a * 2 + par) * 32, (a * 2 + shift) * LANES
                halo_ref[at:at + 32, col:col + LANES] = w_ref[6 + kx]


def expand_blocks(w_in_ref, w_mid_ref, w_out_ref, win_ref, wmid_ref, wout_ref):
    spot = placement(64, 2)
    for j in range(win_ref.shape[0]):
        w_in = w_in_ref[j].astype(F32).T.astype(BF16)
        spread = jnp.dot(w_in, spot, preferred_element_type=F32).astype(BF16)
        for a in range(2):
            win_ref[j, a * LANES:(a + 1) * LANES, :] = spread[:, a * LANES:(a + 1) * LANES]
        for src, ky in enumerate((1, 0, 2)):
            for kx in range(3):
                spread = jnp.dot(w_mid_ref[j, ky * 3 + kx], spot, preferred_element_type=F32).astype(BF16)
                for a in range(2):
                    at = (src * 2 + a) * 64
                    wmid_ref[j, at:at + 64, kx * LANES:(kx + 1) * LANES] = spread[:, a * LANES:(a + 1) * LANES]
        zeros = jnp.zeros((64, LANES), BF16)
        for a in range(2):
            for b in range(2):
                wout_ref[j, a * 64:(a + 1) * 64, b * LANES:(b + 1) * LANES] = w_out_ref[j] if a == b else zeros


def kernel(
    n, img_hbm, wa_hbm, wd_hbm, wi_hbm, wm_hbm, wo_hbm, ba_hbm, bd_hbm, bi_hbm, bm_hbm, bo_hbm, out_hbm,
    wa_raw, wd_raw, wi_raw, wm_raw, wo_raw, ba_raw, bd_raw, bi_raw, bm_raw, bo_raw, w_sem,
    wao_ref, wah_ref, wdo_ref, wdh_ref, win_ref, wmid_ref, wout_ref, bn_ref,
    ximg, xabove, xbelow, tscr, za, rsend, rrecv, zrow, zrow_in, zd, h, zi, u2, habove, hbelow, zabove, zbelow,
    zm, zo, stats, recv,
    img_sem, isend_sem, irecv_sem, rsend_sem, rrecv_sem, zsend_sem, zrecv_sem, hsend_sem, hrecv_sem,
    esend_sem, erecv_sem, ssem, rsem, out_sem,
):
    me = lax.axis_index("sp")
    nxt, prv = me + 1, me - 1
    has_next, has_prev = me < n - 1, me > 0
    pairs = ximg.shape[1]
    half_w = tscr.shape[0] // 2
    full_w = tscr.shape[0]
    count_a = float(2 * pairs * 2 * full_w * n)
    count_b = float(2 * pairs * half_w * n)
    everything = (0, pairs)

    img_load = cuts(0, pairs, (4, 4, 4, 4))
    img_spans = cuts(0, pairs, IMG_CUTS)
    row_early, mid_early = zrow.shape[0], zabove.shape[1]
    row_spans = cuts(row_early, pairs, LATE_CUTS)
    mid_spans = cuts(mid_early, pairs, LATE_CUTS)
    early_spans = cuts(0, mid_early, EARLY_CUTS)
    out_spans = cuts(0, pairs, OUT_CUTS)

    params = [
        pltpu.make_async_copy(src, dst, w_sem.at[i])
        for i, (src, dst) in enumerate((
            (wa_hbm, wa_raw), (wd_hbm, wd_raw), (wi_hbm, wi_raw), (wm_hbm, wm_raw), (wo_hbm, wo_raw),
            (ba_hbm, ba_raw), (bd_hbm, bd_raw), (bi_hbm, bi_raw), (bm_hbm, bm_raw), (bo_hbm, bo_raw),
        ))
    ]
    local_img = [
        pltpu.make_async_copy(img_hbm.at[:, pl.ds(*span)], ximg.at[:, pl.ds(*span)], img_sem.at[c])
        for c, span in enumerate(img_load)
    ]
    barrier = pltpu.get_barrier_semaphore()
    for d in range(1, n):
        pl.semaphore_signal(barrier, inc=1, device_id={"sp": lax.rem(me + d, n)}, device_id_type=MESH)
    params[0].start()
    for copy in local_img:
        copy.start()
    for copy in params[1:]:
        copy.start()

    @pl.when(me == n - 1)
    def _():
        xbelow[...] = jnp.zeros_like(xbelow)
        rrecv[...] = jnp.zeros_like(rrecv)
        hbelow[...] = jnp.zeros_like(hbelow)

    @pl.when(me == 0)
    def _():
        xabove[...] = jnp.zeros_like(xabove)
        habove[...] = jnp.zeros_like(habove)

    pl.semaphore_wait(barrier, n - 1)

    def to_dev(src, dst, send_sem, recv_sem, dev):
        return pltpu.make_async_remote_copy(
            src_ref=src, dst_ref=dst, send_sem=send_sem, recv_sem=recv_sem, device_id={"sp": dev}, device_id_type=MESH
        )

    def img_down(c):
        part = pl.ds(*img_spans[c])
        return to_dev(img_hbm.at[:, part, 1], xabove.at[:, part], isend_sem.at[0, c], irecv_sem.at[0, c], nxt)

    def img_up(c):
        part = pl.ds(*img_spans[c])
        return to_dev(img_hbm.at[:, part, 0], xbelow.at[:, part], isend_sem.at[1, c], irecv_sem.at[1, c], prv)

    def exchange(down, up, c):
        @pl.when(has_next)
        def _():
            down(c).start()

        @pl.when(has_prev)
        def _():
            up(c).start()

    def arrived(down, up, c):
        @pl.when(has_prev)
        def _():
            down(c).wait_recv()

        @pl.when(has_next)
        def _():
            up(c).wait_recv()

    for c in range(len(img_spans)):
        exchange(img_down, img_up, c)

    params[0].wait()
    expand_stage_a(wa_raw[...], wao_ref, wah_ref)

    def shift_down(y):
        row = lax.broadcasted_iota(jnp.int32, y.shape, 0)
        return jnp.where(row == 0, 0.0, pltpu.roll(y, 1, 0))

    def shift_up(y):
        row = lax.broadcasted_iota(jnp.int32, y.shape, 0)
        return jnp.where(row == y.shape[0] - 1, 0.0, pltpu.roll(y, y.shape[0] - 1, 0))

    def add_stats(acc, z):
        blocks = z.reshape(z.shape[0] // 8, 8, LANES)
        return acc[0] + jnp.sum(blocks, axis=0), acc[1] + jnp.sum(blocks * blocks, axis=0)

    zero_acc = (jnp.zeros((8, LANES), F32), jnp.zeros((8, LANES), F32))

    def group_stats(k, acc, group, meanwhile=None):
        def fold(v):
            width = group
            while width < LANES:
                v = v + pltpu.roll(v, width, 1)
                width *= 2
            return jnp.sum(v, axis=0, keepdims=True)

        mine = jnp.concatenate([fold(acc[0]), fold(acc[1])], axis=0)
        stats[k] = mine
        for d in sorted(range(1, n), key=lambda d: abs(2 * d - n)):
            to_dev(stats.at[k], recv.at[k, d - 1], ssem.at[k], rsem.at[k], lax.rem(me + d, n)).start()
        if meanwhile is not None:
            meanwhile()
        to_dev(recv.at[k], recv.at[k], ssem.at[k], rsem.at[k], me).wait_recv()
        return mine + jnp.sum(recv[k], axis=0)

    def norm_of(k, total, count):
        moments = total * (1.0 / count)
        mean = moments[0:1]
        var = moments[1:2] - mean * mean
        scale = bn_ref[k, 0:1] * lax.rsqrt(var + NORM_EPS)
        return mean, scale, bn_ref[k, 1:2]

    def bn(z, norm):
        mean, scale, shift = norm
        return (z - mean) * scale + shift

    lane2 = lax.broadcasted_iota(jnp.int32, (half_w, 2 * LANES), 1)
    even_lane = lax.rem(lane2 // 32, 2) == 0

    def stage_a_part(x, w_ref):
        tscr[...] = x.astype(F32).T
        lhs = jnp.concatenate(
            [tscr[pl.ds(0, half_w, stride=2), :], tscr[pl.ds(1, half_w, stride=2), :]], axis=1
        ).astype(BF16)
        y = jnp.dot(lhs, w_ref[...], preferred_element_type=F32)
        cross = y[:, 2 * LANES:]
        return y[:, : 2 * LANES] + jnp.where(even_lane, shift_down(cross), shift_up(cross))

    def own_a(q, carry):
        x = jnp.concatenate([ximg[0, q].reshape(2 * 32, full_w), ximg[1, q].reshape(2 * 32, full_w)], axis=0)
        z = stage_a_part(x, wao_ref)
        za[0, q] = z[:, :LANES]
        za[1, q] = z[:, LANES:]
        return carry

    for c, span in enumerate(img_load):
        local_img[c].wait()
        over(span, own_a)

    for copy in params[1:]:
        copy.wait()
    expand_down(wd_raw, wdo_ref, wdh_ref)
    expand_blocks(wi_raw, wm_raw, wo_raw, win_ref, wmid_ref, wout_ref)
    bn_ref[0] = jnp.concatenate([ba_raw[0]] * 4, axis=1)
    bn_ref[1] = bd_raw[...]
    for j in range(wi_raw.shape[0]):
        bn_ref[2 + 3 * j] = jnp.concatenate([bi_raw[j]] * 2, axis=1)
        bn_ref[3 + 3 * j] = jnp.concatenate([bm_raw[j]] * 2, axis=1)
        bn_ref[4 + 3 * j] = bo_raw[j]

    def halo_a(q, acc):
        x = jnp.concatenate([xabove[0, q], xbelow[0, q], xabove[1, q], xbelow[1, q]], axis=0)
        z = stage_a_part(x, wah_ref)
        z0 = za[0, q] + z[:, :LANES]
        z1 = za[1, q] + z[:, LANES:]
        za[0, q] = z0
        za[1, q] = z1
        return add_stats(add_stats(acc, z0), z1)

    acc = zero_acc
    for c, span in enumerate(img_spans):
        arrived(img_down, img_up, c)
        acc = over(span, halo_a, acc)

    lane1 = lax.broadcasted_iota(jnp.int32, (half_w, LANES), 1)
    low_lane = lane1 < 64

    def row_up(c):
        part = pl.ds(*row_spans[c])
        return to_dev(rsend.at[part], rrecv.at[part], rsend_sem.at[c], rrecv_sem.at[c], prv)

    def early_row_up():
        return to_dev(zrow, zrow_in, zsend_sem, zrecv_sem, prv)

    def first_rows(t0, t1):
        return jnp.where(low_lane, t0, pltpu.roll(t1, 64, 1))

    def send_early_rows():
        def pack(q, carry):
            zrow[q] = first_rows(za[0, q], za[1, q])
            return carry

        over((0, row_early), pack)

        @pl.when(has_prev)
        def _():
            early_row_up().start()

    norm = norm_of(0, group_stats(0, acc, 32, send_early_rows if row_early else None), count_a)

    def pack_row(q, carry):
        rsend[q] = jnp.maximum(bn(first_rows(za[0, q], za[1, q]), norm), 0.0).astype(BF16)
        return carry

    for c, span in enumerate(row_spans):
        over(span, pack_row)

        @pl.when(has_prev)
        def _():
            row_up(c).start()

    def own_down(q, carry):
        for a in range(2):
            t = jnp.maximum(bn(za[a, q], norm), 0.0).astype(BF16)
            y = jnp.dot(t, wdo_ref[...], preferred_element_type=F32)
            zd[a, q] = y[:, :LANES] + shift_up(y[:, LANES:])
        return carry

    over(everything, own_down)

    if row_early:
        @pl.when(has_next)
        def _():
            early_row_up().wait_recv()

            def norm_row(q, carry):
                rrecv[q] = jnp.maximum(bn(zrow_in[q], norm), 0.0).astype(BF16)
                return carry

            over((0, row_early), norm_row)

    def halo_down(q, acc):
        y = jnp.dot(rrecv[q], wdh_ref[...], preferred_element_type=F32)
        for a in range(2):
            lo = 2 * a * LANES
            z = zd[a, q] + y[:, lo:lo + LANES] + shift_up(y[:, lo + LANES:lo + 2 * LANES])
            zd[a, q] = z
            acc = add_stats(acc, z)
        return acc

    acc = over((0, row_early), halo_down, zero_acc)
    for c, span in enumerate(row_spans):
        @pl.when(has_next)
        def _():
            row_up(c).wait_recv()

        acc = over(span, halo_down, acc)
    norm = norm_of(1, group_stats(1, acc, LANES), count_b)

    blocks = win_ref.shape[0]

    def mid_down(j):
        def copy(c):
            part = pl.ds(*mid_spans[c])
            return to_dev(u2.at[j, part], habove.at[j, part], hsend_sem.at[j, 0, c], hrecv_sem.at[j, 0, c], nxt)
        return copy

    def mid_up(j):
        def copy(c):
            part = pl.ds(*mid_spans[c])
            return to_dev(u2.at[j, part], hbelow.at[j, part], hsend_sem.at[j, 1, c], hrecv_sem.at[j, 1, c], prv)
        return copy

    def early_down(j):
        def copy(c):
            part = pl.ds(*early_spans[c])
            return to_dev(zi.at[j, part], zabove.at[j, part], esend_sem.at[j, 0, c], erecv_sem.at[j, 0, c], nxt)
        return copy

    def early_up(j):
        def copy(c):
            part = pl.ds(*early_spans[c])
            return to_dev(zi.at[j, part], zbelow.at[j, part], esend_sem.at[j, 1, c], erecv_sem.at[j, 1, c], prv)
        return copy

    for j in range(blocks):
        def layer_in(q, acc):
            parts = []
            for a in range(2):
                if j == 0:
                    t = bn(zd[a, q], norm)
                else:
                    t = bn(zo[a, q], norm) + h[a, q].astype(F32)
                t = jnp.maximum(t, 0.0).astype(BF16)
                h[a, q] = t
                parts.append(t)
            z = jnp.dot(jnp.concatenate(parts, axis=1), win_ref[j], preferred_element_type=F32)
            zi[j, q] = z
            return add_stats(acc, z)

        acc, done = zero_acc, 0
        if early_spans:
            done = early_spans[0][1]
            acc = over(early_spans[0], layer_in, acc)
            exchange(early_down(j), early_up(j), 0)
        acc = over((done, pairs - done), layer_in, acc, 2)

        def send_early():
            for c in range(1, len(early_spans)):
                exchange(early_down(j), early_up(j), c)

        norm = norm_of(2 + 3 * j, group_stats(2 + 3 * j, acc, 64, send_early), count_b)

        def act_in(q, carry):
            u2[j, q] = jnp.maximum(bn(zi[j, q], norm), 0.0).astype(BF16)
            return carry

        for c, span in enumerate(mid_spans):
            over(span, act_in)
            exchange(mid_down(j), mid_up(j), c)
        over((0, mid_early), act_in)

        if early_spans:
            for c in range(len(early_spans)):
                arrived(early_down(j), early_up(j), c)

            def act_above(q, carry):
                habove[j, q] = jnp.maximum(bn(zabove[j, q], norm), 0.0).astype(BF16)
                return carry

            def act_below(q, carry):
                hbelow[j, q] = jnp.maximum(bn(zbelow[j, q], norm), 0.0).astype(BF16)
                return carry

            @pl.when(has_prev)
            def _():
                over((0, mid_early), act_above)

            @pl.when(has_next)
            def _():
                over((0, mid_early), act_below)

        def layer_mid(q, acc):
            lhs = jnp.concatenate([u2[j, q], habove[j, q], hbelow[j, q]], axis=1)
            y = jnp.dot(lhs, wmid_ref[j], preferred_element_type=F32)
            z = shift_down(y[:, :LANES]) + y[:, LANES:2 * LANES] + shift_up(y[:, 2 * LANES:])
            zm[q] = z
            return add_stats(acc, z)

        acc = over((0, mid_early), layer_mid, zero_acc)
        for c, span in enumerate(mid_spans):
            arrived(mid_down(j), mid_up(j), c)
            acc = over(span, layer_mid, acc)
        norm = norm_of(3 + 3 * j, group_stats(3 + 3 * j, acc, 64), count_b)

        def layer_out(q, acc):
            u = jnp.maximum(bn(zm[q], norm), 0.0).astype(BF16)
            y = jnp.dot(u, wout_ref[j], preferred_element_type=F32)
            for a in range(2):
                z = y[:, a * LANES:(a + 1) * LANES]
                zo[a, q] = z
                acc = add_stats(acc, z)
            return acc

        acc = over(everything, layer_out, zero_acc, 2)
        norm = norm_of(4 + 3 * j, group_stats(4 + 3 * j, acc, LANES), count_b)

    def store(c):
        part = pl.ds(*out_spans[c])
        return pltpu.make_async_copy(h.at[:, part], out_hbm.at[:, part], out_sem.at[c])

    def final(q, carry):
        for a in range(2):
            h[a, q] = jnp.maximum(bn(zo[a, q], norm) + h[a, q].astype(F32), 0.0).astype(BF16)
        return carry

    for c, span in enumerate(out_spans):
        over(span, final)
        store(c).start()

    for k in range(stats.shape[0]):
        to_dev(recv.at[k], recv.at[k], ssem.at[k], rsem.at[k], me).wait_send()

    @pl.when(has_next)
    def _():
        for c in range(len(img_spans)):
            img_down(c).wait_send()
        for j in range(blocks):
            for c in range(len(mid_spans)):
                mid_down(j)(c).wait_send()
            for c in range(len(early_spans)):
                early_down(j)(c).wait_send()

    @pl.when(has_prev)
    def _():
        for c in range(len(img_spans)):
            img_up(c).wait_send()
        for c in range(len(row_spans)):
            row_up(c).wait_send()
        if row_early:
            early_row_up().wait_send()
        for j in range(blocks):
            for c in range(len(mid_spans)):
                mid_up(j)(c).wait_send()
            for c in range(len(early_spans)):
                early_up(j)(c).wait_send()

    for c in range(len(out_spans)):
        store(c).wait()


def solution(mesh):
    n = mesh.shape["sp"]

    def forward(images, w_a, bn_a, w_down, bn_down, w_in, bn_in, w_mid, bn_mid, w_out, bn_out):
        count, rows, width, chan_a = images.shape
        pairs, half_w = count // 2, width // 2
        blocks = w_in.shape[0]
        row_early, mid_early = pairs * ROW_EARLY // OF_PAIRS, pairs * MID_EARLY // OF_PAIRS
        img = jnp.transpose(images, (0, 1, 3, 2)).reshape(2, pairs, rows, chan_a, width)
        taps = w_a.shape[1] * w_a.shape[2]
        raw = [
            w_a.reshape(taps * chan_a, chan_a), w_down.reshape(taps, chan_a, LANES), jnp.transpose(w_in, (0, 2, 1)),
            w_mid.reshape(blocks, taps, 64, 64), w_out, bn_a, bn_down, bn_in, bn_mid, bn_out,
        ]
        steps = 2 + 3 * blocks

        anyspace = pl.BlockSpec(memory_space=pl.ANY)
        dma = pltpu.SemaphoreType.DMA
        out = pl.pallas_call(
            functools.partial(kernel, n),
            out_shape=jax.ShapeDtypeStruct((2, pairs, half_w, LANES), BF16),
            in_specs=[pl.BlockSpec(memory_space=pltpu.HBM)] * 11,
            out_specs=anyspace,
            scratch_shapes=[pltpu.VMEM(x.shape, x.dtype) for x in raw] + [
                dma((len(raw),)),
                pltpu.VMEM((2 * LANES, 4 * LANES), BF16),
                pltpu.VMEM((2 * LANES, 4 * LANES), BF16),
                pltpu.VMEM((LANES, 2 * LANES), BF16),
                pltpu.VMEM((LANES, 4 * LANES), BF16),
                pltpu.VMEM((blocks, 2 * LANES, LANES), BF16),
                pltpu.VMEM((blocks, 3 * LANES, 3 * LANES), BF16),
                pltpu.VMEM((blocks, LANES, 2 * LANES), BF16),
                pltpu.VMEM((steps, 2, LANES), F32),
                pltpu.VMEM((2, pairs, rows, chan_a, width), BF16),
                pltpu.VMEM((2, pairs, chan_a, width), BF16),
                pltpu.VMEM((2, pairs, chan_a, width), BF16),
                pltpu.VMEM((width, LANES), F32),
                pltpu.VMEM((2, pairs, half_w, LANES), F32),
                pltpu.VMEM((pairs, half_w, LANES), BF16),
                pltpu.VMEM((pairs, half_w, LANES), BF16),
                pltpu.VMEM((row_early, half_w, LANES), F32),
                pltpu.VMEM((row_early, half_w, LANES), F32),
                pltpu.VMEM((2, pairs, half_w, LANES), F32),
                pltpu.VMEM((2, pairs, half_w, LANES), BF16),
                pltpu.VMEM((blocks, pairs, half_w, LANES), F32),
                pltpu.VMEM((blocks, pairs, half_w, LANES), BF16),
                pltpu.VMEM((blocks, pairs, half_w, LANES), BF16),
                pltpu.VMEM((blocks, pairs, half_w, LANES), BF16),
                pltpu.VMEM((blocks, mid_early, half_w, LANES), F32),
                pltpu.VMEM((blocks, mid_early, half_w, LANES), F32),
                pltpu.VMEM((pairs, half_w, LANES), F32),
                pltpu.VMEM((2, pairs, half_w, LANES), F32),
                pltpu.VMEM((steps, 2, LANES), F32),
                pltpu.VMEM((steps, n - 1, 2, LANES), F32),
                dma((4,)),
                dma((2, len(IMG_CUTS))),
                dma((2, len(IMG_CUTS))),
                dma((len(LATE_CUTS),)),
                dma((len(LATE_CUTS),)),
                dma,
                dma,
                dma((blocks, 2, len(LATE_CUTS))),
                dma((blocks, 2, len(LATE_CUTS))),
                dma((blocks, 2, len(EARLY_CUTS))),
                dma((blocks, 2, len(EARLY_CUTS))),
                dma((steps,)),
                dma((steps,)),
                dma((len(OUT_CUTS),)),
            ],
            compiler_params=pltpu.CompilerParams(
                collective_id=0, has_side_effects=True, vmem_limit_bytes=60 * 1024 * 1024
            ),
        )(img, *raw)
        return out.reshape(count, rows // 2, half_w, LANES)

    act_spec = P("dp", "sp", None, None)
    return jax.shard_map(forward, mesh=mesh, in_specs=(act_spec,) + (P(),) * 10, out_specs=act_spec, check_vma=False)
```

```python
import functools

import jax
import jax.numpy as jnp
from jax import lax
from jax.experimental import pallas as pl
from jax.experimental.pallas import tpu as pltpu
from jax.sharding import PartitionSpec as P

NORM_EPS = 1e-5
MESH = pl.DeviceIdType.MESH
LANES = 128
IMG_CUTS = (5, 5, 4, 2)
LATE_CUTS = (5, 7, 3, 1)
EARLY_CUTS = (1, 4)
OUT_CUTS = (6, 6, 3, 1)
ROW_EARLY, MID_EARLY, OF_PAIRS = 0, 0, 16
F32 = jnp.float32
BF16 = jnp.bfloat16


def cuts(first, last, weights):
    total, seen, edge, spans = sum(weights), 0, first, []
    for weight in weights:
        seen += weight
        end = first + (last - first) * seen // total
        if end > edge:
            spans.append((edge, end - edge))
        edge = end
    return spans


def over(span, body, carry=0, step=1):
    start, length = span
    trips = length // step

    def trip(i, carry):
        for k in range(step):
            carry = body(start + i * step + k, carry)
        return carry

    if trips == 1:
        carry = trip(0, carry)
    elif trips > 1:
        carry = lax.fori_loop(0, trips, trip, carry)
    for q in range(start + trips * step, start + length):
        carry = body(q, carry)
    return carry


def placement(size, copies):
    row = lax.broadcasted_iota(jnp.int32, (size, copies * LANES), 0)
    lane = lax.broadcasted_iota(jnp.int32, (size, copies * LANES), 1)
    hit = lane == row
    for i in range(1, copies):
        hit = jnp.logical_or(hit, lane == row + i * (LANES + size))
    return hit.astype(F32).astype(BF16)


def expand_stage_a(w, own_ref, halo_ref):
    spread = jnp.dot(w, placement(32, 4), preferred_element_type=F32)
    own_ref[...] = jnp.zeros_like(own_ref)
    halo_ref[...] = jnp.zeros_like(halo_ref)
    for ref, halo in ((own_ref, False), (halo_ref, True)):
        for pi in range(2):
            for ri in range(2):
                for shift in range(2):
                    total = jnp.zeros((32, LANES), F32)
                    for ro in range(2):
                        for po in range(2):
                            if halo and ri != ro:
                                continue
                            if shift and pi == po:
                                continue
                            ky = 2 * ri if halo else ri - ro + 1
                            kx = (0 if pi == 1 else 2) if shift else pi - po + 1
                            tap, i = ky * 3 + kx, ro * 2 + po
                            total += spread[tap * 32:(tap + 1) * 32, i * LANES:(i + 1) * LANES]
                    block = total.astype(BF16)
                    for a in range(2):
                        row, col = ((pi * 2 + a) * 2 + ri) * 32, (shift * 2 + a) * LANES
                        ref[row:row + 32, col:col + LANES] = block


def expand_down(w_ref, own_ref, halo_ref):
    own_ref[...] = jnp.zeros_like(own_ref)
    halo_ref[...] = jnp.zeros_like(halo_ref)
    for par in range(2):
        for shift in range(2 - par):
            kx = 2 if shift else par
            for row in range(2):
                at = (row * 2 + par) * 32
                own_ref[at:at + 32, shift * LANES:(shift + 1) * LANES] = w_ref[row * 3 + kx]
            for a in range(2):
                at, col = (a * 2 + par) * 32, (a * 2 + shift) * LANES
                halo_ref[at:at + 32, col:col + LANES] = w_ref[6 + kx]


def expand_blocks(w_in_ref, w_mid_ref, w_out_ref, win_ref, wmid_ref, wout_ref):
    spot = placement(64, 2)
    for j in range(win_ref.shape[0]):
        w_in = w_in_ref[j].astype(F32).T.astype(BF16)
        spread = jnp.dot(w_in, spot, preferred_element_type=F32).astype(BF16)
        for a in range(2):
            win_ref[j, a * LANES:(a + 1) * LANES, :] = spread[:, a * LANES:(a + 1) * LANES]
        for src, ky in enumerate((1, 0, 2)):
            for kx in range(3):
                spread = jnp.dot(w_mid_ref[j, ky * 3 + kx], spot, preferred_element_type=F32).astype(BF16)
                for a in range(2):
                    at = (src * 2 + a) * 64
                    wmid_ref[j, at:at + 64, kx * LANES:(kx + 1) * LANES] = spread[:, a * LANES:(a + 1) * LANES]
        zeros = jnp.zeros((64, LANES), BF16)
        for a in range(2):
            for b in range(2):
                wout_ref[j, a * 64:(a + 1) * 64, b * LANES:(b + 1) * LANES] = w_out_ref[j] if a == b else zeros


def kernel(
    n, img_hbm, wa_hbm, wd_hbm, wi_hbm, wm_hbm, wo_hbm, ba_hbm, bd_hbm, bi_hbm, bm_hbm, bo_hbm, out_hbm,
    wa_raw, wd_raw, wi_raw, wm_raw, wo_raw, ba_raw, bd_raw, bi_raw, bm_raw, bo_raw, w_sem,
    wao_ref, wah_ref, wdo_ref, wdh_ref, win_ref, wmid_ref, wout_ref, bn_ref,
    ximg, xabove, xbelow, tscr, za, rsend, rrecv, zrow, zrow_in, zd, h, zi, u2, habove, hbelow, zabove, zbelow,
    zm, zo, stats, recv,
    img_sem, isend_sem, irecv_sem, rsend_sem, rrecv_sem, zsend_sem, zrecv_sem, hsend_sem, hrecv_sem,
    esend_sem, erecv_sem, ssem, rsem, out_sem,
):
    me = lax.axis_index("sp")
    nxt, prv = me + 1, me - 1
    has_next, has_prev = me < n - 1, me > 0
    pairs = ximg.shape[1]
    half_w = tscr.shape[0] // 2
    full_w = tscr.shape[0]
    count_a = float(2 * pairs * 2 * full_w * n)
    count_b = float(2 * pairs * half_w * n)
    everything = (0, pairs)

    img_load = cuts(0, pairs, (4, 4, 4, 4))
    img_spans = cuts(0, pairs, IMG_CUTS)
    row_early, mid_early = zrow.shape[0], zabove.shape[1]
    row_spans = cuts(row_early, pairs, LATE_CUTS)
    mid_spans = cuts(mid_early, pairs, LATE_CUTS)
    early_spans = cuts(0, mid_early, EARLY_CUTS)
    out_spans = cuts(0, pairs, OUT_CUTS)

    params = [
        pltpu.make_async_copy(src, dst, w_sem.at[i])
        for i, (src, dst) in enumerate((
            (wa_hbm, wa_raw), (wd_hbm, wd_raw), (wi_hbm, wi_raw), (wm_hbm, wm_raw), (wo_hbm, wo_raw),
            (ba_hbm, ba_raw), (bd_hbm, bd_raw), (bi_hbm, bi_raw), (bm_hbm, bm_raw), (bo_hbm, bo_raw),
        ))
    ]
    local_img = [
        pltpu.make_async_copy(img_hbm.at[:, pl.ds(*span)], ximg.at[:, pl.ds(*span)], img_sem.at[c])
        for c, span in enumerate(img_load)
    ]
    barrier = pltpu.get_barrier_semaphore()
    for d in range(1, n):
        pl.semaphore_signal(barrier, inc=1, device_id={"sp": lax.rem(me + d, n)}, device_id_type=MESH)
    params[0].start()
    for copy in local_img:
        copy.start()
    for copy in params[1:]:
        copy.start()

    @pl.when(me == n - 1)
    def _():
        xbelow[...] = jnp.zeros_like(xbelow)
        rrecv[...] = jnp.zeros_like(rrecv)
        hbelow[...] = jnp.zeros_like(hbelow)

    @pl.when(me == 0)
    def _():
        xabove[...] = jnp.zeros_like(xabove)
        habove[...] = jnp.zeros_like(habove)

    pl.semaphore_wait(barrier, n - 1)

    def to_dev(src, dst, send_sem, recv_sem, dev):
        return pltpu.make_async_remote_copy(
            src_ref=src, dst_ref=dst, send_sem=send_sem, recv_sem=recv_sem, device_id={"sp": dev}, device_id_type=MESH
        )

    def img_down(c):
        part = pl.ds(*img_spans[c])
        return to_dev(img_hbm.at[:, part, 1], xabove.at[:, part], isend_sem.at[0, c], irecv_sem.at[0, c], nxt)

    def img_up(c):
        part = pl.ds(*img_spans[c])
        return to_dev(img_hbm.at[:, part, 0], xbelow.at[:, part], isend_sem.at[1, c], irecv_sem.at[1, c], prv)

    def exchange(down, up, c):
        @pl.when(has_next)
        def _():
            down(c).start()

        @pl.when(has_prev)
        def _():
            up(c).start()

    def arrived(down, up, c):
        @pl.when(has_prev)
        def _():
            down(c).wait_recv()

        @pl.when(has_next)
        def _():
            up(c).wait_recv()

    for c in range(len(img_spans)):
        exchange(img_down, img_up, c)

    params[0].wait()
    expand_stage_a(wa_raw[...], wao_ref, wah_ref)

    def shift_down(y):
        row = lax.broadcasted_iota(jnp.int32, y.shape, 0)
        return jnp.where(row == 0, 0.0, pltpu.roll(y, 1, 0))

    def shift_up(y):
        row = lax.broadcasted_iota(jnp.int32, y.shape, 0)
        return jnp.where(row == y.shape[0] - 1, 0.0, pltpu.roll(y, y.shape[0] - 1, 0))

    def add_stats(acc, z):
        blocks = z.reshape(z.shape[0] // 8, 8, LANES)
        return acc[0] + jnp.sum(blocks, axis=0), acc[1] + jnp.sum(blocks * blocks, axis=0)

    zero_acc = (jnp.zeros((8, LANES), F32), jnp.zeros((8, LANES), F32))

    def group_stats(k, acc, group, meanwhile=None):
        def fold(v):
            width = group
            while width < LANES:
                v = v + pltpu.roll(v, width, 1)
                width *= 2
            return jnp.sum(v, axis=0, keepdims=True)

        mine = jnp.concatenate([fold(acc[0]), fold(acc[1])], axis=0)
        stats[k] = mine
        for d in sorted(range(1, n), key=lambda d: abs(2 * d - n)):
            to_dev(stats.at[k], recv.at[k, d - 1], ssem.at[k], rsem.at[k], lax.rem(me + d, n)).start()
        if meanwhile is not None:
            meanwhile()
        to_dev(recv.at[k], recv.at[k], ssem.at[k], rsem.at[k], me).wait_recv()
        return mine + jnp.sum(recv[k], axis=0)

    def norm_of(k, total, count):
        moments = total * (1.0 / count)
        mean = moments[0:1]
        var = moments[1:2] - mean * mean
        scale = bn_ref[k, 0:1] * lax.rsqrt(var + NORM_EPS)
        return mean, scale, bn_ref[k, 1:2]

    def bn(z, norm):
        mean, scale, shift = norm
        return (z - mean) * scale + shift

    lane2 = lax.broadcasted_iota(jnp.int32, (half_w, 2 * LANES), 1)
    even_lane = lax.rem(lane2 // 32, 2) == 0

    def stage_a_part(x, w_ref):
        tscr[...] = x.astype(F32).T
        lhs = jnp.concatenate(
            [tscr[pl.ds(0, half_w, stride=2), :], tscr[pl.ds(1, half_w, stride=2), :]], axis=1
        ).astype(BF16)
        y = jnp.dot(lhs, w_ref[...], preferred_element_type=F32)
        cross = y[:, 2 * LANES:]
        return y[:, : 2 * LANES] + jnp.where(even_lane, shift_down(cross), shift_up(cross))

    def own_a(q, carry):
        x = jnp.concatenate([ximg[0, q].reshape(2 * 32, full_w), ximg[1, q].reshape(2 * 32, full_w)], axis=0)
        z = stage_a_part(x, wao_ref)
        za[0, q] = z[:, :LANES]
        za[1, q] = z[:, LANES:]
        return carry

    for c, span in enumerate(img_load):
        local_img[c].wait()
        over(span, own_a)

    for copy in params[1:]:
        copy.wait()
    expand_down(wd_raw, wdo_ref, wdh_ref)
    expand_blocks(wi_raw, wm_raw, wo_raw, win_ref, wmid_ref, wout_ref)
    bn_ref[0] = jnp.concatenate([ba_raw[0]] * 4, axis=1)
    bn_ref[1] = bd_raw[...]
    for j in range(wi_raw.shape[0]):
        bn_ref[2 + 3 * j] = jnp.concatenate([bi_raw[j]] * 2, axis=1)
        bn_ref[3 + 3 * j] = jnp.concatenate([bm_raw[j]] * 2, axis=1)
        bn_ref[4 + 3 * j] = bo_raw[j]

    def halo_a(q, acc):
        x = jnp.concatenate([xabove[0, q], xbelow[0, q], xabove[1, q], xbelow[1, q]], axis=0)
        z = stage_a_part(x, wah_ref)
        z0 = za[0, q] + z[:, :LANES]
        z1 = za[1, q] + z[:, LANES:]
        za[0, q] = z0
        za[1, q] = z1
        return add_stats(add_stats(acc, z0), z1)

    acc = zero_acc
    for c, span in enumerate(img_spans):
        arrived(img_down, img_up, c)
        acc = over(span, halo_a, acc)

    lane1 = lax.broadcasted_iota(jnp.int32, (half_w, LANES), 1)
    low_lane = lane1 < 64

    def row_up(c):
        part = pl.ds(*row_spans[c])
        return to_dev(rsend.at[part], rrecv.at[part], rsend_sem.at[c], rrecv_sem.at[c], prv)

    def early_row_up():
        return to_dev(zrow, zrow_in, zsend_sem, zrecv_sem, prv)

    def first_rows(t0, t1):
        return jnp.where(low_lane, t0, pltpu.roll(t1, 64, 1))

    def send_early_rows():
        def pack(q, carry):
            zrow[q] = first_rows(za[0, q], za[1, q])
            return carry

        over((0, row_early), pack)

        @pl.when(has_prev)
        def _():
            early_row_up().start()

    norm = norm_of(0, group_stats(0, acc, 32, send_early_rows if row_early else None), count_a)

    def pack_row(q, carry):
        rsend[q] = jnp.maximum(bn(first_rows(za[0, q], za[1, q]), norm), 0.0).astype(BF16)
        return carry

    for c, span in enumerate(row_spans):
        over(span, pack_row)

        @pl.when(has_prev)
        def _():
            row_up(c).start()

    def own_down(q, carry):
        for a in range(2):
            t = jnp.maximum(bn(za[a, q], norm), 0.0).astype(BF16)
            y = jnp.dot(t, wdo_ref[...], preferred_element_type=F32)
            zd[a, q] = y[:, :LANES] + shift_up(y[:, LANES:])
        return carry

    over(everything, own_down)

    if row_early:
        @pl.when(has_next)
        def _():
            early_row_up().wait_recv()

            def norm_row(q, carry):
                rrecv[q] = jnp.maximum(bn(zrow_in[q], norm), 0.0).astype(BF16)
                return carry

            over((0, row_early), norm_row)

    def halo_down(q, acc):
        y = jnp.dot(rrecv[q], wdh_ref[...], preferred_element_type=F32)
        for a in range(2):
            lo = 2 * a * LANES
            z = zd[a, q] + y[:, lo:lo + LANES] + shift_up(y[:, lo + LANES:lo + 2 * LANES])
            zd[a, q] = z
            acc = add_stats(acc, z)
        return acc

    acc = over((0, row_early), halo_down, zero_acc) if row_early else zero_acc
    for c, span in enumerate(row_spans):
        @pl.when(has_next)
        def _():
            row_up(c).wait_recv()

        acc = over(span, halo_down, acc)
    norm = norm_of(1, group_stats(1, acc, LANES), count_b)

    blocks = win_ref.shape[0]

    def mid_down(j):
        def copy(c):
            part = pl.ds(*mid_spans[c])
            return to_dev(u2.at[j, part], habove.at[j, part], hsend_sem.at[j, 0, c], hrecv_sem.at[j, 0, c], nxt)
        return copy

    def mid_up(j):
        def copy(c):
            part = pl.ds(*mid_spans[c])
            return to_dev(u2.at[j, part], hbelow.at[j, part], hsend_sem.at[j, 1, c], hrecv_sem.at[j, 1, c], prv)
        return copy

    def early_down(j):
        def copy(c):
            part = pl.ds(*early_spans[c])
            return to_dev(zi.at[j, part], zabove.at[j, part], esend_sem.at[j, 0, c], erecv_sem.at[j, 0, c], nxt)
        return copy

    def early_up(j):
        def copy(c):
            part = pl.ds(*early_spans[c])
            return to_dev(zi.at[j, part], zbelow.at[j, part], esend_sem.at[j, 1, c], erecv_sem.at[j, 1, c], prv)
        return copy

    for j in range(blocks):
        def layer_in(q, acc):
            parts = []
            for a in range(2):
                if j == 0:
                    t = bn(zd[a, q], norm)
                else:
                    t = bn(zo[a, q], norm) + h[a, q].astype(F32)
                t = jnp.maximum(t, 0.0).astype(BF16)
                h[a, q] = t
                parts.append(t)
            z = jnp.dot(jnp.concatenate(parts, axis=1), win_ref[j], preferred_element_type=F32)
            zi[j, q] = z
            return add_stats(acc, z)

        acc, done = zero_acc, 0
        if early_spans:
            done = early_spans[0][1]
            acc = over(early_spans[0], layer_in, acc)
            exchange(early_down(j), early_up(j), 0)
        acc = over((done, pairs - done), layer_in, acc, 2)

        def send_early():
            for c in range(1, len(early_spans)):
                exchange(early_down(j), early_up(j), c)

        norm = norm_of(2 + 3 * j, group_stats(2 + 3 * j, acc, 64, send_early), count_b)

        def act_in(q, carry):
            u2[j, q] = jnp.maximum(bn(zi[j, q], norm), 0.0).astype(BF16)
            return carry

        for c, span in enumerate(mid_spans):
            over(span, act_in)
            exchange(mid_down(j), mid_up(j), c)
        over((0, mid_early), act_in)

        if early_spans:
            for c in range(len(early_spans)):
                arrived(early_down(j), early_up(j), c)

            def act_above(q, carry):
                habove[j, q] = jnp.maximum(bn(zabove[j, q], norm), 0.0).astype(BF16)
                return carry

            def act_below(q, carry):
                hbelow[j, q] = jnp.maximum(bn(zbelow[j, q], norm), 0.0).astype(BF16)
                return carry

            @pl.when(has_prev)
            def _():
                over((0, mid_early), act_above)

            @pl.when(has_next)
            def _():
                over((0, mid_early), act_below)

        def layer_mid(q, acc):
            lhs = jnp.concatenate([u2[j, q], habove[j, q], hbelow[j, q]], axis=1)
            y = jnp.dot(lhs, wmid_ref[j], preferred_element_type=F32)
            z = shift_down(y[:, :LANES]) + y[:, LANES:2 * LANES] + shift_up(y[:, 2 * LANES:])
            zm[q] = z
            return add_stats(acc, z)

        acc = over((0, mid_early), layer_mid, zero_acc)
        for c, span in enumerate(mid_spans):
            arrived(mid_down(j), mid_up(j), c)
            acc = over(span, layer_mid, acc)
        norm = norm_of(3 + 3 * j, group_stats(3 + 3 * j, acc, 64), count_b)

        def layer_out(q, acc):
            u = jnp.maximum(bn(zm[q], norm), 0.0).astype(BF16)
            y = jnp.dot(u, wout_ref[j], preferred_element_type=F32)
            for a in range(2):
                z = y[:, a * LANES:(a + 1) * LANES]
                zo[a, q] = z
                acc = add_stats(acc, z)
            return acc

        acc = over(everything, layer_out, zero_acc, 2)
        norm = norm_of(4 + 3 * j, group_stats(4 + 3 * j, acc, LANES), count_b)

    def store(c):
        part = pl.ds(*out_spans[c])
        return pltpu.make_async_copy(h.at[:, part], out_hbm.at[:, part], out_sem.at[c])

    def final(q, carry):
        for a in range(2):
            h[a, q] = jnp.maximum(bn(zo[a, q], norm) + h[a, q].astype(F32), 0.0).astype(BF16)
        return carry

    for c, span in enumerate(out_spans):
        over(span, final)
        store(c).start()

    for k in range(stats.shape[0]):
        to_dev(recv.at[k], recv.at[k], ssem.at[k], rsem.at[k], me).wait_send()

    @pl.when(has_next)
    def _():
        for c in range(len(img_spans)):
            img_down(c).wait_send()
        for j in range(blocks):
            for c in range(len(mid_spans)):
                mid_down(j)(c).wait_send()
            for c in range(len(early_spans)):
                early_down(j)(c).wait_send()

    @pl.when(has_prev)
    def _():
        for c in range(len(img_spans)):
            img_up(c).wait_send()
        for c in range(len(row_spans)):
            row_up(c).wait_send()
        if row_early:
            early_row_up().wait_send()
        for j in range(blocks):
            for c in range(len(mid_spans)):
                mid_up(j)(c).wait_send()
            for c in range(len(early_spans)):
                early_up(j)(c).wait_send()

    for c in range(len(out_spans)):
        store(c).wait()


def solution(mesh):
    n = mesh.shape["sp"]

    def forward(images, w_a, bn_a, w_down, bn_down, w_in, bn_in, w_mid, bn_mid, w_out, bn_out):
        count, rows, width, chan_a = images.shape
        pairs, half_w = count // 2, width // 2
        blocks = w_in.shape[0]
        row_early, mid_early = pairs * ROW_EARLY // OF_PAIRS, pairs * MID_EARLY // OF_PAIRS
        img = jnp.transpose(images, (0, 1, 3, 2)).reshape(2, pairs, rows, chan_a, width)
        taps = w_a.shape[1] * w_a.shape[2]
        raw = [
            w_a.reshape(taps * chan_a, chan_a), w_down.reshape(taps, chan_a, LANES), jnp.transpose(w_in, (0, 2, 1)),
            w_mid.reshape(blocks, taps, 64, 64), w_out, bn_a, bn_down, bn_in, bn_mid, bn_out,
        ]
        steps = 2 + 3 * blocks

        anyspace = pl.BlockSpec(memory_space=pl.ANY)
        dma = pltpu.SemaphoreType.DMA
        out = pl.pallas_call(
            functools.partial(kernel, n),
            out_shape=jax.ShapeDtypeStruct((2, pairs, half_w, LANES), BF16),
            in_specs=[pl.BlockSpec(memory_space=pltpu.HBM)] * 11,
            out_specs=anyspace,
            scratch_shapes=[pltpu.VMEM(x.shape, x.dtype) for x in raw] + [
                dma((len(raw),)),
                pltpu.VMEM((2 * LANES, 4 * LANES), BF16),
                pltpu.VMEM((2 * LANES, 4 * LANES), BF16),
                pltpu.VMEM((LANES, 2 * LANES), BF16),
                pltpu.VMEM((LANES, 4 * LANES), BF16),
                pltpu.VMEM((blocks, 2 * LANES, LANES), BF16),
                pltpu.VMEM((blocks, 3 * LANES, 3 * LANES), BF16),
                pltpu.VMEM((blocks, LANES, 2 * LANES), BF16),
                pltpu.VMEM((steps, 2, LANES), F32),
                pltpu.VMEM((2, pairs, rows, chan_a, width), BF16),
                pltpu.VMEM((2, pairs, chan_a, width), BF16),
                pltpu.VMEM((2, pairs, chan_a, width), BF16),
                pltpu.VMEM((width, LANES), F32),
                pltpu.VMEM((2, pairs, half_w, LANES), F32),
                pltpu.VMEM((pairs, half_w, LANES), BF16),
                pltpu.VMEM((pairs, half_w, LANES), BF16),
                pltpu.VMEM((row_early, half_w, LANES), F32),
                pltpu.VMEM((row_early, half_w, LANES), F32),
                pltpu.VMEM((2, pairs, half_w, LANES), F32),
                pltpu.VMEM((2, pairs, half_w, LANES), BF16),
                pltpu.VMEM((blocks, pairs, half_w, LANES), F32),
                pltpu.VMEM((blocks, pairs, half_w, LANES), BF16),
                pltpu.VMEM((blocks, pairs, half_w, LANES), BF16),
                pltpu.VMEM((blocks, pairs, half_w, LANES), BF16),
                pltpu.VMEM((blocks, mid_early, half_w, LANES), F32),
                pltpu.VMEM((blocks, mid_early, half_w, LANES), F32),
                pltpu.VMEM((pairs, half_w, LANES), F32),
                pltpu.VMEM((2, pairs, half_w, LANES), F32),
                pltpu.VMEM((steps, 2, LANES), F32),
                pltpu.VMEM((steps, n - 1, 2, LANES), F32),
                dma((4,)),
                dma((2, len(IMG_CUTS))),
                dma((2, len(IMG_CUTS))),
                dma((len(LATE_CUTS),)),
                dma((len(LATE_CUTS),)),
                dma,
                dma,
                dma((blocks, 2, len(LATE_CUTS))),
                dma((blocks, 2, len(LATE_CUTS))),
                dma((blocks, 2, len(EARLY_CUTS))),
                dma((blocks, 2, len(EARLY_CUTS))),
                dma((steps,)),
                dma((steps,)),
                dma((len(OUT_CUTS),)),
            ],
            compiler_params=pltpu.CompilerParams(
                collective_id=0, has_side_effects=True, vmem_limit_bytes=60 * 1024 * 1024
            ),
        )(img, *raw)
        return out.reshape(count, rows // 2, half_w, LANES)

    act_spec = P("dp", "sp", None, None)
    return jax.shard_map(forward, mesh=mesh, in_specs=(act_spec,) + (P(),) * 10, out_specs=act_spec, check_vma=False)
```

```python
import functools

import jax
import jax.numpy as jnp
from jax import lax
from jax.experimental import pallas as pl
from jax.experimental.pallas import tpu as pltpu
from jax.sharding import PartitionSpec as P

NORM_EPS = 1e-5
MESH = pl.DeviceIdType.MESH
LANES = 128
IMG_CUTS = (5, 5, 4, 2)
LATE_CUTS = (5, 7, 3, 1)
F32 = jnp.float32
BF16 = jnp.bfloat16


def cuts(first, last, weights):
    total, seen, edge, spans = sum(weights), 0, first, []
    for weight in weights:
        seen += weight
        end = first + (last - first) * seen // total
        if end > edge:
            spans.append((edge, end - edge))
        edge = end
    return spans


def over(span, body, carry=0, step=1):
    start, length = span
    trips = length // step

    def trip(i, carry):
        for k in range(step):
            carry = body(start + i * step + k, carry)
        return carry

    if trips == 1:
        carry = trip(0, carry)
    elif trips > 1:
        carry = lax.fori_loop(0, trips, trip, carry)
    for q in range(start + trips * step, start + length):
        carry = body(q, carry)
    return carry


def placement(size, copies):
    row = lax.broadcasted_iota(jnp.int32, (size, copies * LANES), 0)
    lane = lax.broadcasted_iota(jnp.int32, (size, copies * LANES), 1)
    hit = lane == row
    for i in range(1, copies):
        hit = jnp.logical_or(hit, lane == row + i * (LANES + size))
    return hit.astype(F32).astype(BF16)


def expand_stage_a(w, own_ref, halo_ref):
    spread = jnp.dot(w, placement(32, 4), preferred_element_type=F32)
    own_ref[...] = jnp.zeros_like(own_ref)
    halo_ref[...] = jnp.zeros_like(halo_ref)
    for ref, halo in ((own_ref, False), (halo_ref, True)):
        for pi in range(2):
            for ri in range(2):
                for shift in range(2):
                    total = jnp.zeros((32, LANES), F32)
                    for ro in range(2):
                        for po in range(2):
                            if halo and ri != ro:
                                continue
                            if shift and pi == po:
                                continue
                            ky = 2 * ri if halo else ri - ro + 1
                            kx = (0 if pi == 1 else 2) if shift else pi - po + 1
                            tap, i = ky * 3 + kx, ro * 2 + po
                            total += spread[tap * 32:(tap + 1) * 32, i * LANES:(i + 1) * LANES]
                    block = total.astype(BF16)
                    for a in range(2):
                        row, col = ((pi * 2 + a) * 2 + ri) * 32, (shift * 2 + a) * LANES
                        ref[row:row + 32, col:col + LANES] = block


def expand_down(w_ref, own_ref, halo_ref):
    own_ref[...] = jnp.zeros_like(own_ref)
    halo_ref[...] = jnp.zeros_like(halo_ref)
    for par in range(2):
        for shift in range(2 - par):
            kx = 2 if shift else par
            for row in range(2):
                at = (row * 2 + par) * 32
                own_ref[at:at + 32, shift * LANES:(shift + 1) * LANES] = w_ref[row * 3 + kx]
            for a in range(2):
                at, col = (a * 2 + par) * 32, (a * 2 + shift) * LANES
                halo_ref[at:at + 32, col:col + LANES] = w_ref[6 + kx]


def expand_blocks(w_in_ref, w_mid_ref, w_out_ref, win_ref, wmid_ref, wout_ref):
    spot = placement(64, 2)
    for j in range(win_ref.shape[0]):
        w_in = w_in_ref[j].astype(F32).T.astype(BF16)
        spread = jnp.dot(w_in, spot, preferred_element_type=F32).astype(BF16)
        for a in range(2):
            win_ref[j, a * LANES:(a + 1) * LANES, :] = spread[:, a * LANES:(a + 1) * LANES]
        for src, ky in enumerate((1, 0, 2)):
            for kx in range(3):
                spread = jnp.dot(w_mid_ref[j, ky * 3 + kx], spot, preferred_element_type=F32).astype(BF16)
                for a in range(2):
                    at = (src * 2 + a) * 64
                    wmid_ref[j, at:at + 64, kx * LANES:(kx + 1) * LANES] = spread[:, a * LANES:(a + 1) * LANES]
        zeros = jnp.zeros((64, LANES), BF16)
        for a in range(2):
            for b in range(2):
                wout_ref[j, a * 64:(a + 1) * 64, b * LANES:(b + 1) * LANES] = w_out_ref[j] if a == b else zeros


def kernel(
    n, img_hbm, wa_hbm, wd_hbm, wi_hbm, wm_hbm, wo_hbm, ba_hbm, bd_hbm, bi_hbm, bm_hbm, bo_hbm, out_ref,
    wa_raw, wd_raw, wi_raw, wm_raw, wo_raw, ba_raw, bd_raw, bi_raw, bm_raw, bo_raw, w_sem,
    wao_ref, wah_ref, wdo_ref, wdh_ref, win_ref, wmid_ref, wout_ref, bn_ref,
    ximg, xabove, xbelow, tscr, za, rsend, rrecv, zd, h, zi, u2, habove, hbelow,
    zm, zo, stats, recv,
    img_sem, isend_sem, irecv_sem, rsend_sem, rrecv_sem, hsend_sem, hrecv_sem,
    ssem, rsem,
):
    me = lax.axis_index("sp")
    nxt, prv = me + 1, me - 1
    has_next, has_prev = me < n - 1, me > 0
    pairs = ximg.shape[1]
    half_w = tscr.shape[0] // 2
    full_w = tscr.shape[0]
    count_a = float(2 * pairs * 2 * full_w * n)
    count_b = float(2 * pairs * half_w * n)
    everything = (0, pairs)

    img_load = cuts(0, pairs, (4, 4, 4, 4))
    img_spans = cuts(0, pairs, IMG_CUTS)
    row_spans = cuts(0, pairs, LATE_CUTS)
    mid_spans = cuts(0, pairs, LATE_CUTS)

    params = [
        pltpu.make_async_copy(src, dst, w_sem.at[i])
        for i, (src, dst) in enumerate((
            (wa_hbm, wa_raw), (wd_hbm, wd_raw), (wi_hbm, wi_raw), (wm_hbm, wm_raw), (wo_hbm, wo_raw),
            (ba_hbm, ba_raw), (bd_hbm, bd_raw), (bi_hbm, bi_raw), (bm_hbm, bm_raw), (bo_hbm, bo_raw),
        ))
    ]
    local_img = [
        pltpu.make_async_copy(img_hbm.at[:, pl.ds(*span)], ximg.at[:, pl.ds(*span)], img_sem.at[c])
        for c, span in enumerate(img_load)
    ]
    barrier = pltpu.get_barrier_semaphore()
    for d in range(1, n):
        pl.semaphore_signal(barrier, inc=1, device_id={"sp": lax.rem(me + d, n)}, device_id_type=MESH)
    params[0].start()
    for copy in local_img:
        copy.start()
    for copy in params[1:]:
        copy.start()

    @pl.when(me == n - 1)
    def _():
        xbelow[...] = jnp.zeros_like(xbelow)
        rrecv[...] = jnp.zeros_like(rrecv)
        hbelow[...] = jnp.zeros_like(hbelow)

    @pl.when(me == 0)
    def _():
        xabove[...] = jnp.zeros_like(xabove)
        habove[...] = jnp.zeros_like(habove)

    pl.semaphore_wait(barrier, n - 1)

    def to_dev(src, dst, send_sem, recv_sem, dev):
        return pltpu.make_async_remote_copy(
            src_ref=src, dst_ref=dst, send_sem=send_sem, recv_sem=recv_sem, device_id={"sp": dev}, device_id_type=MESH
        )

    def img_down(c):
        part = pl.ds(*img_spans[c])
        return to_dev(img_hbm.at[:, part, 1], xabove.at[:, part], isend_sem.at[0, c], irecv_sem.at[0, c], nxt)

    def img_up(c):
        part = pl.ds(*img_spans[c])
        return to_dev(img_hbm.at[:, part, 0], xbelow.at[:, part], isend_sem.at[1, c], irecv_sem.at[1, c], prv)

    def exchange(down, up, c):
        @pl.when(has_next)
        def _():
            down(c).start()

        @pl.when(has_prev)
        def _():
            up(c).start()

    def arrived(down, up, c):
        @pl.when(has_prev)
        def _():
            down(c).wait_recv()

        @pl.when(has_next)
        def _():
            up(c).wait_recv()

    for c in range(len(img_spans)):
        exchange(img_down, img_up, c)

    params[0].wait()
    expand_stage_a(wa_raw[...], wao_ref, wah_ref)

    def shift_down(y):
        row = lax.broadcasted_iota(jnp.int32, y.shape, 0)
        return jnp.where(row == 0, 0.0, pltpu.roll(y, 1, 0))

    def shift_up(y):
        row = lax.broadcasted_iota(jnp.int32, y.shape, 0)
        return jnp.where(row == y.shape[0] - 1, 0.0, pltpu.roll(y, y.shape[0] - 1, 0))

    def add_stats(acc, z):
        blocks = z.reshape(z.shape[0] // 8, 8, LANES)
        return acc[0] + jnp.sum(blocks, axis=0), acc[1] + jnp.sum(blocks * blocks, axis=0)

    zero_acc = (jnp.zeros((8, LANES), F32), jnp.zeros((8, LANES), F32))

    def group_stats(k, acc, group):
        def fold(v):
            width = group
            while width < LANES:
                v = v + pltpu.roll(v, width, 1)
                width *= 2
            return jnp.sum(v, axis=0, keepdims=True)

        mine = jnp.concatenate([fold(acc[0]), fold(acc[1])], axis=0)
        stats[k] = mine
        for d in sorted(range(1, n), key=lambda d: abs(2 * d - n)):
            to_dev(stats.at[k], recv.at[k, d - 1], ssem.at[k], rsem.at[k], lax.rem(me + d, n)).start()
        to_dev(recv.at[k], recv.at[k], ssem.at[k], rsem.at[k], me).wait_recv()
        return mine + jnp.sum(recv[k], axis=0)

    def norm_of(k, total, count):
        moments = total * (1.0 / count)
        mean = moments[0:1]
        var = moments[1:2] - mean * mean
        scale = bn_ref[k, 0:1] * lax.rsqrt(var + NORM_EPS)
        return mean, scale, bn_ref[k, 1:2]

    def bn(z, norm):
        mean, scale, shift = norm
        return (z - mean) * scale + shift

    lane2 = lax.broadcasted_iota(jnp.int32, (half_w, 2 * LANES), 1)
    even_lane = lax.rem(lane2 // 32, 2) == 0

    def stage_a_part(x, w_ref):
        tscr[...] = x.astype(F32).T
        lhs = jnp.concatenate(
            [tscr[pl.ds(0, half_w, stride=2), :], tscr[pl.ds(1, half_w, stride=2), :]], axis=1
        ).astype(BF16)
        y = jnp.dot(lhs, w_ref[...], preferred_element_type=F32)
        cross = y[:, 2 * LANES:]
        return y[:, : 2 * LANES] + jnp.where(even_lane, shift_down(cross), shift_up(cross))

    def own_a(q, carry):
        x = jnp.concatenate([ximg[0, q].reshape(2 * 32, full_w), ximg[1, q].reshape(2 * 32, full_w)], axis=0)
        z = stage_a_part(x, wao_ref)
        za[0, q] = z[:, :LANES]
        za[1, q] = z[:, LANES:]
        return carry

    for c, span in enumerate(img_load):
        local_img[c].wait()
        over(span, own_a)

    for copy in params[1:]:
        copy.wait()
    expand_down(wd_raw, wdo_ref, wdh_ref)
    expand_blocks(wi_raw, wm_raw, wo_raw, win_ref, wmid_ref, wout_ref)
    bn_ref[0] = jnp.concatenate([ba_raw[0]] * 4, axis=1)
    bn_ref[1] = bd_raw[...]
    for j in range(wi_raw.shape[0]):
        bn_ref[2 + 3 * j] = jnp.concatenate([bi_raw[j]] * 2, axis=1)
        bn_ref[3 + 3 * j] = jnp.concatenate([bm_raw[j]] * 2, axis=1)
        bn_ref[4 + 3 * j] = bo_raw[j]

    def halo_a(q, acc):
        x = jnp.concatenate([xabove[0, q], xbelow[0, q], xabove[1, q], xbelow[1, q]], axis=0)
        z = stage_a_part(x, wah_ref)
        z0 = za[0, q] + z[:, :LANES]
        z1 = za[1, q] + z[:, LANES:]
        za[0, q] = z0
        za[1, q] = z1
        return add_stats(add_stats(acc, z0), z1)

    acc = zero_acc
    for c, span in enumerate(img_spans):
        arrived(img_down, img_up, c)
        acc = over(span, halo_a, acc)

    lane1 = lax.broadcasted_iota(jnp.int32, (half_w, LANES), 1)
    low_lane = lane1 < 64

    def row_up(c):
        part = pl.ds(*row_spans[c])
        return to_dev(rsend.at[part], rrecv.at[part], rsend_sem.at[c], rrecv_sem.at[c], prv)

    def first_rows(t0, t1):
        return jnp.where(low_lane, t0, pltpu.roll(t1, 64, 1))

    norm = norm_of(0, group_stats(0, acc, 32), count_a)

    def pack_row(q, carry):
        rsend[q] = jnp.maximum(bn(first_rows(za[0, q], za[1, q]), norm), 0.0).astype(BF16)
        return carry

    for c, span in enumerate(row_spans):
        over(span, pack_row)

        @pl.when(has_prev)
        def _():
            row_up(c).start()

    def own_down(q, carry):
        for a in range(2):
            t = jnp.maximum(bn(za[a, q], norm), 0.0).astype(BF16)
            y = jnp.dot(t, wdo_ref[...], preferred_element_type=F32)
            zd[a, q] = y[:, :LANES] + shift_up(y[:, LANES:])
        return carry

    over(everything, own_down)

    def halo_down(q, acc):
        y = jnp.dot(rrecv[q], wdh_ref[...], preferred_element_type=F32)
        for a in range(2):
            lo = 2 * a * LANES
            z = zd[a, q] + y[:, lo:lo + LANES] + shift_up(y[:, lo + LANES:lo + 2 * LANES])
            zd[a, q] = z
            acc = add_stats(acc, z)
        return acc

    acc = zero_acc
    for c, span in enumerate(row_spans):
        @pl.when(has_next)
        def _():
            row_up(c).wait_recv()

        acc = over(span, halo_down, acc)
    norm = norm_of(1, group_stats(1, acc, LANES), count_b)

    blocks = win_ref.shape[0]

    def mid_down(j):
        def copy(c):
            part = pl.ds(*mid_spans[c])
            return to_dev(u2.at[j, part], habove.at[j, part], hsend_sem.at[j, 0, c], hrecv_sem.at[j, 0, c], nxt)
        return copy

    def mid_up(j):
        def copy(c):
            part = pl.ds(*mid_spans[c])
            return to_dev(u2.at[j, part], hbelow.at[j, part], hsend_sem.at[j, 1, c], hrecv_sem.at[j, 1, c], prv)
        return copy

    for j in range(blocks):
        def layer_in(q, acc):
            parts = []
            for a in range(2):
                if j == 0:
                    t = bn(zd[a, q], norm)
                else:
                    t = bn(zo[a, q], norm) + h[a, q].astype(F32)
                t = jnp.maximum(t, 0.0).astype(BF16)
                h[a, q] = t
                parts.append(t)
            z = jnp.dot(jnp.concatenate(parts, axis=1), win_ref[j], preferred_element_type=F32)
            zi[q] = z
            return add_stats(acc, z)

        acc = over(everything, layer_in, zero_acc, 4)
        norm = norm_of(2 + 3 * j, group_stats(2 + 3 * j, acc, 64), count_b)

        def act_in(q, carry):
            u2[j, q] = jnp.maximum(bn(zi[q], norm), 0.0).astype(BF16)
            return carry

        for c, span in enumerate(mid_spans):
            over(span, act_in)
            exchange(mid_down(j), mid_up(j), c)
        def layer_mid(q, acc):
            lhs = jnp.concatenate([u2[j, q], habove[j, q], hbelow[j, q]], axis=1)
            y = jnp.dot(lhs, wmid_ref[j], preferred_element_type=F32)
            z = shift_down(y[:, :LANES]) + y[:, LANES:2 * LANES] + shift_up(y[:, 2 * LANES:])
            zm[q] = z
            return add_stats(acc, z)

        acc = zero_acc
        for c, span in enumerate(mid_spans):
            arrived(mid_down(j), mid_up(j), c)
            acc = over(span, layer_mid, acc)
        norm = norm_of(3 + 3 * j, group_stats(3 + 3 * j, acc, 64), count_b)

        def layer_out(q, acc):
            u = jnp.maximum(bn(zm[q], norm), 0.0).astype(BF16)
            y = jnp.dot(u, wout_ref[j], preferred_element_type=F32)
            for a in range(2):
                z = y[:, a * LANES:(a + 1) * LANES]
                zo[a, q] = z
                acc = add_stats(acc, z)
            return acc

        acc = over(everything, layer_out, zero_acc, 4)
        norm = norm_of(4 + 3 * j, group_stats(4 + 3 * j, acc, LANES), count_b)

    def final(q, carry):
        for a in range(2):
            out_ref[a, q] = jnp.maximum(bn(zo[a, q], norm) + h[a, q].astype(F32), 0.0).astype(BF16)
        return carry

    over(everything, final, 0, 2)

    for k in range(stats.shape[0]):
        to_dev(recv.at[k], recv.at[k], ssem.at[k], rsem.at[k], me).wait_send()

    @pl.when(has_next)
    def _():
        for c in range(len(img_spans)):
            img_down(c).wait_send()
        for j in range(blocks):
            for c in range(len(mid_spans)):
                mid_down(j)(c).wait_send()

    @pl.when(has_prev)
    def _():
        for c in range(len(img_spans)):
            img_up(c).wait_send()
        for c in range(len(row_spans)):
            row_up(c).wait_send()
        for j in range(blocks):
            for c in range(len(mid_spans)):
                mid_up(j)(c).wait_send()


def solution(mesh):
    n = mesh.shape["sp"]

    def forward(images, w_a, bn_a, w_down, bn_down, w_in, bn_in, w_mid, bn_mid, w_out, bn_out):
        count, rows, width, chan_a = images.shape
        pairs, half_w = count // 2, width // 2
        blocks = w_in.shape[0]
        img = jnp.transpose(images, (0, 1, 3, 2)).reshape(2, pairs, rows, chan_a, width)
        taps = w_a.shape[1] * w_a.shape[2]
        raw = [
            w_a.reshape(taps * chan_a, chan_a), w_down.reshape(taps, chan_a, LANES), jnp.transpose(w_in, (0, 2, 1)),
            w_mid.reshape(blocks, taps, 64, 64), w_out, bn_a, bn_down, bn_in, bn_mid, bn_out,
        ]
        steps = 2 + 3 * blocks

        dma = pltpu.SemaphoreType.DMA
        out = pl.pallas_call(
            functools.partial(kernel, n),
            out_shape=pltpu.VMEM((2, pairs, half_w, LANES), BF16),
            in_specs=[pl.BlockSpec(memory_space=pltpu.HBM)] * 11,
            out_specs=pl.BlockSpec(memory_space=pltpu.VMEM),
            scratch_shapes=[pltpu.VMEM(x.shape, x.dtype) for x in raw] + [
                dma((len(raw),)),
                pltpu.VMEM((2 * LANES, 4 * LANES), BF16),
                pltpu.VMEM((2 * LANES, 4 * LANES), BF16),
                pltpu.VMEM((LANES, 2 * LANES), BF16),
                pltpu.VMEM((LANES, 4 * LANES), BF16),
                pltpu.VMEM((blocks, 2 * LANES, LANES), BF16),
                pltpu.VMEM((blocks, 3 * LANES, 3 * LANES), BF16),
                pltpu.VMEM((blocks, LANES, 2 * LANES), BF16),
                pltpu.VMEM((steps, 2, LANES), F32),
                pltpu.VMEM((2, pairs, rows, chan_a, width), BF16),
                pltpu.VMEM((2, pairs, chan_a, width), BF16),
                pltpu.VMEM((2, pairs, chan_a, width), BF16),
                pltpu.VMEM((width, LANES), F32),
                pltpu.VMEM((2, pairs, half_w, LANES), F32),
                pltpu.VMEM((pairs, half_w, LANES), BF16),
                pltpu.VMEM((pairs, half_w, LANES), BF16),
                pltpu.VMEM((2, pairs, half_w, LANES), F32),
                pltpu.VMEM((2, pairs, half_w, LANES), BF16),
                pltpu.VMEM((pairs, half_w, LANES), F32),
                pltpu.VMEM((blocks, pairs, half_w, LANES), BF16),
                pltpu.VMEM((blocks, pairs, half_w, LANES), BF16),
                pltpu.VMEM((blocks, pairs, half_w, LANES), BF16),
                pltpu.VMEM((pairs, half_w, LANES), F32),
                pltpu.VMEM((2, pairs, half_w, LANES), F32),
                pltpu.VMEM((steps, 2, LANES), F32),
                pltpu.VMEM((steps, n - 1, 2, LANES), F32),
                dma((4,)),
                dma((2, len(IMG_CUTS))),
                dma((2, len(IMG_CUTS))),
                dma((len(LATE_CUTS),)),
                dma((len(LATE_CUTS),)),
                dma((blocks, 2, len(LATE_CUTS))),
                dma((blocks, 2, len(LATE_CUTS))),
                dma((steps,)),
                dma((steps,)),
            ],
            compiler_params=pltpu.CompilerParams(
                collective_id=0, has_side_effects=True, vmem_limit_bytes=52 * 1024 * 1024
            ),
        )(img, *raw)
        return out.reshape(count, rows // 2, half_w, LANES)

    act_spec = P("dp", "sp", None, None)
    return jax.shard_map(forward, mesh=mesh, in_specs=(act_spec,) + (P(),) * 10, out_specs=act_spec, check_vma=False)
```

```python
import functools
import math

import jax
import jax.numpy as jnp
from jax import lax
from jax.experimental import pallas as pl
from jax.experimental.pallas import tpu as pltpu
from jax.sharding import PartitionSpec as P

NORM_EPS = 1e-5
MESH = pl.DeviceIdType.MESH
LANES = 128
IMG_CUTS = (5, 5, 4, 2)
LATE_CUTS = (5, 7, 3, 1)
F32 = jnp.float32
BF16 = jnp.bfloat16


def cuts(first, last, weights):
    total, seen, edge, spans = sum(weights), 0, first, []
    for weight in weights:
        seen += weight
        end = first + (last - first) * seen // total
        if end > edge:
            spans.append((edge, end - edge))
        edge = end
    return spans


def over(span, body, carry=0, step=1):
    start, length = span
    trips = length // step

    def trip(i, carry):
        for k in range(step):
            carry = body(start + i * step + k, carry)
        return carry

    if trips == 1:
        carry = trip(0, carry)
    elif trips > 1:
        carry = lax.fori_loop(0, trips, trip, carry)
    for q in range(start + trips * step, start + length):
        carry = body(q, carry)
    return carry


def far_first(n):
    side = max(1, math.isqrt(n // 2))

    def hops(d):
        x, y = d // 2 % side, d // (2 * side)
        return min(x, side - x) + min(y, abs(side - y))

    return sorted(range(1, n), key=lambda d: (-hops(d), d))


def placement(size, copies):
    row = lax.broadcasted_iota(jnp.int32, (size, copies * LANES), 0)
    lane = lax.broadcasted_iota(jnp.int32, (size, copies * LANES), 1)
    hit = lane == row
    for i in range(1, copies):
        hit = jnp.logical_or(hit, lane == row + i * (LANES + size))
    return hit.astype(F32).astype(BF16)


def expand_stage_a(w, own_ref, halo_ref):
    spread = jnp.dot(w, placement(32, 4), preferred_element_type=F32)
    own_ref[...] = jnp.zeros_like(own_ref)
    halo_ref[...] = jnp.zeros_like(halo_ref)
    for ref, halo in ((own_ref, False), (halo_ref, True)):
        for pi in range(2):
            for ri in range(2):
                for shift in range(2):
                    total = jnp.zeros((32, LANES), F32)
                    for ro in range(2):
                        for po in range(2):
                            if halo and ri != ro:
                                continue
                            if shift and pi == po:
                                continue
                            ky = 2 * ri if halo else ri - ro + 1
                            kx = (0 if pi == 1 else 2) if shift else pi - po + 1
                            tap, i = ky * 3 + kx, ro * 2 + po
                            total += spread[tap * 32:(tap + 1) * 32, i * LANES:(i + 1) * LANES]
                    block = total.astype(BF16)
                    for a in range(2):
                        row, col = ((pi * 2 + a) * 2 + ri) * 32, (shift * 2 + a) * LANES
                        ref[row:row + 32, col:col + LANES] = block


def expand_down(w_ref, own_ref, halo_ref):
    own_ref[...] = jnp.zeros_like(own_ref)
    halo_ref[...] = jnp.zeros_like(halo_ref)
    for par in range(2):
        for shift in range(2 - par):
            kx = 2 if shift else par
            for row in range(2):
                at = (row * 2 + par) * 32
                own_ref[at:at + 32, shift * LANES:(shift + 1) * LANES] = w_ref[row * 3 + kx]
            for a in range(2):
                at, col = (a * 2 + par) * 32, (a * 2 + shift) * LANES
                halo_ref[at:at + 32, col:col + LANES] = w_ref[6 + kx]


def expand_blocks(w_in_ref, w_mid_ref, w_out_ref, win_ref, wmid_ref, wout_ref):
    spot = placement(64, 2)
    for j in range(win_ref.shape[0]):
        w_in = w_in_ref[j].astype(F32).T.astype(BF16)
        spread = jnp.dot(w_in, spot, preferred_element_type=F32).astype(BF16)
        for a in range(2):
            win_ref[j, a * LANES:(a + 1) * LANES, :] = spread[:, a * LANES:(a + 1) * LANES]
        for src, ky in enumerate((1, 0, 2)):
            for kx in range(3):
                spread = jnp.dot(w_mid_ref[j, ky * 3 + kx], spot, preferred_element_type=F32).astype(BF16)
                for a in range(2):
                    at = (src * 2 + a) * 64
                    wmid_ref[j, at:at + 64, kx * LANES:(kx + 1) * LANES] = spread[:, a * LANES:(a + 1) * LANES]
        zeros = jnp.zeros((64, LANES), BF16)
        for a in range(2):
            for b in range(2):
                wout_ref[j, a * 64:(a + 1) * 64, b * LANES:(b + 1) * LANES] = w_out_ref[j] if a == b else zeros


def kernel(
    n, img_hbm, wa_hbm, wd_hbm, wi_hbm, wm_hbm, wo_hbm, ba_hbm, bd_hbm, bi_hbm, bm_hbm, bo_hbm, out_ref,
    wa_raw, wd_raw, wi_raw, wm_raw, wo_raw, ba_raw, bd_raw, bi_raw, bm_raw, bo_raw, w_sem,
    wao_ref, wah_ref, wdo_ref, wdh_ref, win_ref, wmid_ref, wout_ref, bn_ref,
    ximg, xabove, xbelow, tscr, za, rsend, rrecv, zd, h, zi, u2, habove, hbelow,
    zm, zo, stats, recv,
    img_sem, isend_sem, irecv_sem, rsend_sem, rrecv_sem, hsend_sem, hrecv_sem,
    ssem, rsem,
):
    me = lax.axis_index("sp")
    nxt, prv = me + 1, me - 1
    has_next, has_prev = me < n - 1, me > 0
    pairs = ximg.shape[1]
    half_w = tscr.shape[0] // 2
    full_w = tscr.shape[0]
    count_a = float(2 * pairs * 2 * full_w * n)
    count_b = float(2 * pairs * half_w * n)
    everything = (0, pairs)

    img_load = cuts(0, pairs, (4, 4, 4, 4))
    img_spans = cuts(0, pairs, IMG_CUTS)
    row_spans = cuts(0, pairs, LATE_CUTS)
    mid_spans = cuts(0, pairs, LATE_CUTS)

    params = [
        pltpu.make_async_copy(src, dst, w_sem.at[i])
        for i, (src, dst) in enumerate((
            (wa_hbm, wa_raw), (wd_hbm, wd_raw), (wi_hbm, wi_raw), (wm_hbm, wm_raw), (wo_hbm, wo_raw),
            (ba_hbm, ba_raw), (bd_hbm, bd_raw), (bi_hbm, bi_raw), (bm_hbm, bm_raw), (bo_hbm, bo_raw),
        ))
    ]
    local_img = [
        pltpu.make_async_copy(img_hbm.at[:, pl.ds(*span)], ximg.at[:, pl.ds(*span)], img_sem.at[c])
        for c, span in enumerate(img_load)
    ]
    barrier = pltpu.get_barrier_semaphore()
    for d in range(1, n):
        pl.semaphore_signal(barrier, inc=1, device_id={"sp": lax.rem(me + d, n)}, device_id_type=MESH)
    params[0].start()
    for copy in local_img:
        copy.start()
    for copy in params[1:]:
        copy.start()

    pl.semaphore_wait(barrier, n - 1)

    def to_dev(src, dst, send_sem, recv_sem, dev):
        return pltpu.make_async_remote_copy(
            src_ref=src, dst_ref=dst, send_sem=send_sem, recv_sem=recv_sem, device_id={"sp": dev}, device_id_type=MESH
        )

    def img_down(c):
        part = pl.ds(*img_spans[c])
        return to_dev(ximg.at[:, part, 1], xabove.at[:, part], isend_sem.at[0, c], irecv_sem.at[0, c], nxt)

    def img_up(c):
        part = pl.ds(*img_spans[c])
        return to_dev(ximg.at[:, part, 0], xbelow.at[:, part], isend_sem.at[1, c], irecv_sem.at[1, c], prv)

    def exchange(down, up, c):
        @pl.when(has_next)
        def _():
            down(c).start()

        @pl.when(has_prev)
        def _():
            up(c).start()

    def arrived(down, up, c):
        @pl.when(has_prev)
        def _():
            down(c).wait_recv()

        @pl.when(has_next)
        def _():
            up(c).wait_recv()

    for copy in local_img:
        copy.wait()
    for c in range(len(img_spans)):
        exchange(img_down, img_up, c)

    @pl.when(me == n - 1)
    def _():
        xbelow[...] = jnp.zeros_like(xbelow)
        rrecv[...] = jnp.zeros_like(rrecv)
        hbelow[...] = jnp.zeros_like(hbelow)

    @pl.when(me == 0)
    def _():
        xabove[...] = jnp.zeros_like(xabove)
        habove[...] = jnp.zeros_like(habove)

    params[0].wait()
    expand_stage_a(wa_raw[...], wao_ref, wah_ref)

    def shift_down(y):
        row = lax.broadcasted_iota(jnp.int32, y.shape, 0)
        return jnp.where(row == 0, 0.0, pltpu.roll(y, 1, 0))

    def shift_up(y):
        row = lax.broadcasted_iota(jnp.int32, y.shape, 0)
        return jnp.where(row == y.shape[0] - 1, 0.0, pltpu.roll(y, y.shape[0] - 1, 0))

    def add_stats(acc, z):
        blocks = z.reshape(z.shape[0] // 8, 8, LANES)
        return acc[0] + jnp.sum(blocks, axis=0), acc[1] + jnp.sum(blocks * blocks, axis=0)

    zero_acc = (jnp.zeros((8, LANES), F32), jnp.zeros((8, LANES), F32))

    def group_stats(k, acc, group):
        def fold(v):
            width = group
            while width < LANES:
                v = v + pltpu.roll(v, width, 1)
                width *= 2
            return jnp.sum(v, axis=0, keepdims=True)

        mine = jnp.concatenate([fold(acc[0]), fold(acc[1])], axis=0)
        stats[k] = mine
        for d in far_first(n):
            to_dev(stats.at[k], recv.at[k, d - 1], ssem.at[k], rsem.at[k], lax.rem(me + d, n)).start()
        to_dev(recv.at[k], recv.at[k], ssem.at[k], rsem.at[k], me).wait_recv()
        return mine + jnp.sum(recv[k], axis=0)

    def norm_of(k, total, count):
        moments = total * (1.0 / count)
        mean = moments[0:1]
        var = moments[1:2] - mean * mean
        scale = bn_ref[k, 0:1] * lax.rsqrt(var + NORM_EPS)
        return mean, scale, bn_ref[k, 1:2]

    def bn(z, norm):
        mean, scale, shift = norm
        return (z - mean) * scale + shift

    lane2 = lax.broadcasted_iota(jnp.int32, (half_w, 2 * LANES), 1)
    even_lane = lax.rem(lane2 // 32, 2) == 0

    def stage_a_part(x, w_ref):
        tscr[...] = x.astype(F32).T
        lhs = jnp.concatenate(
            [tscr[pl.ds(0, half_w, stride=2), :], tscr[pl.ds(1, half_w, stride=2), :]], axis=1
        ).astype(BF16)
        y = jnp.dot(lhs, w_ref[...], preferred_element_type=F32)
        cross = y[:, 2 * LANES:]
        return y[:, : 2 * LANES] + jnp.where(even_lane, shift_down(cross), shift_up(cross))

    def own_a(q, carry):
        x = jnp.concatenate([ximg[0, q].reshape(2 * 32, full_w), ximg[1, q].reshape(2 * 32, full_w)], axis=0)
        z = stage_a_part(x, wao_ref)
        za[0, q] = z[:, :LANES]
        za[1, q] = z[:, LANES:]
        return carry

    over(everything, own_a)

    for copy in params[1:]:
        copy.wait()
    expand_down(wd_raw, wdo_ref, wdh_ref)
    expand_blocks(wi_raw, wm_raw, wo_raw, win_ref, wmid_ref, wout_ref)
    bn_ref[0] = jnp.concatenate([ba_raw[0]] * 4, axis=1)
    bn_ref[1] = bd_raw[...]
    for j in range(wi_raw.shape[0]):
        bn_ref[2 + 3 * j] = jnp.concatenate([bi_raw[j]] * 2, axis=1)
        bn_ref[3 + 3 * j] = jnp.concatenate([bm_raw[j]] * 2, axis=1)
        bn_ref[4 + 3 * j] = bo_raw[j]

    def halo_a(q, acc):
        x = jnp.concatenate([xabove[0, q], xbelow[0, q], xabove[1, q], xbelow[1, q]], axis=0)
        z = stage_a_part(x, wah_ref)
        z0 = za[0, q] + z[:, :LANES]
        z1 = za[1, q] + z[:, LANES:]
        za[0, q] = z0
        za[1, q] = z1
        return add_stats(add_stats(acc, z0), z1)

    acc = zero_acc
    for c, span in enumerate(img_spans):
        arrived(img_down, img_up, c)
        acc = over(span, halo_a, acc)

    lane1 = lax.broadcasted_iota(jnp.int32, (half_w, LANES), 1)
    low_lane = lane1 < 64

    def row_up(c):
        part = pl.ds(*row_spans[c])
        return to_dev(rsend.at[part], rrecv.at[part], rsend_sem.at[c], rrecv_sem.at[c], prv)

    def first_rows(t0, t1):
        return jnp.where(low_lane, t0, pltpu.roll(t1, 64, 1))

    norm = norm_of(0, group_stats(0, acc, 32), count_a)

    def pack_row(q, carry):
        rsend[q] = jnp.maximum(bn(first_rows(za[0, q], za[1, q]), norm), 0.0).astype(BF16)
        return carry

    for c, span in enumerate(row_spans):
        over(span, pack_row)

        @pl.when(has_prev)
        def _():
            row_up(c).start()

    def own_down(q, carry):
        for a in range(2):
            t = jnp.maximum(bn(za[a, q], norm), 0.0).astype(BF16)
            y = jnp.dot(t, wdo_ref[...], preferred_element_type=F32)
            zd[a, q] = y[:, :LANES] + shift_up(y[:, LANES:])
        return carry

    over(everything, own_down)

    def halo_down(q, acc):
        y = jnp.dot(rrecv[q], wdh_ref[...], preferred_element_type=F32)
        for a in range(2):
            lo = 2 * a * LANES
            z = zd[a, q] + y[:, lo:lo + LANES] + shift_up(y[:, lo + LANES:lo + 2 * LANES])
            zd[a, q] = z
            acc = add_stats(acc, z)
        return acc

    acc = zero_acc
    for c, span in enumerate(row_spans):
        @pl.when(has_next)
        def _():
            row_up(c).wait_recv()

        acc = over(span, halo_down, acc)
    norm = norm_of(1, group_stats(1, acc, LANES), count_b)

    blocks = win_ref.shape[0]

    def mid_down(j):
        def copy(c):
            part = pl.ds(*mid_spans[c])
            return to_dev(u2.at[j, part], habove.at[j, part], hsend_sem.at[j, 0, c], hrecv_sem.at[j, 0, c], nxt)
        return copy

    def mid_up(j):
        def copy(c):
            part = pl.ds(*mid_spans[c])
            return to_dev(u2.at[j, part], hbelow.at[j, part], hsend_sem.at[j, 1, c], hrecv_sem.at[j, 1, c], prv)
        return copy

    for j in range(blocks):
        def layer_in(q, acc):
            parts = []
            for a in range(2):
                if j == 0:
                    t = bn(zd[a, q], norm)
                else:
                    t = bn(zo[a, q], norm) + h[a, q].astype(F32)
                t = jnp.maximum(t, 0.0).astype(BF16)
                h[a, q] = t
                parts.append(t)
            z = jnp.dot(jnp.concatenate(parts, axis=1), win_ref[j], preferred_element_type=F32)
            zi[q] = z
            return add_stats(acc, z)

        acc = over(everything, layer_in, zero_acc, 4)
        norm = norm_of(2 + 3 * j, group_stats(2 + 3 * j, acc, 64), count_b)

        def act_in(q, carry):
            u2[j, q] = jnp.maximum(bn(zi[q], norm), 0.0).astype(BF16)
            return carry

        for c, span in enumerate(mid_spans):
            over(span, act_in)
            exchange(mid_down(j), mid_up(j), c)
        def layer_mid(q, acc):
            lhs = jnp.concatenate([u2[j, q], habove[j, q], hbelow[j, q]], axis=1)
            y = jnp.dot(lhs, wmid_ref[j], preferred_element_type=F32)
            z = shift_down(y[:, :LANES]) + y[:, LANES:2 * LANES] + shift_up(y[:, 2 * LANES:])
            zm[q] = z
            return add_stats(acc, z)

        acc = zero_acc
        for c, span in enumerate(mid_spans):
            arrived(mid_down(j), mid_up(j), c)
            acc = over(span, layer_mid, acc)
        norm = norm_of(3 + 3 * j, group_stats(3 + 3 * j, acc, 64), count_b)

        def layer_out(q, acc):
            u = jnp.maximum(bn(zm[q], norm), 0.0).astype(BF16)
            y = jnp.dot(u, wout_ref[j], preferred_element_type=F32)
            for a in range(2):
                z = y[:, a * LANES:(a + 1) * LANES]
                zo[a, q] = z
                acc = add_stats(acc, z)
            return acc

        acc = over(everything, layer_out, zero_acc, 4)
        norm = norm_of(4 + 3 * j, group_stats(4 + 3 * j, acc, LANES), count_b)

    def final(q, carry):
        for a in range(2):
            out_ref[a, q] = jnp.maximum(bn(zo[a, q], norm) + h[a, q].astype(F32), 0.0).astype(BF16)
        return carry

    over(everything, final, 0, 2)

    for k in range(stats.shape[0]):
        to_dev(recv.at[k], recv.at[k], ssem.at[k], rsem.at[k], me).wait_send()

    @pl.when(has_next)
    def _():
        for c in range(len(img_spans)):
            img_down(c).wait_send()
        for j in range(blocks):
            for c in range(len(mid_spans)):
                mid_down(j)(c).wait_send()

    @pl.when(has_prev)
    def _():
        for c in range(len(img_spans)):
            img_up(c).wait_send()
        for c in range(len(row_spans)):
            row_up(c).wait_send()
        for j in range(blocks):
            for c in range(len(mid_spans)):
                mid_up(j)(c).wait_send()


def solution(mesh):
    n = mesh.shape["sp"]

    def forward(images, w_a, bn_a, w_down, bn_down, w_in, bn_in, w_mid, bn_mid, w_out, bn_out):
        count, rows, width, chan_a = images.shape
        pairs, half_w = count // 2, width // 2
        blocks = w_in.shape[0]
        img = jnp.transpose(images, (0, 1, 3, 2)).reshape(2, pairs, rows, chan_a, width)
        taps = w_a.shape[1] * w_a.shape[2]
        raw = [
            w_a.reshape(taps * chan_a, chan_a), w_down.reshape(taps, chan_a, LANES), jnp.transpose(w_in, (0, 2, 1)),
            w_mid.reshape(blocks, taps, 64, 64), w_out, bn_a, bn_down, bn_in, bn_mid, bn_out,
        ]
        steps = 2 + 3 * blocks

        dma = pltpu.SemaphoreType.DMA
        out = pl.pallas_call(
            functools.partial(kernel, n),
            out_shape=pltpu.VMEM((2, pairs, half_w, LANES), BF16),
            in_specs=[pl.BlockSpec(memory_space=pltpu.HBM)] * 11,
            out_specs=pl.BlockSpec(memory_space=pltpu.VMEM),
            scratch_shapes=[pltpu.VMEM(x.shape, x.dtype) for x in raw] + [
                dma((len(raw),)),
                pltpu.VMEM((2 * LANES, 4 * LANES), BF16),
                pltpu.VMEM((2 * LANES, 4 * LANES), BF16),
                pltpu.VMEM((LANES, 2 * LANES), BF16),
                pltpu.VMEM((LANES, 4 * LANES), BF16),
                pltpu.VMEM((blocks, 2 * LANES, LANES), BF16),
                pltpu.VMEM((blocks, 3 * LANES, 3 * LANES), BF16),
                pltpu.VMEM((blocks, LANES, 2 * LANES), BF16),
                pltpu.VMEM((steps, 2, LANES), F32),
                pltpu.VMEM((2, pairs, rows, chan_a, width), BF16),
                pltpu.VMEM((2, pairs, chan_a, width), BF16),
                pltpu.VMEM((2, pairs, chan_a, width), BF16),
                pltpu.VMEM((width, LANES), F32),
                pltpu.VMEM((2, pairs, half_w, LANES), F32),
                pltpu.VMEM((pairs, half_w, LANES), BF16),
                pltpu.VMEM((pairs, half_w, LANES), BF16),
                pltpu.VMEM((2, pairs, half_w, LANES), F32),
                pltpu.VMEM((2, pairs, half_w, LANES), BF16),
                pltpu.VMEM((pairs, half_w, LANES), F32),
                pltpu.VMEM((blocks, pairs, half_w, LANES), BF16),
                pltpu.VMEM((blocks, pairs, half_w, LANES), BF16),
                pltpu.VMEM((blocks, pairs, half_w, LANES), BF16),
                pltpu.VMEM((pairs, half_w, LANES), F32),
                pltpu.VMEM((2, pairs, half_w, LANES), F32),
                pltpu.VMEM((steps, 2, LANES), F32),
                pltpu.VMEM((steps, n - 1, 2, LANES), F32),
                dma((4,)),
                dma((2, len(IMG_CUTS))),
                dma((2, len(IMG_CUTS))),
                dma((len(LATE_CUTS),)),
                dma((len(LATE_CUTS),)),
                dma((blocks, 2, len(LATE_CUTS))),
                dma((blocks, 2, len(LATE_CUTS))),
                dma((steps,)),
                dma((steps,)),
            ],
            compiler_params=pltpu.CompilerParams(
                collective_id=0, has_side_effects=True, vmem_limit_bytes=52 * 1024 * 1024
            ),
        )(img, *raw)
        return out.reshape(count, rows // 2, half_w, LANES)

    act_spec = P("dp", "sp", None, None)
    return jax.shard_map(forward, mesh=mesh, in_specs=(act_spec,) + (P(),) * 10, out_specs=act_spec, check_vma=False)
```

```python
import functools
import math

import jax
import jax.numpy as jnp
from jax import lax
from jax.experimental import pallas as pl
from jax.experimental.pallas import tpu as pltpu
from jax.sharding import PartitionSpec as P

NORM_EPS = 1e-5
MESH = pl.DeviceIdType.MESH
LANES = 128
IMG_CUTS = (5, 5, 4, 2)
ROW_CUTS = (5, 5, 4, 2)
LATE_CUTS = (5, 7, 3, 1)
F32 = jnp.float32
BF16 = jnp.bfloat16


def cuts(first, last, weights):
    total, seen, edge, spans = sum(weights), 0, first, []
    for weight in weights:
        seen += weight
        end = first + (last - first) * seen // total
        if end > edge:
            spans.append((edge, end - edge))
        edge = end
    return spans


def over(span, body, carry=0, step=1):
    start, length = span
    trips = length // step

    def trip(i, carry):
        for k in range(step):
            carry = body(start + i * step + k, carry)
        return carry

    if trips == 1:
        carry = trip(0, carry)
    elif trips > 1:
        carry = lax.fori_loop(0, trips, trip, carry)
    for q in range(start + trips * step, start + length):
        carry = body(q, carry)
    return carry


def far_first(n):
    side = max(1, math.isqrt(n // 2))

    def hops(d):
        x, y = d // 2 % side, d // (2 * side)
        return min(x, side - x) + min(y, abs(side - y))

    return sorted(range(1, n), key=lambda d: (-hops(d), d))


def placement(size, copies):
    row = lax.broadcasted_iota(jnp.int32, (size, copies * LANES), 0)
    lane = lax.broadcasted_iota(jnp.int32, (size, copies * LANES), 1)
    hit = lane == row
    for i in range(1, copies):
        hit = jnp.logical_or(hit, lane == row + i * (LANES + size))
    return hit.astype(F32).astype(BF16)


def expand_stage_a(w, own_ref, halo_ref, third_ref):
    spread = jnp.dot(w, placement(32, 4), preferred_element_type=F32)
    own_ref[...] = jnp.zeros_like(own_ref)
    halo_ref[...] = jnp.zeros_like(halo_ref)
    for ref, halo in ((own_ref, False), (halo_ref, True)):
        for pi in range(2):
            for ri in range(2):
                for shift in range(2):
                    total = jnp.zeros((32, LANES), F32)
                    for ro in range(2):
                        for po in range(2):
                            if halo and ri != ro:
                                continue
                            if shift and pi == po:
                                continue
                            ky = 2 * ri if halo else ri - ro + 1
                            kx = (0 if pi == 1 else 2) if shift else pi - po + 1
                            tap, i = ky * 3 + kx, ro * 2 + po
                            total += spread[tap * 32:(tap + 1) * 32, i * LANES:(i + 1) * LANES]
                    block = total.astype(BF16)
                    for a in range(2):
                        row, col = ((pi * 2 + a) * 2 + ri) * 32, (shift * 2 + a) * LANES
                        ref[row:row + 32, col:col + LANES] = block
    third_ref[...] = jnp.zeros_like(third_ref)
    for a in range(2):
        for pi in range(2):
            for ky in range(3):
                for shift in range(2):
                    total = jnp.zeros((32, LANES), F32)
                    for po in range(2):
                        if shift and pi == po:
                            continue
                        kx = (0 if pi == 1 else 2) if shift else pi - po + 1
                        tap, i = ky * 3 + kx, a * 2 + po
                        total += spread[tap * 32:(tap + 1) * 32, i * LANES:(i + 1) * LANES]
                    row = ((a * 2 + pi) * 4 + ky) * 32
                    third_ref[row:row + 32, shift * LANES:(shift + 1) * LANES] = total.astype(BF16)


def expand_down(w_ref, own_ref, halo_ref):
    own_ref[...] = jnp.zeros_like(own_ref)
    halo_ref[...] = jnp.zeros_like(halo_ref)
    for par in range(2):
        for shift in range(2 - par):
            kx = 2 if shift else par
            for row in range(2):
                at = (row * 2 + par) * 32
                own_ref[at:at + 32, shift * LANES:(shift + 1) * LANES] = w_ref[row * 3 + kx]
            for a in range(2):
                at, col = (a * 2 + par) * 32, (a * 2 + shift) * LANES
                halo_ref[at:at + 32, col:col + LANES] = w_ref[6 + kx]


def expand_blocks(w_in_ref, w_mid_ref, w_out_ref, win_ref, wmid_ref, wout_ref):
    spot = placement(64, 2)
    for j in range(win_ref.shape[0]):
        w_in = w_in_ref[j].astype(F32).T.astype(BF16)
        spread = jnp.dot(w_in, spot, preferred_element_type=F32).astype(BF16)
        for a in range(2):
            win_ref[j, a * LANES:(a + 1) * LANES, :] = spread[:, a * LANES:(a + 1) * LANES]
        for src, ky in enumerate((1, 0, 2)):
            for kx in range(3):
                spread = jnp.dot(w_mid_ref[j, ky * 3 + kx], spot, preferred_element_type=F32).astype(BF16)
                for a in range(2):
                    at = (src * 2 + a) * 64
                    wmid_ref[j, at:at + 64, kx * LANES:(kx + 1) * LANES] = spread[:, a * LANES:(a + 1) * LANES]
        zeros = jnp.zeros((64, LANES), BF16)
        for a in range(2):
            for b in range(2):
                wout_ref[j, a * 64:(a + 1) * 64, b * LANES:(b + 1) * LANES] = w_out_ref[j] if a == b else zeros


def kernel(
    n, img_hbm, wa_hbm, wd_hbm, wi_hbm, wm_hbm, wo_hbm, ba_hbm, bd_hbm, bi_hbm, bm_hbm, bo_hbm, out_ref,
    wa_raw, wd_raw, wi_raw, wm_raw, wo_raw, ba_raw, bd_raw, bi_raw, bm_raw, bo_raw, w_sem,
    wao_ref, wah_ref, wat_ref, wdo_ref, wdh_ref, win_ref, wmid_ref, wout_ref, bn_ref,
    ximg, xabove, xbelow, tscr, za, zthird, rrow, zd, h, zi, u2, habove, hbelow,
    zm, zo, stats, recv,
    img_sem, isend_sem, irecv_sem, rowsend_sem, rowrecv_sem, hsend_sem, hrecv_sem,
    ssem, rsem,
):
    me = lax.axis_index("sp")
    nxt, prv = me + 1, me - 1
    has_next, has_prev = me < n - 1, me > 0
    pairs = ximg.shape[1]
    half_w = tscr.shape[1] // 2
    full_w = tscr.shape[1]
    count_a = float(2 * pairs * 2 * full_w * n)
    count_b = float(2 * pairs * half_w * n)
    everything = (0, pairs)

    img_load = cuts(0, pairs, (4, 4, 4, 4))
    img_spans = cuts(0, pairs, IMG_CUTS)
    row_spans = cuts(0, pairs, ROW_CUTS)
    mid_spans = cuts(0, pairs, LATE_CUTS)

    params = [
        pltpu.make_async_copy(src, dst, w_sem.at[i])
        for i, (src, dst) in enumerate((
            (wa_hbm, wa_raw), (wd_hbm, wd_raw), (wi_hbm, wi_raw), (wm_hbm, wm_raw), (wo_hbm, wo_raw),
            (ba_hbm, ba_raw), (bd_hbm, bd_raw), (bi_hbm, bi_raw), (bm_hbm, bm_raw), (bo_hbm, bo_raw),
        ))
    ]
    local_img = [
        pltpu.make_async_copy(img_hbm.at[:, pl.ds(*span)], ximg.at[:, pl.ds(*span)], img_sem.at[c])
        for c, span in enumerate(img_load)
    ]
    barrier = pltpu.get_barrier_semaphore()
    for d in range(1, n):
        pl.semaphore_signal(barrier, inc=1, device_id={"sp": lax.rem(me + d, n)}, device_id_type=MESH)
    params[0].start()
    for copy in local_img:
        copy.start()
    for copy in params[1:]:
        copy.start()

    pl.semaphore_wait(barrier, n - 1)

    def to_dev(src, dst, send_sem, recv_sem, dev):
        return pltpu.make_async_remote_copy(
            src_ref=src, dst_ref=dst, send_sem=send_sem, recv_sem=recv_sem, device_id={"sp": dev}, device_id_type=MESH
        )

    def img_down(c):
        part = pl.ds(*img_spans[c])
        return to_dev(ximg.at[:, part, 1], xabove.at[:, part], isend_sem.at[0, c], irecv_sem.at[0, c], nxt)

    def img_up(c):
        part = pl.ds(*img_spans[c])
        return to_dev(ximg.at[:, part, 0], xbelow.at[:, part, 0], isend_sem.at[1, c], irecv_sem.at[1, c], prv)

    def row_up(c):
        part = pl.ds(*row_spans[c])
        return to_dev(ximg.at[:, part, 1], xbelow.at[:, part, 1], rowsend_sem.at[c], rowrecv_sem.at[c], prv)

    def exchange(down, up, c):
        @pl.when(has_next)
        def _():
            down(c).start()

        @pl.when(has_prev)
        def _():
            up(c).start()

    def arrived(down, up, c):
        @pl.when(has_prev)
        def _():
            down(c).wait_recv()

        @pl.when(has_next)
        def _():
            up(c).wait_recv()

    for copy in local_img:
        copy.wait()
    for c in range(len(img_spans)):
        exchange(img_down, img_up, c)
    @pl.when(me == n - 1)
    def _():
        xbelow[...] = jnp.zeros_like(xbelow)
        rrow[...] = jnp.zeros_like(rrow)
        hbelow[...] = jnp.zeros_like(hbelow)

    @pl.when(me == 0)
    def _():
        xabove[...] = jnp.zeros_like(xabove)
        habove[...] = jnp.zeros_like(habove)

    params[0].wait()
    expand_stage_a(wa_raw[...], wao_ref, wah_ref, wat_ref)

    def shift_down(y):
        row = lax.broadcasted_iota(jnp.int32, y.shape, 0)
        return jnp.where(row == 0, 0.0, pltpu.roll(y, 1, 0))

    def shift_up(y):
        row = lax.broadcasted_iota(jnp.int32, y.shape, 0)
        return jnp.where(row == y.shape[0] - 1, 0.0, pltpu.roll(y, y.shape[0] - 1, 0))

    def add_stats(acc, z):
        blocks = z.reshape(z.shape[0] // 8, 8, LANES)
        return acc[0] + jnp.sum(blocks, axis=0), acc[1] + jnp.sum(blocks * blocks, axis=0)

    zero_acc = (jnp.zeros((8, LANES), F32), jnp.zeros((8, LANES), F32))

    def start_stats(k, acc, group):
        def fold(v):
            width = group
            while width < LANES:
                v = v + pltpu.roll(v, width, 1)
                width *= 2
            return jnp.sum(v, axis=0, keepdims=True)

        mine = jnp.concatenate([fold(acc[0]), fold(acc[1])], axis=0)
        stats[k] = mine
        for d in far_first(n):
            to_dev(stats.at[k], recv.at[k, d - 1], ssem.at[k], rsem.at[k], lax.rem(me + d, n)).start()
        return mine

    def end_stats(k, mine):
        to_dev(recv.at[k], recv.at[k], ssem.at[k], rsem.at[k], me).wait_recv()
        return mine + jnp.sum(recv[k], axis=0)

    def group_stats(k, acc, group):
        return end_stats(k, start_stats(k, acc, group))

    def norm_of(k, total, count):
        moments = total * (1.0 / count)
        mean = moments[0:1]
        var = moments[1:2] - mean * mean
        scale = bn_ref[k, 0:1] * lax.rsqrt(var + NORM_EPS)
        return mean, scale, bn_ref[k, 1:2]

    def bn(z, norm):
        mean, scale, shift = norm
        return (z - mean) * scale + shift

    lane2 = lax.broadcasted_iota(jnp.int32, (half_w, 2 * LANES), 1)
    even_lane = lax.rem(lane2 // 32, 2) == 0

    def split_parity(x, a):
        tscr[a] = x.astype(F32).T
        return [tscr[a, pl.ds(0, half_w, stride=2), :], tscr[a, pl.ds(1, half_w, stride=2), :]]

    def stage_a_part(x, w_ref):
        lhs = jnp.concatenate(split_parity(x, 0), axis=1).astype(BF16)
        y = jnp.dot(lhs, w_ref[...], preferred_element_type=F32)
        cross = y[:, 2 * LANES:]
        return y[:, : 2 * LANES] + jnp.where(even_lane, shift_down(cross), shift_up(cross))

    def third_row(q, carry):
        parts = []
        for a in range(2):
            x = jnp.concatenate([ximg[a, q, 1], xbelow[a, q, 0], xbelow[a, q, 1], ximg[a, q, 0]], axis=0)
            parts += split_parity(x, a)
        y = jnp.dot(jnp.concatenate(parts, axis=1).astype(BF16), wat_ref[...], preferred_element_type=F32)
        cross = y[:, LANES:]
        zthird[q] = y[:, :LANES] + jnp.where(even_lane[:, :LANES], shift_down(cross), shift_up(cross))
        return carry

    def own_a(q, carry):
        x = jnp.concatenate([ximg[0, q].reshape(2 * 32, full_w), ximg[1, q].reshape(2 * 32, full_w)], axis=0)
        z = stage_a_part(x, wao_ref)
        za[0, q] = z[:, :LANES]
        za[1, q] = z[:, LANES:]
        return carry

    over(everything, own_a)

    for copy in params[1:]:
        copy.wait()
    expand_down(wd_raw, wdo_ref, wdh_ref)
    expand_blocks(wi_raw, wm_raw, wo_raw, win_ref, wmid_ref, wout_ref)
    bn_ref[0] = jnp.concatenate([ba_raw[0]] * 4, axis=1)
    bn_ref[1] = bd_raw[...]
    for j in range(wi_raw.shape[0]):
        bn_ref[2 + 3 * j] = jnp.concatenate([bi_raw[j]] * 2, axis=1)
        bn_ref[3 + 3 * j] = jnp.concatenate([bm_raw[j]] * 2, axis=1)
        bn_ref[4 + 3 * j] = bo_raw[j]

    def halo_a(q, acc):
        x = jnp.concatenate([xabove[0, q], xbelow[0, q, 0], xabove[1, q], xbelow[1, q, 0]], axis=0)
        z = stage_a_part(x, wah_ref)
        z0 = za[0, q] + z[:, :LANES]
        z1 = za[1, q] + z[:, LANES:]
        za[0, q] = z0
        za[1, q] = z1
        return add_stats(add_stats(acc, z0), z1)

    acc = zero_acc
    for c, span in enumerate(img_spans):
        arrived(img_down, img_up, c)
        acc = over(span, halo_a, acc)

    mine = start_stats(0, acc, 32)
    for c in range(len(row_spans)):
        @pl.when(has_prev)
        def _():
            row_up(c).start()

    @pl.when(has_next)
    def _():
        row_up(0).wait_recv()
        over(row_spans[0], third_row)

    norm = norm_of(0, end_stats(0, mine), count_a)

    def own_down(q, carry):
        for a in range(2):
            t = jnp.maximum(bn(za[a, q], norm), 0.0).astype(BF16)
            y = jnp.dot(t, wdo_ref[...], preferred_element_type=F32)
            zd[a, q] = y[:, :LANES] + shift_up(y[:, LANES:])
        return carry

    over(everything, own_down)

    def halo_down(q, acc):
        y = jnp.dot(rrow[q], wdh_ref[...], preferred_element_type=F32)
        for a in range(2):
            lo = 2 * a * LANES
            z = zd[a, q] + y[:, lo:lo + LANES] + shift_up(y[:, lo + LANES:lo + 2 * LANES])
            zd[a, q] = z
            acc = add_stats(acc, z)
        return acc

    def norm_row(q, carry):
        rrow[q] = jnp.maximum(bn(zthird[q], norm), 0.0).astype(BF16)
        return carry

    acc = zero_acc
    for c, span in enumerate(row_spans):
        @pl.when(has_next)
        def _():
            if c:
                row_up(c).wait_recv()
                over(span, third_row)
            over(span, norm_row)

        acc = over(span, halo_down, acc)
    norm = norm_of(1, group_stats(1, acc, LANES), count_b)

    blocks = win_ref.shape[0]

    def mid_down(j):
        def copy(c):
            part = pl.ds(*mid_spans[c])
            return to_dev(u2.at[j, part], habove.at[j, part], hsend_sem.at[j, 0, c], hrecv_sem.at[j, 0, c], nxt)
        return copy

    def mid_up(j):
        def copy(c):
            part = pl.ds(*mid_spans[c])
            return to_dev(u2.at[j, part], hbelow.at[j, part], hsend_sem.at[j, 1, c], hrecv_sem.at[j, 1, c], prv)
        return copy

    for j in range(blocks):
        def layer_in(q, acc):
            parts = []
            for a in range(2):
                if j == 0:
                    t = bn(zd[a, q], norm)
                else:
                    t = bn(zo[a, q], norm) + h[a, q].astype(F32)
                t = jnp.maximum(t, 0.0).astype(BF16)
                h[a, q] = t
                parts.append(t)
            z = jnp.dot(jnp.concatenate(parts, axis=1), win_ref[j], preferred_element_type=F32)
            zi[q] = z
            return add_stats(acc, z)

        acc = over(everything, layer_in, zero_acc, 4)
        norm = norm_of(2 + 3 * j, group_stats(2 + 3 * j, acc, 64), count_b)

        def act_in(q, carry):
            u2[j, q] = jnp.maximum(bn(zi[q], norm), 0.0).astype(BF16)
            return carry

        for c, span in enumerate(mid_spans):
            over(span, act_in)
            exchange(mid_down(j), mid_up(j), c)
        def layer_mid(q, acc):
            lhs = jnp.concatenate([u2[j, q], habove[j, q], hbelow[j, q]], axis=1)
            y = jnp.dot(lhs, wmid_ref[j], preferred_element_type=F32)
            z = shift_down(y[:, :LANES]) + y[:, LANES:2 * LANES] + shift_up(y[:, 2 * LANES:])
            zm[q] = z
            return add_stats(acc, z)

        acc = zero_acc
        for c, span in enumerate(mid_spans):
            arrived(mid_down(j), mid_up(j), c)
            acc = over(span, layer_mid, acc)
        norm = norm_of(3 + 3 * j, group_stats(3 + 3 * j, acc, 64), count_b)

        def layer_out(q, acc):
            u = jnp.maximum(bn(zm[q], norm), 0.0).astype(BF16)
            y = jnp.dot(u, wout_ref[j], preferred_element_type=F32)
            for a in range(2):
                z = y[:, a * LANES:(a + 1) * LANES]
                zo[a, q] = z
                acc = add_stats(acc, z)
            return acc

        acc = over(everything, layer_out, zero_acc, 4)
        norm = norm_of(4 + 3 * j, group_stats(4 + 3 * j, acc, LANES), count_b)

    def final(q, carry):
        for a in range(2):
            out_ref[a, q] = jnp.maximum(bn(zo[a, q], norm) + h[a, q].astype(F32), 0.0).astype(BF16)
        return carry

    over(everything, final, 0, 2)

    for k in range(stats.shape[0]):
        to_dev(recv.at[k], recv.at[k], ssem.at[k], rsem.at[k], me).wait_send()

    @pl.when(has_next)
    def _():
        for c in range(len(img_spans)):
            img_down(c).wait_send()
        for j in range(blocks):
            for c in range(len(mid_spans)):
                mid_down(j)(c).wait_send()

    @pl.when(has_prev)
    def _():
        for c in range(len(img_spans)):
            img_up(c).wait_send()
        for c in range(len(row_spans)):
            row_up(c).wait_send()
        for j in range(blocks):
            for c in range(len(mid_spans)):
                mid_up(j)(c).wait_send()


def solution(mesh):
    n = mesh.shape["sp"]

    def forward(images, w_a, bn_a, w_down, bn_down, w_in, bn_in, w_mid, bn_mid, w_out, bn_out):
        count, rows, width, chan_a = images.shape
        pairs, half_w = count // 2, width // 2
        blocks = w_in.shape[0]
        img = jnp.transpose(images, (0, 1, 3, 2)).reshape(2, pairs, rows, chan_a, width)
        taps = w_a.shape[1] * w_a.shape[2]
        raw = [
            w_a.reshape(taps * chan_a, chan_a), w_down.reshape(taps, chan_a, LANES), jnp.transpose(w_in, (0, 2, 1)),
            w_mid.reshape(blocks, taps, 64, 64), w_out, bn_a, bn_down, bn_in, bn_mid, bn_out,
        ]
        steps = 2 + 3 * blocks

        dma = pltpu.SemaphoreType.DMA
        out = pl.pallas_call(
            functools.partial(kernel, n),
            out_shape=pltpu.VMEM((2, pairs, half_w, LANES), BF16),
            in_specs=[pl.BlockSpec(memory_space=pltpu.HBM)] * 11,
            out_specs=pl.BlockSpec(memory_space=pltpu.VMEM),
            scratch_shapes=[pltpu.VMEM(x.shape, x.dtype) for x in raw] + [
                dma((len(raw),)),
                pltpu.VMEM((2 * LANES, 4 * LANES), BF16),
                pltpu.VMEM((2 * LANES, 4 * LANES), BF16),
                pltpu.VMEM((4 * LANES, 2 * LANES), BF16),
                pltpu.VMEM((LANES, 2 * LANES), BF16),
                pltpu.VMEM((LANES, 4 * LANES), BF16),
                pltpu.VMEM((blocks, 2 * LANES, LANES), BF16),
                pltpu.VMEM((blocks, 3 * LANES, 3 * LANES), BF16),
                pltpu.VMEM((blocks, LANES, 2 * LANES), BF16),
                pltpu.VMEM((steps, 2, LANES), F32),
                pltpu.VMEM((2, pairs, rows, chan_a, width), BF16),
                pltpu.VMEM((2, pairs, chan_a, width), BF16),
                pltpu.VMEM((2, pairs, rows, chan_a, width), BF16),
                pltpu.VMEM((2, width, LANES), F32),
                pltpu.VMEM((2, pairs, half_w, LANES), F32),
                pltpu.VMEM((pairs, half_w, LANES), F32),
                pltpu.VMEM((pairs, half_w, LANES), BF16),
                pltpu.VMEM((2, pairs, half_w, LANES), F32),
                pltpu.VMEM((2, pairs, half_w, LANES), BF16),
                pltpu.VMEM((pairs, half_w, LANES), F32),
                pltpu.VMEM((blocks, pairs, half_w, LANES), BF16),
                pltpu.VMEM((blocks, pairs, half_w, LANES), BF16),
                pltpu.VMEM((blocks, pairs, half_w, LANES), BF16),
                pltpu.VMEM((pairs, half_w, LANES), F32),
                pltpu.VMEM((2, pairs, half_w, LANES), F32),
                pltpu.VMEM((steps, 2, LANES), F32),
                pltpu.VMEM((steps, n - 1, 2, LANES), F32),
                dma((4,)),
                dma((2, len(IMG_CUTS))),
                dma((2, len(IMG_CUTS))),
                dma((len(ROW_CUTS),)),
                dma((len(ROW_CUTS),)),
                dma((blocks, 2, len(LATE_CUTS))),
                dma((blocks, 2, len(LATE_CUTS))),
                dma((steps,)),
                dma((steps,)),
            ],
            compiler_params=pltpu.CompilerParams(
                collective_id=0, has_side_effects=True, vmem_limit_bytes=52 * 1024 * 1024
            ),
        )(img, *raw)
        return out.reshape(count, rows // 2, half_w, LANES)

    act_spec = P("dp", "sp", None, None)
    return jax.shard_map(forward, mesh=mesh, in_specs=(act_spec,) + (P(),) * 10, out_specs=act_spec, check_vma=False)
```

```python
import functools
import math

import jax
import jax.numpy as jnp
from jax import lax
from jax.experimental import pallas as pl
from jax.experimental.pallas import tpu as pltpu
from jax.sharding import PartitionSpec as P

NORM_EPS = 1e-5
MESH = pl.DeviceIdType.MESH
LANES = 128
IMG_CUTS = (5, 5, 4, 2)
ROW_CUTS = (5, 5, 4, 2)
ROWS_AHEAD = 2
LATE_CUTS = (5, 7, 3, 1)
F32 = jnp.float32
BF16 = jnp.bfloat16


def cuts(first, last, weights):
    total, seen, edge, spans = sum(weights), 0, first, []
    for weight in weights:
        seen += weight
        end = first + (last - first) * seen // total
        if end > edge:
            spans.append((edge, end - edge))
        edge = end
    return spans


def over(span, body, carry=0, step=1):
    start, length = span
    trips = length // step

    def trip(i, carry):
        for k in range(step):
            carry = body(start + i * step + k, carry)
        return carry

    if trips == 1:
        carry = trip(0, carry)
    elif trips > 1:
        carry = lax.fori_loop(0, trips, trip, carry)
    for q in range(start + trips * step, start + length):
        carry = body(q, carry)
    return carry


def far_first(n):
    side = max(1, math.isqrt(n // 2))

    def hops(d):
        x, y = d // 2 % side, d // (2 * side)
        return min(x, side - x) + min(y, abs(side - y))

    return sorted(range(1, n), key=lambda d: (-hops(d), d))


def placement(size, copies):
    row = lax.broadcasted_iota(jnp.int32, (size, copies * LANES), 0)
    lane = lax.broadcasted_iota(jnp.int32, (size, copies * LANES), 1)
    hit = lane == row
    for i in range(1, copies):
        hit = jnp.logical_or(hit, lane == row + i * (LANES + size))
    return hit.astype(F32).astype(BF16)


def expand_stage_a(w, own_ref, halo_ref, third_ref):
    spread = jnp.dot(w, placement(32, 4), preferred_element_type=F32)
    own_ref[...] = jnp.zeros_like(own_ref)
    halo_ref[...] = jnp.zeros_like(halo_ref)
    for ref, halo in ((own_ref, False), (halo_ref, True)):
        for pi in range(2):
            for ri in range(2):
                for shift in range(2):
                    total = jnp.zeros((32, LANES), F32)
                    for ro in range(2):
                        for po in range(2):
                            if halo and ri != ro:
                                continue
                            if shift and pi == po:
                                continue
                            ky = 2 * ri if halo else ri - ro + 1
                            kx = (0 if pi == 1 else 2) if shift else pi - po + 1
                            tap, i = ky * 3 + kx, ro * 2 + po
                            total += spread[tap * 32:(tap + 1) * 32, i * LANES:(i + 1) * LANES]
                    block = total.astype(BF16)
                    for a in range(2):
                        row, col = ((pi * 2 + a) * 2 + ri) * 32, (shift * 2 + a) * LANES
                        ref[row:row + 32, col:col + LANES] = block
    third_ref[...] = jnp.zeros_like(third_ref)
    for a in range(2):
        for pi in range(2):
            for ky in range(3):
                for shift in range(2):
                    total = jnp.zeros((32, LANES), F32)
                    for po in range(2):
                        if shift and pi == po:
                            continue
                        kx = (0 if pi == 1 else 2) if shift else pi - po + 1
                        tap, i = ky * 3 + kx, a * 2 + po
                        total += spread[tap * 32:(tap + 1) * 32, i * LANES:(i + 1) * LANES]
                    row = ((a * 2 + pi) * 4 + ky) * 32
                    third_ref[row:row + 32, shift * LANES:(shift + 1) * LANES] = total.astype(BF16)


def expand_down(w_ref, down_ref):
    down_ref[...] = jnp.zeros_like(down_ref)
    for par in range(2):
        for shift in range(2 - par):
            kx, col = 2 if shift else par, shift * LANES
            for a in range(2):
                for row in range(2):
                    at = (row * 2 + par) * 32
                    down_ref[a, at:at + 32, col:col + LANES] = w_ref[row * 3 + kx]
                at = LANES + (a * 2 + par) * 32
                down_ref[a, at:at + 32, col:col + LANES] = w_ref[6 + kx]


def expand_blocks(w_in_ref, w_mid_ref, w_out_ref, win_ref, wmid_ref, wout_ref):
    spot = placement(64, 2)
    for j in range(win_ref.shape[0]):
        w_in = w_in_ref[j].astype(F32).T.astype(BF16)
        spread = jnp.dot(w_in, spot, preferred_element_type=F32).astype(BF16)
        for a in range(2):
            win_ref[j, a * LANES:(a + 1) * LANES, :] = spread[:, a * LANES:(a + 1) * LANES]
        for src, ky in enumerate((1, 0, 2)):
            for kx in range(3):
                spread = jnp.dot(w_mid_ref[j, ky * 3 + kx], spot, preferred_element_type=F32).astype(BF16)
                for a in range(2):
                    at = (src * 2 + a) * 64
                    wmid_ref[j, at:at + 64, kx * LANES:(kx + 1) * LANES] = spread[:, a * LANES:(a + 1) * LANES]
        zeros = jnp.zeros((64, LANES), BF16)
        for a in range(2):
            for b in range(2):
                wout_ref[j, a * 64:(a + 1) * 64, b * LANES:(b + 1) * LANES] = w_out_ref[j] if a == b else zeros


def kernel(
    n, img_hbm, wa_hbm, wd_hbm, wi_hbm, wm_hbm, wo_hbm, ba_hbm, bd_hbm, bi_hbm, bm_hbm, bo_hbm, out_ref,
    wa_raw, wd_raw, wi_raw, wm_raw, wo_raw, ba_raw, bd_raw, bi_raw, bm_raw, bo_raw, w_sem,
    wao_ref, wah_ref, wat_ref, wdn_ref, win_ref, wmid_ref, wout_ref, bn_ref,
    ximg, xabove, xbelow, tscr, za, zthird, zd, h, zi, u2, habove, hbelow,
    zm, zo, stats, recv,
    img_sem, isend_sem, irecv_sem, rowsend_sem, rowrecv_sem, hsend_sem, hrecv_sem,
    ssem, rsem,
):
    me = lax.axis_index("sp")
    nxt, prv = me + 1, me - 1
    has_next, has_prev = me < n - 1, me > 0
    pairs = ximg.shape[1]
    half_w = tscr.shape[1] // 2
    full_w = tscr.shape[1]
    count_a = float(2 * pairs * 2 * full_w * n)
    count_b = float(2 * pairs * half_w * n)
    everything = (0, pairs)

    img_load = cuts(0, pairs, (4, 4, 4, 4))
    img_spans = cuts(0, pairs, IMG_CUTS)
    row_spans = cuts(0, pairs, ROW_CUTS)
    mid_spans = cuts(0, pairs, LATE_CUTS)

    params = [
        pltpu.make_async_copy(src, dst, w_sem.at[i])
        for i, (src, dst) in enumerate((
            (wa_hbm, wa_raw), (wd_hbm, wd_raw), (wi_hbm, wi_raw), (wm_hbm, wm_raw), (wo_hbm, wo_raw),
            (ba_hbm, ba_raw), (bd_hbm, bd_raw), (bi_hbm, bi_raw), (bm_hbm, bm_raw), (bo_hbm, bo_raw),
        ))
    ]
    local_img = [
        pltpu.make_async_copy(img_hbm.at[:, pl.ds(*span)], ximg.at[:, pl.ds(*span)], img_sem.at[c])
        for c, span in enumerate(img_load)
    ]
    barrier = pltpu.get_barrier_semaphore()
    for d in range(1, n):
        pl.semaphore_signal(barrier, inc=1, device_id={"sp": lax.rem(me + d, n)}, device_id_type=MESH)
    params[0].start()
    for copy in local_img:
        copy.start()
    for copy in params[1:]:
        copy.start()

    pl.semaphore_wait(barrier, n - 1)

    def to_dev(src, dst, send_sem, recv_sem, dev):
        return pltpu.make_async_remote_copy(
            src_ref=src, dst_ref=dst, send_sem=send_sem, recv_sem=recv_sem, device_id={"sp": dev}, device_id_type=MESH
        )

    def img_down(c):
        part = pl.ds(*img_spans[c])
        return to_dev(ximg.at[:, part, 1], xabove.at[:, part], isend_sem.at[0, c], irecv_sem.at[0, c], nxt)

    def img_up(c):
        part = pl.ds(*img_spans[c])
        return to_dev(ximg.at[:, part, 0], xbelow.at[:, part, 0], isend_sem.at[1, c], irecv_sem.at[1, c], prv)

    def row_up(c):
        part = pl.ds(*row_spans[c])
        return to_dev(ximg.at[:, part, 1], xbelow.at[:, part, 1], rowsend_sem.at[c], rowrecv_sem.at[c], prv)

    def exchange(down, up, c):
        @pl.when(has_next)
        def _():
            down(c).start()

        @pl.when(has_prev)
        def _():
            up(c).start()

    def arrived(down, up, c):
        @pl.when(has_prev)
        def _():
            down(c).wait_recv()

        @pl.when(has_next)
        def _():
            up(c).wait_recv()

    for copy in local_img:
        copy.wait()
    for c in range(len(img_spans)):
        exchange(img_down, img_up, c)
    @pl.when(me == n - 1)
    def _():
        xbelow[...] = jnp.zeros_like(xbelow)
        zthird[...] = jnp.zeros_like(zthird)
        hbelow[...] = jnp.zeros_like(hbelow)

    @pl.when(me == 0)
    def _():
        xabove[...] = jnp.zeros_like(xabove)
        habove[...] = jnp.zeros_like(habove)

    params[0].wait()
    expand_stage_a(wa_raw[...], wao_ref, wah_ref, wat_ref)

    def shift_down(y):
        row = lax.broadcasted_iota(jnp.int32, y.shape, 0)
        return jnp.where(row == 0, 0.0, pltpu.roll(y, 1, 0))

    def shift_up(y):
        row = lax.broadcasted_iota(jnp.int32, y.shape, 0)
        return jnp.where(row == y.shape[0] - 1, 0.0, pltpu.roll(y, y.shape[0] - 1, 0))

    def add_stats(acc, z):
        blocks = z.reshape(z.shape[0] // 8, 8, LANES)
        return acc[0] + jnp.sum(blocks, axis=0), acc[1] + jnp.sum(blocks * blocks, axis=0)

    zero_acc = (jnp.zeros((8, LANES), F32), jnp.zeros((8, LANES), F32))

    def start_stats(k, acc, group):
        def fold(v):
            width = group
            while width < LANES:
                v = v + pltpu.roll(v, width, 1)
                width *= 2
            return jnp.sum(v, axis=0, keepdims=True)

        mine = jnp.concatenate([fold(acc[0]), fold(acc[1])], axis=0)
        stats[k] = mine
        for d in far_first(n):
            to_dev(stats.at[k], recv.at[k, d - 1], ssem.at[k], rsem.at[k], lax.rem(me + d, n)).start()
        return mine

    def end_stats(k, mine):
        to_dev(recv.at[k], recv.at[k], ssem.at[k], rsem.at[k], me).wait_recv()
        return mine + jnp.sum(recv[k], axis=0)

    def group_stats(k, acc, group):
        return end_stats(k, start_stats(k, acc, group))

    def norm_of(k, total, count):
        moments = total * (1.0 / count)
        mean = moments[0:1]
        var = moments[1:2] - mean * mean
        scale = bn_ref[k, 0:1] * lax.rsqrt(var + NORM_EPS)
        return mean, scale, bn_ref[k, 1:2]

    def bn(z, norm):
        mean, scale, shift = norm
        return (z - mean) * scale + shift

    lane2 = lax.broadcasted_iota(jnp.int32, (half_w, 2 * LANES), 1)
    even_lane = lax.rem(lane2 // 32, 2) == 0

    def split_parity(x, a):
        tscr[a] = x.astype(F32).T
        return [tscr[a, pl.ds(0, half_w, stride=2), :], tscr[a, pl.ds(1, half_w, stride=2), :]]

    def stage_a_part(x, w_ref):
        lhs = jnp.concatenate(split_parity(x, 0), axis=1).astype(BF16)
        y = jnp.dot(lhs, w_ref[...], preferred_element_type=F32)
        cross = y[:, 2 * LANES:]
        return y[:, : 2 * LANES] + jnp.where(even_lane, shift_down(cross), shift_up(cross))

    def third_row(q, carry):
        parts = []
        for a in range(2):
            x = jnp.concatenate([ximg[a, q, 1], xbelow[a, q, 0], xbelow[a, q, 1], ximg[a, q, 0]], axis=0)
            parts += split_parity(x, a)
        y = jnp.dot(jnp.concatenate(parts, axis=1).astype(BF16), wat_ref[...], preferred_element_type=F32)
        cross = y[:, LANES:]
        zthird[q] = y[:, :LANES] + jnp.where(even_lane[:, :LANES], shift_down(cross), shift_up(cross))
        return carry

    def own_a(q, carry):
        x = jnp.concatenate([ximg[0, q].reshape(2 * 32, full_w), ximg[1, q].reshape(2 * 32, full_w)], axis=0)
        z = stage_a_part(x, wao_ref)
        za[0, q] = z[:, :LANES]
        za[1, q] = z[:, LANES:]
        return carry

    over(everything, own_a)

    for copy in params[1:]:
        copy.wait()
    expand_down(wd_raw, wdn_ref)
    expand_blocks(wi_raw, wm_raw, wo_raw, win_ref, wmid_ref, wout_ref)
    bn_ref[0] = jnp.concatenate([ba_raw[0]] * 4, axis=1)
    bn_ref[1] = bd_raw[...]
    for j in range(wi_raw.shape[0]):
        bn_ref[2 + 3 * j] = jnp.concatenate([bi_raw[j]] * 2, axis=1)
        bn_ref[3 + 3 * j] = jnp.concatenate([bm_raw[j]] * 2, axis=1)
        bn_ref[4 + 3 * j] = bo_raw[j]

    def halo_a(q, acc):
        x = jnp.concatenate([xabove[0, q], xbelow[0, q, 0], xabove[1, q], xbelow[1, q, 0]], axis=0)
        z = stage_a_part(x, wah_ref)
        z0 = za[0, q] + z[:, :LANES]
        z1 = za[1, q] + z[:, LANES:]
        za[0, q] = z0
        za[1, q] = z1
        return add_stats(add_stats(acc, z0), z1)

    acc = zero_acc
    for c, span in enumerate(img_spans):
        arrived(img_down, img_up, c)
        acc = over(span, halo_a, acc)

    mine = start_stats(0, acc, 32)
    for c in range(len(row_spans)):
        @pl.when(has_prev)
        def _():
            row_up(c).start()

    @pl.when(has_next)
    def _():
        for c, span in enumerate(row_spans[:ROWS_AHEAD]):
            row_up(c).wait_recv()
            over(span, third_row)

    norm = norm_of(0, end_stats(0, mine), count_a)

    def down(q, acc):
        third = jnp.where(has_next, jnp.maximum(bn(zthird[q], norm), 0.0), 0.0).astype(BF16)
        for a in range(2):
            own = jnp.maximum(bn(za[a, q], norm), 0.0).astype(BF16)
            y = jnp.dot(jnp.concatenate([own, third], axis=1), wdn_ref[a], preferred_element_type=F32)
            z = y[:, :LANES] + shift_up(y[:, LANES:])
            zd[a, q] = z
            acc = add_stats(acc, z)
        return acc

    acc = zero_acc
    for c, span in enumerate(row_spans):
        if c >= ROWS_AHEAD:
            @pl.when(has_next)
            def _():
                row_up(c).wait_recv()
                over(span, third_row)

        acc = over(span, down, acc)
    norm = norm_of(1, group_stats(1, acc, LANES), count_b)

    blocks = win_ref.shape[0]

    def mid_down(j):
        def copy(c):
            part = pl.ds(*mid_spans[c])
            return to_dev(u2.at[j, part], habove.at[j, part], hsend_sem.at[j, 0, c], hrecv_sem.at[j, 0, c], nxt)
        return copy

    def mid_up(j):
        def copy(c):
            part = pl.ds(*mid_spans[c])
            return to_dev(u2.at[j, part], hbelow.at[j, part], hsend_sem.at[j, 1, c], hrecv_sem.at[j, 1, c], prv)
        return copy

    for j in range(blocks):
        def layer_in(q, acc):
            parts = []
            for a in range(2):
                if j == 0:
                    t = bn(zd[a, q], norm)
                else:
                    t = bn(zo[a, q], norm) + h[a, q].astype(F32)
                t = jnp.maximum(t, 0.0).astype(BF16)
                h[a, q] = t
                parts.append(t)
            z = jnp.dot(jnp.concatenate(parts, axis=1), win_ref[j], preferred_element_type=F32)
            zi[q] = z
            return add_stats(acc, z)

        acc = over(everything, layer_in, zero_acc, 4)
        norm = norm_of(2 + 3 * j, group_stats(2 + 3 * j, acc, 64), count_b)

        def act_in(q, carry):
            u2[j, q] = jnp.maximum(bn(zi[q], norm), 0.0).astype(BF16)
            return carry

        for c, span in enumerate(mid_spans):
            over(span, act_in)
            exchange(mid_down(j), mid_up(j), c)
        def layer_mid(q, acc):
            lhs = jnp.concatenate([u2[j, q], habove[j, q], hbelow[j, q]], axis=1)
            y = jnp.dot(lhs, wmid_ref[j], preferred_element_type=F32)
            z = shift_down(y[:, :LANES]) + y[:, LANES:2 * LANES] + shift_up(y[:, 2 * LANES:])
            zm[q] = z
            return add_stats(acc, z)

        acc = zero_acc
        for c, span in enumerate(mid_spans):
            arrived(mid_down(j), mid_up(j), c)
            acc = over(span, layer_mid, acc)
        norm = norm_of(3 + 3 * j, group_stats(3 + 3 * j, acc, 64), count_b)

        def layer_out(q, acc):
            u = jnp.maximum(bn(zm[q], norm), 0.0).astype(BF16)
            y = jnp.dot(u, wout_ref[j], preferred_element_type=F32)
            for a in range(2):
                z = y[:, a * LANES:(a + 1) * LANES]
                zo[a, q] = z
                acc = add_stats(acc, z)
            return acc

        acc = over(everything, layer_out, zero_acc, 4)
        norm = norm_of(4 + 3 * j, group_stats(4 + 3 * j, acc, LANES), count_b)

    def final(q, carry):
        for a in range(2):
            out_ref[a, q] = jnp.maximum(bn(zo[a, q], norm) + h[a, q].astype(F32), 0.0).astype(BF16)
        return carry

    over(everything, final, 0, 2)

    for k in range(stats.shape[0]):
        to_dev(recv.at[k], recv.at[k], ssem.at[k], rsem.at[k], me).wait_send()

    @pl.when(has_next)
    def _():
        for c in range(len(img_spans)):
            img_down(c).wait_send()
        for j in range(blocks):
            for c in range(len(mid_spans)):
                mid_down(j)(c).wait_send()

    @pl.when(has_prev)
    def _():
        for c in range(len(img_spans)):
            img_up(c).wait_send()
        for c in range(len(row_spans)):
            row_up(c).wait_send()
        for j in range(blocks):
            for c in range(len(mid_spans)):
                mid_up(j)(c).wait_send()


def solution(mesh):
    n = mesh.shape["sp"]

    def forward(images, w_a, bn_a, w_down, bn_down, w_in, bn_in, w_mid, bn_mid, w_out, bn_out):
        count, rows, width, chan_a = images.shape
        pairs, half_w = count // 2, width // 2
        blocks = w_in.shape[0]
        img = jnp.transpose(images, (0, 1, 3, 2)).reshape(2, pairs, rows, chan_a, width)
        taps = w_a.shape[1] * w_a.shape[2]
        raw = [
            w_a.reshape(taps * chan_a, chan_a), w_down.reshape(taps, chan_a, LANES), jnp.transpose(w_in, (0, 2, 1)),
            w_mid.reshape(blocks, taps, 64, 64), w_out, bn_a, bn_down, bn_in, bn_mid, bn_out,
        ]
        steps = 2 + 3 * blocks

        dma = pltpu.SemaphoreType.DMA
        out = pl.pallas_call(
            functools.partial(kernel, n),
            out_shape=pltpu.VMEM((2, pairs, half_w, LANES), BF16),
            in_specs=[pl.BlockSpec(memory_space=pltpu.HBM)] * 11,
            out_specs=pl.BlockSpec(memory_space=pltpu.VMEM),
            scratch_shapes=[pltpu.VMEM(x.shape, x.dtype) for x in raw] + [
                dma((len(raw),)),
                pltpu.VMEM((2 * LANES, 4 * LANES), BF16),
                pltpu.VMEM((2 * LANES, 4 * LANES), BF16),
                pltpu.VMEM((4 * LANES, 2 * LANES), BF16),
                pltpu.VMEM((2, 2 * LANES, 2 * LANES), BF16),
                pltpu.VMEM((blocks, 2 * LANES, LANES), BF16),
                pltpu.VMEM((blocks, 3 * LANES, 3 * LANES), BF16),
                pltpu.VMEM((blocks, LANES, 2 * LANES), BF16),
                pltpu.VMEM((steps, 2, LANES), F32),
                pltpu.VMEM((2, pairs, rows, chan_a, width), BF16),
                pltpu.VMEM((2, pairs, chan_a, width), BF16),
                pltpu.VMEM((2, pairs, rows, chan_a, width), BF16),
                pltpu.VMEM((2, width, LANES), F32),
                pltpu.VMEM((2, pairs, half_w, LANES), F32),
                pltpu.VMEM((pairs, half_w, LANES), F32),
                pltpu.VMEM((2, pairs, half_w, LANES), F32),
                pltpu.VMEM((2, pairs, half_w, LANES), BF16),
                pltpu.VMEM((pairs, half_w, LANES), F32),
                pltpu.VMEM((blocks, pairs, half_w, LANES), BF16),
                pltpu.VMEM((blocks, pairs, half_w, LANES), BF16),
                pltpu.VMEM((blocks, pairs, half_w, LANES), BF16),
                pltpu.VMEM((pairs, half_w, LANES), F32),
                pltpu.VMEM((2, pairs, half_w, LANES), F32),
                pltpu.VMEM((steps, 2, LANES), F32),
                pltpu.VMEM((steps, n - 1, 2, LANES), F32),
                dma((4,)),
                dma((2, len(IMG_CUTS))),
                dma((2, len(IMG_CUTS))),
                dma((len(ROW_CUTS),)),
                dma((len(ROW_CUTS),)),
                dma((blocks, 2, len(LATE_CUTS))),
                dma((blocks, 2, len(LATE_CUTS))),
                dma((steps,)),
                dma((steps,)),
            ],
            compiler_params=pltpu.CompilerParams(
                collective_id=0, has_side_effects=True, vmem_limit_bytes=52 * 1024 * 1024
            ),
        )(img, *raw)
        return out.reshape(count, rows // 2, half_w, LANES)

    act_spec = P("dp", "sp", None, None)
    return jax.shard_map(forward, mesh=mesh, in_specs=(act_spec,) + (P(),) * 10, out_specs=act_spec, check_vma=False)
```

```python
import functools
import math

import jax
import jax.numpy as jnp
from jax import lax
from jax.experimental import pallas as pl
from jax.experimental.pallas import tpu as pltpu
from jax.sharding import PartitionSpec as P

NORM_EPS = 1e-5
MESH = pl.DeviceIdType.MESH
LANES = 128
IMG_CUTS = (6, 5, 4, 1)
ROW_CUTS = (6, 5, 4, 1)
ROWS_AHEAD = 2
LATE_CUTS = (3, 7, 5, 1)
F32 = jnp.float32
BF16 = jnp.bfloat16


def cuts(first, last, weights):
    total, seen, edge, spans = sum(weights), 0, first, []
    for weight in weights:
        seen += weight
        end = first + (last - first) * seen // total
        if end > edge:
            spans.append((edge, end - edge))
        edge = end
    return spans


def over(span, body, carry=0, step=1):
    start, length = span
    trips = length // step

    def trip(i, carry):
        for k in range(step):
            carry = body(start + i * step + k, carry)
        return carry

    if trips == 1:
        carry = trip(0, carry)
    elif trips > 1:
        carry = lax.fori_loop(0, trips, trip, carry)
    for q in range(start + trips * step, start + length):
        carry = body(q, carry)
    return carry


def far_first(n):
    side = max(1, math.isqrt(n // 2))

    def hops(d):
        x, y = d // 2 % side, d // (2 * side)
        return min(x, side - x) + min(y, abs(side - y))

    return sorted(range(1, n), key=lambda d: (-hops(d), d))


def placement(size, copies):
    row = lax.broadcasted_iota(jnp.int32, (size, copies * LANES), 0)
    lane = lax.broadcasted_iota(jnp.int32, (size, copies * LANES), 1)
    hit = lane == row
    for i in range(1, copies):
        hit = jnp.logical_or(hit, lane == row + i * (LANES + size))
    return hit.astype(F32).astype(BF16)


def expand_stage_a(w, own_ref, halo_ref, third_ref):
    spread = jnp.dot(w, placement(32, 4), preferred_element_type=F32)
    own_ref[...] = jnp.zeros_like(own_ref)
    halo_ref[...] = jnp.zeros_like(halo_ref)
    for ref, halo in ((own_ref, False), (halo_ref, True)):
        for pi in range(2):
            for ri in range(2):
                for shift in range(2):
                    total = jnp.zeros((32, LANES), F32)
                    for ro in range(2):
                        for po in range(2):
                            if halo and ri != ro:
                                continue
                            if shift and pi == po:
                                continue
                            ky = 2 * ri if halo else ri - ro + 1
                            kx = (0 if pi == 1 else 2) if shift else pi - po + 1
                            tap, i = ky * 3 + kx, ro * 2 + po
                            total += spread[tap * 32:(tap + 1) * 32, i * LANES:(i + 1) * LANES]
                    block = total.astype(BF16)
                    for a in range(2):
                        row, col = ((pi * 2 + a) * 2 + ri) * 32, (shift * 2 + a) * LANES
                        ref[row:row + 32, col:col + LANES] = block
    third_ref[...] = jnp.zeros_like(third_ref)
    for a in range(2):
        for pi in range(2):
            for ky in range(3):
                for shift in range(2):
                    total = jnp.zeros((32, LANES), F32)
                    for po in range(2):
                        if shift and pi == po:
                            continue
                        kx = (0 if pi == 1 else 2) if shift else pi - po + 1
                        tap, i = ky * 3 + kx, a * 2 + po
                        total += spread[tap * 32:(tap + 1) * 32, i * LANES:(i + 1) * LANES]
                    row = ((a * 2 + pi) * 4 + ky) * 32
                    third_ref[row:row + 32, shift * LANES:(shift + 1) * LANES] = total.astype(BF16)


def expand_down(w_ref, down_ref):
    down_ref[...] = jnp.zeros_like(down_ref)
    for par in range(2):
        for shift in range(2 - par):
            kx, col = 2 if shift else par, shift * LANES
            for a in range(2):
                for row in range(2):
                    at = (row * 2 + par) * 32
                    down_ref[a, at:at + 32, col:col + LANES] = w_ref[row * 3 + kx]
                at = LANES + (a * 2 + par) * 32
                down_ref[a, at:at + 32, col:col + LANES] = w_ref[6 + kx]


def expand_blocks(w_in_ref, w_mid_ref, w_out_ref, win_ref, wmid_ref, wout_ref):
    spot = placement(64, 2)
    for j in range(win_ref.shape[0]):
        w_in = w_in_ref[j].astype(F32).T.astype(BF16)
        spread = jnp.dot(w_in, spot, preferred_element_type=F32).astype(BF16)
        for a in range(2):
            win_ref[j, a * LANES:(a + 1) * LANES, :] = spread[:, a * LANES:(a + 1) * LANES]
        for src, ky in enumerate((1, 0, 2)):
            for kx in range(3):
                spread = jnp.dot(w_mid_ref[j, ky * 3 + kx], spot, preferred_element_type=F32).astype(BF16)
                for a in range(2):
                    at = (src * 2 + a) * 64
                    wmid_ref[j, at:at + 64, kx * LANES:(kx + 1) * LANES] = spread[:, a * LANES:(a + 1) * LANES]
        zeros = jnp.zeros((64, LANES), BF16)
        for a in range(2):
            for b in range(2):
                wout_ref[j, a * 64:(a + 1) * 64, b * LANES:(b + 1) * LANES] = w_out_ref[j] if a == b else zeros


def kernel(
    n, img_hbm, wa_hbm, wd_hbm, wi_hbm, wm_hbm, wo_hbm, ba_hbm, bd_hbm, bi_hbm, bm_hbm, bo_hbm, out_ref,
    wa_raw, wd_raw, wi_raw, wm_raw, wo_raw, ba_raw, bd_raw, bi_raw, bm_raw, bo_raw, w_sem,
    wao_ref, wah_ref, wat_ref, wdn_ref, win_ref, wmid_ref, wout_ref, bn_ref,
    ximg, xabove, xbelow, tscr, za, zthird, zd, h, zi, u2, habove, hbelow,
    zm, zo, stats, recv,
    img_sem, isend_sem, irecv_sem, rowsend_sem, rowrecv_sem, hsend_sem, hrecv_sem,
    ssem, rsem,
):
    me = lax.axis_index("sp")
    nxt, prv = me + 1, me - 1
    has_next, has_prev = me < n - 1, me > 0
    pairs = ximg.shape[1]
    half_w = tscr.shape[1] // 2
    full_w = tscr.shape[1]
    count_a = float(2 * pairs * 2 * full_w * n)
    count_b = float(2 * pairs * half_w * n)
    everything = (0, pairs)

    img_load = cuts(0, pairs, (4, 4, 4, 4))
    img_spans = cuts(0, pairs, IMG_CUTS)
    row_spans = cuts(0, pairs, ROW_CUTS)
    mid_spans = cuts(0, pairs, LATE_CUTS)

    params = [
        pltpu.make_async_copy(src, dst, w_sem.at[i])
        for i, (src, dst) in enumerate((
            (wa_hbm, wa_raw), (wd_hbm, wd_raw), (wi_hbm, wi_raw), (wm_hbm, wm_raw), (wo_hbm, wo_raw),
            (ba_hbm, ba_raw), (bd_hbm, bd_raw), (bi_hbm, bi_raw), (bm_hbm, bm_raw), (bo_hbm, bo_raw),
        ))
    ]
    local_img = [
        pltpu.make_async_copy(img_hbm.at[:, pl.ds(*span)], ximg.at[:, pl.ds(*span)], img_sem.at[c])
        for c, span in enumerate(img_load)
    ]
    barrier = pltpu.get_barrier_semaphore()
    for copy in local_img:
        copy.start()
    for d in far_first(n):
        pl.semaphore_signal(barrier, inc=1, device_id={"sp": lax.rem(me + d, n)}, device_id_type=MESH)
    params[0].start()
    for copy in params[1:]:
        copy.start()

    pl.semaphore_wait(barrier, n - 1)

    def to_dev(src, dst, send_sem, recv_sem, dev):
        return pltpu.make_async_remote_copy(
            src_ref=src, dst_ref=dst, send_sem=send_sem, recv_sem=recv_sem, device_id={"sp": dev}, device_id_type=MESH
        )

    def img_down(c):
        part = pl.ds(*img_spans[c])
        return to_dev(ximg.at[:, part, 1], xabove.at[:, part], isend_sem.at[0, c], irecv_sem.at[0, c], nxt)

    def img_up(c):
        part = pl.ds(*img_spans[c])
        return to_dev(ximg.at[:, part, 0], xbelow.at[:, part, 0], isend_sem.at[1, c], irecv_sem.at[1, c], prv)

    def row_up(c):
        part = pl.ds(*row_spans[c])
        return to_dev(ximg.at[:, part, 1], xbelow.at[:, part, 1], rowsend_sem.at[c], rowrecv_sem.at[c], prv)

    def exchange(down, up, c):
        @pl.when(has_next)
        def _():
            down(c).start()

        @pl.when(has_prev)
        def _():
            up(c).start()

    def arrived(down, up, c):
        @pl.when(has_prev)
        def _():
            down(c).wait_recv()

        @pl.when(has_next)
        def _():
            up(c).wait_recv()

    for copy in local_img:
        copy.wait()
    for c in range(len(img_spans)):
        exchange(img_down, img_up, c)
    @pl.when(me == n - 1)
    def _():
        xbelow[...] = jnp.zeros_like(xbelow)
        zthird[...] = jnp.zeros_like(zthird)
        hbelow[...] = jnp.zeros_like(hbelow)

    @pl.when(me == 0)
    def _():
        xabove[...] = jnp.zeros_like(xabove)
        habove[...] = jnp.zeros_like(habove)

    params[0].wait()
    expand_stage_a(wa_raw[...], wao_ref, wah_ref, wat_ref)

    def shift_down(y):
        row = lax.broadcasted_iota(jnp.int32, y.shape, 0)
        return jnp.where(row == 0, 0.0, pltpu.roll(y, 1, 0))

    def shift_up(y):
        row = lax.broadcasted_iota(jnp.int32, y.shape, 0)
        return jnp.where(row == y.shape[0] - 1, 0.0, pltpu.roll(y, y.shape[0] - 1, 0))

    def add_stats(acc, z):
        blocks = z.reshape(z.shape[0] // 8, 8, LANES)
        return acc[0] + jnp.sum(blocks, axis=0), acc[1] + jnp.sum(blocks * blocks, axis=0)

    zero_acc = (jnp.zeros((8, LANES), F32), jnp.zeros((8, LANES), F32))

    def start_stats(k, acc, group):
        def fold(v):
            width = group
            while width < LANES:
                v = v + pltpu.roll(v, width, 1)
                width *= 2
            return jnp.sum(v, axis=0, keepdims=True)

        mine = jnp.concatenate([fold(acc[0]), fold(acc[1])], axis=0)
        stats[k] = mine
        for d in far_first(n):
            to_dev(stats.at[k], recv.at[k, d - 1], ssem.at[k], rsem.at[k], lax.rem(me + d, n)).start()
        return mine

    def end_stats(k, mine):
        to_dev(recv.at[k], recv.at[k], ssem.at[k], rsem.at[k], me).wait_recv()
        return mine + jnp.sum(recv[k], axis=0)

    def group_stats(k, acc, group):
        return end_stats(k, start_stats(k, acc, group))

    def norm_of(k, total, count):
        moments = total * (1.0 / count)
        mean = moments[0:1]
        var = moments[1:2] - mean * mean
        scale = bn_ref[k, 0:1] * lax.rsqrt(var + NORM_EPS)
        return mean, scale, bn_ref[k, 1:2]

    def bn(z, norm):
        mean, scale, shift = norm
        return (z - mean) * scale + shift

    lane2 = lax.broadcasted_iota(jnp.int32, (half_w, 2 * LANES), 1)
    even_lane = lax.rem(lane2 // 32, 2) == 0

    def split_parity(x, a):
        tscr[a] = x.astype(F32).T
        return [tscr[a, pl.ds(0, half_w, stride=2), :], tscr[a, pl.ds(1, half_w, stride=2), :]]

    def stage_a_part(x, w_ref):
        lhs = jnp.concatenate(split_parity(x, 0), axis=1).astype(BF16)
        y = jnp.dot(lhs, w_ref[...], preferred_element_type=F32)
        cross = y[:, 2 * LANES:]
        return y[:, : 2 * LANES] + jnp.where(even_lane, shift_down(cross), shift_up(cross))

    def third_row(q, carry):
        parts = []
        for a in range(2):
            x = jnp.concatenate([ximg[a, q, 1], xbelow[a, q, 0], xbelow[a, q, 1], ximg[a, q, 0]], axis=0)
            parts += split_parity(x, a)
        y = jnp.dot(jnp.concatenate(parts, axis=1).astype(BF16), wat_ref[...], preferred_element_type=F32)
        cross = y[:, LANES:]
        zthird[q] = y[:, :LANES] + jnp.where(even_lane[:, :LANES], shift_down(cross), shift_up(cross))
        return carry

    def own_a(q, carry):
        x = jnp.concatenate([ximg[0, q].reshape(2 * 32, full_w), ximg[1, q].reshape(2 * 32, full_w)], axis=0)
        z = stage_a_part(x, wao_ref)
        za[0, q] = z[:, :LANES]
        za[1, q] = z[:, LANES:]
        return carry

    over(everything, own_a)

    for copy in params[1:]:
        copy.wait()
    expand_down(wd_raw, wdn_ref)
    expand_blocks(wi_raw, wm_raw, wo_raw, win_ref, wmid_ref, wout_ref)
    bn_ref[0] = jnp.concatenate([ba_raw[0]] * 4, axis=1)
    bn_ref[1] = bd_raw[...]
    for j in range(wi_raw.shape[0]):
        bn_ref[2 + 3 * j] = jnp.concatenate([bi_raw[j]] * 2, axis=1)
        bn_ref[3 + 3 * j] = jnp.concatenate([bm_raw[j]] * 2, axis=1)
        bn_ref[4 + 3 * j] = bo_raw[j]

    def halo_a(q, acc):
        x = jnp.concatenate([xabove[0, q], xbelow[0, q, 0], xabove[1, q], xbelow[1, q, 0]], axis=0)
        z = stage_a_part(x, wah_ref)
        z0 = za[0, q] + z[:, :LANES]
        z1 = za[1, q] + z[:, LANES:]
        za[0, q] = z0
        za[1, q] = z1
        return add_stats(add_stats(acc, z0), z1)

    acc = zero_acc
    for c, span in enumerate(img_spans):
        arrived(img_down, img_up, c)
        acc = over(span, halo_a, acc)

    mine = start_stats(0, acc, 32)
    for c in range(len(row_spans)):
        @pl.when(has_prev)
        def _():
            row_up(c).start()

    @pl.when(has_next)
    def _():
        for c, span in enumerate(row_spans[:ROWS_AHEAD]):
            row_up(c).wait_recv()
            over(span, third_row)

    norm = norm_of(0, end_stats(0, mine), count_a)

    def down(q, acc):
        third = jnp.where(has_next, jnp.maximum(bn(zthird[q], norm), 0.0), 0.0).astype(BF16)
        for a in range(2):
            own = jnp.maximum(bn(za[a, q], norm), 0.0).astype(BF16)
            y = jnp.dot(jnp.concatenate([own, third], axis=1), wdn_ref[a], preferred_element_type=F32)
            z = y[:, :LANES] + shift_up(y[:, LANES:])
            zd[a, q] = z
            acc = add_stats(acc, z)
        return acc

    acc = zero_acc
    for c, span in enumerate(row_spans):
        if c >= ROWS_AHEAD:
            @pl.when(has_next)
            def _():
                row_up(c).wait_recv()
                over(span, third_row)

        acc = over(span, down, acc)
    norm = norm_of(1, group_stats(1, acc, LANES), count_b)

    blocks = win_ref.shape[0]

    def mid_down(j):
        def copy(c):
            part = pl.ds(*mid_spans[c])
            return to_dev(u2.at[j, part], habove.at[j, part], hsend_sem.at[j, 0, c], hrecv_sem.at[j, 0, c], nxt)
        return copy

    def mid_up(j):
        def copy(c):
            part = pl.ds(*mid_spans[c])
            return to_dev(u2.at[j, part], hbelow.at[j, part], hsend_sem.at[j, 1, c], hrecv_sem.at[j, 1, c], prv)
        return copy

    for j in range(blocks):
        def layer_in(q, acc):
            parts = []
            for a in range(2):
                if j == 0:
                    t = bn(zd[a, q], norm)
                else:
                    t = bn(zo[a, q], norm) + h[a, q].astype(F32)
                t = jnp.maximum(t, 0.0).astype(BF16)
                h[a, q] = t
                parts.append(t)
            z = jnp.dot(jnp.concatenate(parts, axis=1), win_ref[j], preferred_element_type=F32)
            zi[q] = z
            return add_stats(acc, z)

        acc = over(everything, layer_in, zero_acc, 4)
        norm = norm_of(2 + 3 * j, group_stats(2 + 3 * j, acc, 64), count_b)

        def act_in(q, carry):
            u2[j, q] = jnp.maximum(bn(zi[q], norm), 0.0).astype(BF16)
            return carry

        for c, span in enumerate(mid_spans):
            over(span, act_in)
            exchange(mid_down(j), mid_up(j), c)
        def layer_mid(q, acc):
            lhs = jnp.concatenate([u2[j, q], habove[j, q], hbelow[j, q]], axis=1)
            y = jnp.dot(lhs, wmid_ref[j], preferred_element_type=F32)
            z = shift_down(y[:, :LANES]) + y[:, LANES:2 * LANES] + shift_up(y[:, 2 * LANES:])
            zm[q] = z
            return add_stats(acc, z)

        acc = zero_acc
        for c, span in enumerate(mid_spans):
            arrived(mid_down(j), mid_up(j), c)
            acc = over(span, layer_mid, acc)
        norm = norm_of(3 + 3 * j, group_stats(3 + 3 * j, acc, 64), count_b)

        def layer_out(q, acc):
            u = jnp.maximum(bn(zm[q], norm), 0.0).astype(BF16)
            y = jnp.dot(u, wout_ref[j], preferred_element_type=F32)
            for a in range(2):
                z = y[:, a * LANES:(a + 1) * LANES]
                zo[a, q] = z
                acc = add_stats(acc, z)
            return acc

        acc = over(everything, layer_out, zero_acc, 4)
        norm = norm_of(4 + 3 * j, group_stats(4 + 3 * j, acc, LANES), count_b)

    def final(q, carry):
        for a in range(2):
            out_ref[a, q] = jnp.maximum(bn(zo[a, q], norm) + h[a, q].astype(F32), 0.0).astype(BF16)
        return carry

    over(everything, final, 0, 2)

    for k in range(stats.shape[0]):
        to_dev(recv.at[k], recv.at[k], ssem.at[k], rsem.at[k], me).wait_send()

    @pl.when(has_next)
    def _():
        for c in range(len(img_spans)):
            img_down(c).wait_send()
        for j in range(blocks):
            for c in range(len(mid_spans)):
                mid_down(j)(c).wait_send()

    @pl.when(has_prev)
    def _():
        for c in range(len(img_spans)):
            img_up(c).wait_send()
        for c in range(len(row_spans)):
            row_up(c).wait_send()
        for j in range(blocks):
            for c in range(len(mid_spans)):
                mid_up(j)(c).wait_send()


def solution(mesh):
    n = mesh.shape["sp"]

    def forward(images, w_a, bn_a, w_down, bn_down, w_in, bn_in, w_mid, bn_mid, w_out, bn_out):
        count, rows, width, chan_a = images.shape
        pairs, half_w = count // 2, width // 2
        blocks = w_in.shape[0]
        img = jnp.transpose(images, (0, 1, 3, 2)).reshape(2, pairs, rows, chan_a, width)
        taps = w_a.shape[1] * w_a.shape[2]
        raw = [
            w_a.reshape(taps * chan_a, chan_a), w_down.reshape(taps, chan_a, LANES), jnp.transpose(w_in, (0, 2, 1)),
            w_mid.reshape(blocks, taps, 64, 64), w_out, bn_a, bn_down, bn_in, bn_mid, bn_out,
        ]
        steps = 2 + 3 * blocks

        dma = pltpu.SemaphoreType.DMA
        out = pl.pallas_call(
            functools.partial(kernel, n),
            out_shape=pltpu.VMEM((2, pairs, half_w, LANES), BF16),
            in_specs=[pl.BlockSpec(memory_space=pltpu.HBM)] * 11,
            out_specs=pl.BlockSpec(memory_space=pltpu.VMEM),
            scratch_shapes=[pltpu.VMEM(x.shape, x.dtype) for x in raw] + [
                dma((len(raw),)),
                pltpu.VMEM((2 * LANES, 4 * LANES), BF16),
                pltpu.VMEM((2 * LANES, 4 * LANES), BF16),
                pltpu.VMEM((4 * LANES, 2 * LANES), BF16),
                pltpu.VMEM((2, 2 * LANES, 2 * LANES), BF16),
                pltpu.VMEM((blocks, 2 * LANES, LANES), BF16),
                pltpu.VMEM((blocks, 3 * LANES, 3 * LANES), BF16),
                pltpu.VMEM((blocks, LANES, 2 * LANES), BF16),
                pltpu.VMEM((steps, 2, LANES), F32),
                pltpu.VMEM((2, pairs, rows, chan_a, width), BF16),
                pltpu.VMEM((2, pairs, chan_a, width), BF16),
                pltpu.VMEM((2, pairs, rows, chan_a, width), BF16),
                pltpu.VMEM((2, width, LANES), F32),
                pltpu.VMEM((2, pairs, half_w, LANES), F32),
                pltpu.VMEM((pairs, half_w, LANES), F32),
                pltpu.VMEM((2, pairs, half_w, LANES), F32),
                pltpu.VMEM((2, pairs, half_w, LANES), BF16),
                pltpu.VMEM((pairs, half_w, LANES), F32),
                pltpu.VMEM((blocks, pairs, half_w, LANES), BF16),
                pltpu.VMEM((blocks, pairs, half_w, LANES), BF16),
                pltpu.VMEM((blocks, pairs, half_w, LANES), BF16),
                pltpu.VMEM((pairs, half_w, LANES), F32),
                pltpu.VMEM((2, pairs, half_w, LANES), F32),
                pltpu.VMEM((steps, 2, LANES), F32),
                pltpu.VMEM((steps, n - 1, 2, LANES), F32),
                dma((4,)),
                dma((2, len(IMG_CUTS))),
                dma((2, len(IMG_CUTS))),
                dma((len(ROW_CUTS),)),
                dma((len(ROW_CUTS),)),
                dma((blocks, 2, len(LATE_CUTS))),
                dma((blocks, 2, len(LATE_CUTS))),
                dma((steps,)),
                dma((steps,)),
            ],
            compiler_params=pltpu.CompilerParams(
                collective_id=0, has_side_effects=True, vmem_limit_bytes=52 * 1024 * 1024
            ),
        )(img, *raw)
        return out.reshape(count, rows // 2, half_w, LANES)

    act_spec = P("dp", "sp", None, None)
    return jax.shard_map(forward, mesh=mesh, in_specs=(act_spec,) + (P(),) * 10, out_specs=act_spec, check_vma=False)
```

```python
import functools

import jax
import jax.numpy as jnp
from jax import lax
from jax.experimental import pallas as pl
from jax.experimental.pallas import tpu as pltpu
from jax.sharding import PartitionSpec as P

NORM_EPS = 1e-5
MESH = pl.DeviceIdType.MESH
LANES = 128
IMG_CUTS = (5, 5, 4, 2)
ROW_CUTS = (5, 5, 4, 2)
ROWS_AHEAD = 2
LATE_CUTS = (8, 6, 2)
F32 = jnp.float32
BF16 = jnp.bfloat16


def cuts(first, last, weights):
    total, seen, edge, spans = sum(weights), 0, first, []
    for weight in weights:
        seen += weight
        end = first + (last - first) * seen // total
        if end > edge:
            spans.append((edge, end - edge))
        edge = end
    return spans


def over(span, body, carry=0, step=1):
    start, length = span
    trips = length // step

    def trip(i, carry):
        for k in range(step):
            carry = body(start + i * step + k, carry)
        return carry

    if trips == 1:
        carry = trip(0, carry)
    elif trips > 1:
        carry = lax.fori_loop(0, trips, trip, carry)
    for q in range(start + trips * step, start + length):
        carry = body(q, carry)
    return carry


def far_first(n):
    return sorted(range(1, n), key=lambda d: abs(2 * d - n))


def placement(size, copies):
    row = lax.broadcasted_iota(jnp.int32, (size, copies * LANES), 0)
    lane = lax.broadcasted_iota(jnp.int32, (size, copies * LANES), 1)
    hit = lane == row
    for i in range(1, copies):
        hit = jnp.logical_or(hit, lane == row + i * (LANES + size))
    return hit.astype(F32).astype(BF16)


def expand_stage_a(w, own_ref, halo_ref, third_ref):
    spread = jnp.dot(w, placement(32, 4), preferred_element_type=F32)
    own_ref[...] = jnp.zeros_like(own_ref)
    halo_ref[...] = jnp.zeros_like(halo_ref)
    for ref, halo in ((own_ref, False), (halo_ref, True)):
        for pi in range(2):
            for ri in range(2):
                for shift in range(2):
                    total = jnp.zeros((32, LANES), F32)
                    for ro in range(2):
                        for po in range(2):
                            if halo and ri != ro:
                                continue
                            if shift and pi == po:
                                continue
                            ky = 2 * ri if halo else ri - ro + 1
                            kx = (0 if pi == 1 else 2) if shift else pi - po + 1
                            tap, i = ky * 3 + kx, ro * 2 + po
                            total += spread[tap * 32:(tap + 1) * 32, i * LANES:(i + 1) * LANES]
                    block = total.astype(BF16)
                    for a in range(2):
                        row, col = ((pi * 2 + a) * 2 + ri) * 32, (shift * 2 + a) * LANES
                        ref[row:row + 32, col:col + LANES] = block
    third_ref[...] = jnp.zeros_like(third_ref)
    for a in range(2):
        for pi in range(2):
            for ky in range(3):
                for shift in range(2):
                    total = jnp.zeros((32, LANES), F32)
                    for po in range(2):
                        if shift and pi == po:
                            continue
                        kx = (0 if pi == 1 else 2) if shift else pi - po + 1
                        tap, i = ky * 3 + kx, a * 2 + po
                        total += spread[tap * 32:(tap + 1) * 32, i * LANES:(i + 1) * LANES]
                    row = ((a * 2 + pi) * 4 + ky) * 32
                    third_ref[row:row + 32, shift * LANES:(shift + 1) * LANES] = total.astype(BF16)


def expand_down(w_ref, down_ref):
    down_ref[...] = jnp.zeros_like(down_ref)
    for par in range(2):
        for shift in range(2 - par):
            kx, col = 2 if shift else par, shift * LANES
            for a in range(2):
                for row in range(2):
                    at = (row * 2 + par) * 32
                    down_ref[a, at:at + 32, col:col + LANES] = w_ref[row * 3 + kx]
                at = LANES + (a * 2 + par) * 32
                down_ref[a, at:at + 32, col:col + LANES] = w_ref[6 + kx]


def expand_blocks(w_in_ref, w_mid_ref, w_out_ref, win_ref, wmid_ref, wout_ref):
    spot = placement(64, 2)
    for j in range(win_ref.shape[0]):
        w_in = w_in_ref[j].astype(F32).T.astype(BF16)
        spread = jnp.dot(w_in, spot, preferred_element_type=F32).astype(BF16)
        for a in range(2):
            win_ref[j, a * LANES:(a + 1) * LANES, :] = spread[:, a * LANES:(a + 1) * LANES]
        for src, ky in enumerate((1, 0, 2)):
            for kx in range(3):
                spread = jnp.dot(w_mid_ref[j, ky * 3 + kx], spot, preferred_element_type=F32).astype(BF16)
                for a in range(2):
                    at = (src * 2 + a) * 64
                    wmid_ref[j, at:at + 64, kx * LANES:(kx + 1) * LANES] = spread[:, a * LANES:(a + 1) * LANES]
        zeros = jnp.zeros((64, LANES), BF16)
        for a in range(2):
            for b in range(2):
                wout_ref[j, a * 64:(a + 1) * 64, b * LANES:(b + 1) * LANES] = w_out_ref[j] if a == b else zeros


def kernel(
    n, img_hbm, wa_hbm, wd_hbm, wi_hbm, wm_hbm, wo_hbm, ba_hbm, bd_hbm, bi_hbm, bm_hbm, bo_hbm, out_ref,
    wa_raw, wd_raw, wi_raw, wm_raw, wo_raw, ba_raw, bd_raw, bi_raw, bm_raw, bo_raw, w_sem,
    wao_ref, wah_ref, wat_ref, wdn_ref, win_ref, wmid_ref, wout_ref, bn_ref,
    ximg, xabove, xbelow, tscr, za, zthird, zd, h, zi, u2, habove, hbelow,
    zm, zo, stats, recv,
    img_sem, isend_sem, irecv_sem, rowsend_sem, rowrecv_sem, hsend_sem, hrecv_sem,
    ssem, rsem,
):
    me = lax.axis_index("sp")
    nxt, prv = me + 1, me - 1
    has_next, has_prev = me < n - 1, me > 0
    pairs = ximg.shape[1]
    half_w = tscr.shape[1] // 2
    full_w = tscr.shape[1]
    count_a = float(2 * pairs * 2 * full_w * n)
    count_b = float(2 * pairs * half_w * n)
    everything = (0, pairs)

    img_load = cuts(0, pairs, (4, 4, 4, 4))
    img_spans = cuts(0, pairs, IMG_CUTS)
    row_spans = cuts(0, pairs, ROW_CUTS)
    mid_spans = cuts(0, pairs, LATE_CUTS)

    params = [
        pltpu.make_async_copy(src, dst, w_sem.at[i])
        for i, (src, dst) in enumerate((
            (wa_hbm, wa_raw), (wd_hbm, wd_raw), (wi_hbm, wi_raw), (wm_hbm, wm_raw), (wo_hbm, wo_raw),
            (ba_hbm, ba_raw), (bd_hbm, bd_raw), (bi_hbm, bi_raw), (bm_hbm, bm_raw), (bo_hbm, bo_raw),
        ))
    ]
    local_img = [
        pltpu.make_async_copy(img_hbm.at[:, pl.ds(*span)], ximg.at[:, pl.ds(*span)], img_sem.at[c])
        for c, span in enumerate(img_load)
    ]
    barrier = pltpu.get_barrier_semaphore()
    for d in range(1, n):
        pl.semaphore_signal(barrier, inc=1, device_id={"sp": lax.rem(me + d, n)}, device_id_type=MESH)
    params[0].start()
    for copy in local_img:
        copy.start()
    for copy in params[1:]:
        copy.start()

    pl.semaphore_wait(barrier, n - 1)

    def to_dev(src, dst, send_sem, recv_sem, dev):
        return pltpu.make_async_remote_copy(
            src_ref=src, dst_ref=dst, send_sem=send_sem, recv_sem=recv_sem, device_id={"sp": dev}, device_id_type=MESH
        )

    def img_down(c):
        part = pl.ds(*img_spans[c])
        return to_dev(ximg.at[:, part, 1], xabove.at[:, part], isend_sem.at[0, c], irecv_sem.at[0, c], nxt)

    def img_up(c):
        part = pl.ds(*img_spans[c])
        return to_dev(ximg.at[:, part, 0], xbelow.at[:, part, 0], isend_sem.at[1, c], irecv_sem.at[1, c], prv)

    def row_up(c):
        part = pl.ds(*row_spans[c])
        return to_dev(ximg.at[:, part, 1], xbelow.at[:, part, 1], rowsend_sem.at[c], rowrecv_sem.at[c], prv)

    def exchange(down, up, c):
        @pl.when(has_next)
        def _():
            down(c).start()

        @pl.when(has_prev)
        def _():
            up(c).start()

    def arrived(down, up, c):
        @pl.when(has_prev)
        def _():
            down(c).wait_recv()

        @pl.when(has_next)
        def _():
            up(c).wait_recv()

    for copy in local_img:
        copy.wait()
    for c in range(len(img_spans)):
        exchange(img_down, img_up, c)
    @pl.when(me == n - 1)
    def _():
        xbelow[...] = jnp.zeros_like(xbelow)
        zthird[...] = jnp.zeros_like(zthird)
        hbelow[...] = jnp.zeros_like(hbelow)

    @pl.when(me == 0)
    def _():
        xabove[...] = jnp.zeros_like(xabove)
        habove[...] = jnp.zeros_like(habove)

    params[0].wait()
    expand_stage_a(wa_raw[...], wao_ref, wah_ref, wat_ref)

    def shift_down(y):
        row = lax.broadcasted_iota(jnp.int32, y.shape, 0)
        return jnp.where(row == 0, 0.0, pltpu.roll(y, 1, 0))

    def shift_up(y):
        row = lax.broadcasted_iota(jnp.int32, y.shape, 0)
        return jnp.where(row == y.shape[0] - 1, 0.0, pltpu.roll(y, y.shape[0] - 1, 0))

    def add_stats(acc, z):
        blocks = z.reshape(z.shape[0] // 8, 8, LANES)
        return acc[0] + jnp.sum(blocks, axis=0), acc[1] + jnp.sum(blocks * blocks, axis=0)

    zero_acc = (jnp.zeros((8, LANES), F32), jnp.zeros((8, LANES), F32))

    def start_stats(k, acc, group):
        def fold(v):
            width = group
            while width < LANES:
                v = v + pltpu.roll(v, width, 1)
                width *= 2
            return jnp.sum(v, axis=0, keepdims=True)

        mine = jnp.concatenate([fold(acc[0]), fold(acc[1])], axis=0)
        stats[k] = mine
        for d in far_first(n):
            to_dev(stats.at[k], recv.at[k, d - 1], ssem.at[k], rsem.at[k], lax.rem(me + d, n)).start()
        return mine

    def end_stats(k, mine):
        to_dev(recv.at[k], recv.at[k], ssem.at[k], rsem.at[k], me).wait_recv()
        return mine + jnp.sum(recv[k], axis=0)

    def group_stats(k, acc, group):
        return end_stats(k, start_stats(k, acc, group))

    def norm_of(k, total, count):
        moments = total * (1.0 / count)
        mean = moments[0:1]
        var = moments[1:2] - mean * mean
        scale = bn_ref[k, 0:1] * lax.rsqrt(var + NORM_EPS)
        return mean, scale, bn_ref[k, 1:2]

    def bn(z, norm):
        mean, scale, shift = norm
        return (z - mean) * scale + shift

    lane2 = lax.broadcasted_iota(jnp.int32, (half_w, 2 * LANES), 1)
    even_lane = lax.rem(lane2 // 32, 2) == 0

    def split_parity(x, a):
        tscr[a] = x.astype(F32).T
        return [tscr[a, pl.ds(0, half_w, stride=2), :], tscr[a, pl.ds(1, half_w, stride=2), :]]

    def stage_a_part(x, w_ref):
        lhs = jnp.concatenate(split_parity(x, 0), axis=1).astype(BF16)
        y = jnp.dot(lhs, w_ref[...], preferred_element_type=F32)
        cross = y[:, 2 * LANES:]
        return y[:, : 2 * LANES] + jnp.where(even_lane, shift_down(cross), shift_up(cross))

    def third_row(q, carry):
        parts = []
        for a in range(2):
            x = jnp.concatenate([ximg[a, q, 1], xbelow[a, q, 0], xbelow[a, q, 1], ximg[a, q, 0]], axis=0)
            parts += split_parity(x, a)
        y = jnp.dot(jnp.concatenate(parts, axis=1).astype(BF16), wat_ref[...], preferred_element_type=F32)
        cross = y[:, LANES:]
        zthird[q] = y[:, :LANES] + jnp.where(even_lane[:, :LANES], shift_down(cross), shift_up(cross))
        return carry

    def own_a(q, carry):
        x = jnp.concatenate([ximg[0, q].reshape(2 * 32, full_w), ximg[1, q].reshape(2 * 32, full_w)], axis=0)
        z = stage_a_part(x, wao_ref)
        za[0, q] = z[:, :LANES]
        za[1, q] = z[:, LANES:]
        return carry

    over(everything, own_a)

    for copy in params[1:]:
        copy.wait()
    expand_down(wd_raw, wdn_ref)
    expand_blocks(wi_raw, wm_raw, wo_raw, win_ref, wmid_ref, wout_ref)
    bn_ref[0] = jnp.concatenate([ba_raw[0]] * 4, axis=1)
    bn_ref[1] = bd_raw[...]
    for j in range(wi_raw.shape[0]):
        bn_ref[2 + 3 * j] = jnp.concatenate([bi_raw[j]] * 2, axis=1)
        bn_ref[3 + 3 * j] = jnp.concatenate([bm_raw[j]] * 2, axis=1)
        bn_ref[4 + 3 * j] = bo_raw[j]

    def halo_a(q, acc):
        x = jnp.concatenate([xabove[0, q], xbelow[0, q, 0], xabove[1, q], xbelow[1, q, 0]], axis=0)
        z = stage_a_part(x, wah_ref)
        z0 = za[0, q] + z[:, :LANES]
        z1 = za[1, q] + z[:, LANES:]
        za[0, q] = z0
        za[1, q] = z1
        return add_stats(add_stats(acc, z0), z1)

    acc = zero_acc
    for c, span in enumerate(img_spans):
        arrived(img_down, img_up, c)
        acc = over(span, halo_a, acc)

    mine = start_stats(0, acc, 32)
    for c in range(len(row_spans)):
        @pl.when(has_prev)
        def _():
            row_up(c).start()

    @pl.when(has_next)
    def _():
        for c, span in enumerate(row_spans[:ROWS_AHEAD]):
            row_up(c).wait_recv()
            over(span, third_row)

    norm = norm_of(0, end_stats(0, mine), count_a)

    def down(q, acc):
        third = jnp.where(has_next, jnp.maximum(bn(zthird[q], norm), 0.0), 0.0).astype(BF16)
        for a in range(2):
            own = jnp.maximum(bn(za[a, q], norm), 0.0).astype(BF16)
            y = jnp.dot(jnp.concatenate([own, third], axis=1), wdn_ref[a], preferred_element_type=F32)
            z = y[:, :LANES] + shift_up(y[:, LANES:])
            zd[a, q] = z
            acc = add_stats(acc, z)
        return acc

    acc = zero_acc
    for c, span in enumerate(row_spans):
        if c >= ROWS_AHEAD:
            @pl.when(has_next)
            def _():
                row_up(c).wait_recv()
                over(span, third_row)

        acc = over(span, down, acc)
    norm = norm_of(1, group_stats(1, acc, LANES), count_b)

    blocks = win_ref.shape[0]

    def mid_down(j):
        def copy(c):
            part = pl.ds(*mid_spans[c])
            return to_dev(u2.at[j, part], habove.at[j, part], hsend_sem.at[j, 0, c], hrecv_sem.at[j, 0, c], nxt)
        return copy

    def mid_up(j):
        def copy(c):
            part = pl.ds(*mid_spans[c])
            return to_dev(u2.at[j, part], hbelow.at[j, part], hsend_sem.at[j, 1, c], hrecv_sem.at[j, 1, c], prv)
        return copy

    for j in range(blocks):
        def layer_in(q, acc):
            parts = []
            for a in range(2):
                if j == 0:
                    t = bn(zd[a, q], norm)
                else:
                    t = bn(zo[a, q], norm) + h[a, q].astype(F32)
                t = jnp.maximum(t, 0.0).astype(BF16)
                h[a, q] = t
                parts.append(t)
            z = jnp.dot(jnp.concatenate(parts, axis=1), win_ref[j], preferred_element_type=F32)
            zi[q] = z
            return add_stats(acc, z)

        acc = over(everything, layer_in, zero_acc, 4)
        norm = norm_of(2 + 3 * j, group_stats(2 + 3 * j, acc, 64), count_b)

        def act_in(q, carry):
            u2[j, q] = jnp.maximum(bn(zi[q], norm), 0.0).astype(BF16)
            return carry

        for c, span in enumerate(mid_spans):
            over(span, act_in)
            exchange(mid_down(j), mid_up(j), c)
        def layer_mid(q, acc):
            lhs = jnp.concatenate([u2[j, q], habove[j, q], hbelow[j, q]], axis=1)
            y = jnp.dot(lhs, wmid_ref[j], preferred_element_type=F32)
            z = shift_down(y[:, :LANES]) + y[:, LANES:2 * LANES] + shift_up(y[:, 2 * LANES:])
            zm[q] = z
            return add_stats(acc, z)

        acc = zero_acc
        for c, span in enumerate(mid_spans):
            arrived(mid_down(j), mid_up(j), c)
            acc = over(span, layer_mid, acc)
        norm = norm_of(3 + 3 * j, group_stats(3 + 3 * j, acc, 64), count_b)

        def layer_out(q, acc):
            u = jnp.maximum(bn(zm[q], norm), 0.0).astype(BF16)
            y = jnp.dot(u, wout_ref[j], preferred_element_type=F32)
            for a in range(2):
                z = y[:, a * LANES:(a + 1) * LANES]
                zo[a, q] = z
                acc = add_stats(acc, z)
            return acc

        acc = over(everything, layer_out, zero_acc, 4)
        norm = norm_of(4 + 3 * j, group_stats(4 + 3 * j, acc, LANES), count_b)

    def final(q, carry):
        for a in range(2):
            out_ref[a, q] = jnp.maximum(bn(zo[a, q], norm) + h[a, q].astype(F32), 0.0).astype(BF16)
        return carry

    over(everything, final, 0, 2)

    for k in range(stats.shape[0]):
        to_dev(recv.at[k], recv.at[k], ssem.at[k], rsem.at[k], me).wait_send()

    @pl.when(has_next)
    def _():
        for c in range(len(img_spans)):
            img_down(c).wait_send()
        for j in range(blocks):
            for c in range(len(mid_spans)):
                mid_down(j)(c).wait_send()

    @pl.when(has_prev)
    def _():
        for c in range(len(img_spans)):
            img_up(c).wait_send()
        for c in range(len(row_spans)):
            row_up(c).wait_send()
        for j in range(blocks):
            for c in range(len(mid_spans)):
                mid_up(j)(c).wait_send()


def solution(mesh):
    n = mesh.shape["sp"]

    def forward(images, w_a, bn_a, w_down, bn_down, w_in, bn_in, w_mid, bn_mid, w_out, bn_out):
        count, rows, width, chan_a = images.shape
        pairs, half_w = count // 2, width // 2
        blocks = w_in.shape[0]
        img = jnp.transpose(images, (0, 1, 3, 2)).reshape(2, pairs, rows, chan_a, width)
        taps = w_a.shape[1] * w_a.shape[2]
        raw = [
            w_a.reshape(taps * chan_a, chan_a), w_down.reshape(taps, chan_a, LANES), jnp.transpose(w_in, (0, 2, 1)),
            w_mid.reshape(blocks, taps, 64, 64), w_out, bn_a, bn_down, bn_in, bn_mid, bn_out,
        ]
        steps = 2 + 3 * blocks

        dma = pltpu.SemaphoreType.DMA
        out = pl.pallas_call(
            functools.partial(kernel, n),
            out_shape=pltpu.VMEM((2, pairs, half_w, LANES), BF16),
            in_specs=[pl.BlockSpec(memory_space=pltpu.HBM)] * 11,
            out_specs=pl.BlockSpec(memory_space=pltpu.VMEM),
            scratch_shapes=[pltpu.VMEM(x.shape, x.dtype) for x in raw] + [
                dma((len(raw),)),
                pltpu.VMEM((2 * LANES, 4 * LANES), BF16),
                pltpu.VMEM((2 * LANES, 4 * LANES), BF16),
                pltpu.VMEM((4 * LANES, 2 * LANES), BF16),
                pltpu.VMEM((2, 2 * LANES, 2 * LANES), BF16),
                pltpu.VMEM((blocks, 2 * LANES, LANES), BF16),
                pltpu.VMEM((blocks, 3 * LANES, 3 * LANES), BF16),
                pltpu.VMEM((blocks, LANES, 2 * LANES), BF16),
                pltpu.VMEM((steps, 2, LANES), F32),
                pltpu.VMEM((2, pairs, rows, chan_a, width), BF16),
                pltpu.VMEM((2, pairs, chan_a, width), BF16),
                pltpu.VMEM((2, pairs, rows, chan_a, width), BF16),
                pltpu.VMEM((2, width, LANES), F32),
                pltpu.VMEM((2, pairs, half_w, LANES), F32),
                pltpu.VMEM((pairs, half_w, LANES), F32),
                pltpu.VMEM((2, pairs, half_w, LANES), F32),
                pltpu.VMEM((2, pairs, half_w, LANES), BF16),
                pltpu.VMEM((pairs, half_w, LANES), F32),
                pltpu.VMEM((blocks, pairs, half_w, LANES), BF16),
                pltpu.VMEM((blocks, pairs, half_w, LANES), BF16),
                pltpu.VMEM((blocks, pairs, half_w, LANES), BF16),
                pltpu.VMEM((pairs, half_w, LANES), F32),
                pltpu.VMEM((2, pairs, half_w, LANES), F32),
                pltpu.VMEM((steps, 2, LANES), F32),
                pltpu.VMEM((steps, n - 1, 2, LANES), F32),
                dma((4,)),
                dma((2, len(IMG_CUTS))),
                dma((2, len(IMG_CUTS))),
                dma((len(ROW_CUTS),)),
                dma((len(ROW_CUTS),)),
                dma((blocks, 2, len(LATE_CUTS))),
                dma((blocks, 2, len(LATE_CUTS))),
                dma((steps,)),
                dma((steps,)),
            ],
            compiler_params=pltpu.CompilerParams(
                collective_id=0, has_side_effects=True, vmem_limit_bytes=52 * 1024 * 1024
            ),
        )(img, *raw)
        return out.reshape(count, rows // 2, half_w, LANES)

    act_spec = P("dp", "sp", None, None)
    return jax.shard_map(forward, mesh=mesh, in_specs=(act_spec,) + (P(),) * 10, out_specs=act_spec, check_vma=False)
```
